32 devices in a mesh: fsdp: 16 (over z, y, x), seq: 2 (over core).
Axes of the slice: x: 2, y: 2, z: 4, core: 2. Of those that a mesh axis runs over, the one named last changes fastest.
Arguments:
- block_input: bfloat16 [64, 512, 1024], P(('fsdp', 'seq')), may hold values from -6 to 6
- w_qkv: bfloat16 [1024, 3072], P('fsdp'), as said below
- w_out: bfloat16 [1024, 1024], P('fsdp'), may hold values from -1.5 to 1.5
- w_up: bfloat16 [1024, 4096], P('fsdp'), may hold values from -0.1875 to 0.1875
- w_down: bfloat16 [4096, 1024], P('fsdp'), may hold values from -0.09375 to 0.09375
- b_query: bfloat16 [1024], P('fsdp'), may hold values from -3 to 3
- b_value: bfloat16 [1024], P('fsdp'), may hold values from -3 to 3
- b_out: bfloat16 [1024], P('fsdp'), may hold values from -3 to 3
- b_up: bfloat16 [4096], P('fsdp'), may hold values from -3 to 3
- b_down: bfloat16 [1024], P('fsdp'), may hold values from -3 to 3
- gain_one: bfloat16 [1024], P('fsdp'), may hold values from 0.5 to 1.5
- shift_one: bfloat16 [1024], P('fsdp'), may hold values from -2 to 2
- gain_two: bfloat16 [1024], P('fsdp'), may hold values from 0.5 to 1.5
- shift_two: bfloat16 [1024], P('fsdp'), may hold values from -2 to 2
- cotangent: bfloat16 [64, 512, 1024], P(('fsdp', 'seq')), may hold values from -6 to 6
Outputs:
- block_output: bfloat16 [64, 512, 1024], P(('fsdp', 'seq'))
- input_grad: float32 [64, 512, 1024], P(('fsdp', 'seq'))
- grad_qkv: float32 [1024, 3072], P('fsdp')
- grad_out: float32 [1024, 1024], P('fsdp')
- grad_up: float32 [1024, 4096], P('fsdp')
- grad_down: float32 [4096, 1024], P('fsdp')
- grad_query_bias: float32 [1024], P('fsdp')
- grad_value_bias: float32 [1024], P('fsdp')
- grad_out_bias: float32 [1024], P('fsdp')
- grad_up_bias: float32 [4096], P('fsdp')
- grad_down_bias: float32 [1024], P('fsdp')
- grad_gain_one: float32 [1024], P('fsdp')
- grad_shift_one: float32 [1024], P('fsdp')
- grad_gain_two: float32 [1024], P('fsdp')
- grad_shift_two: float32 [1024], P('fsdp')
The draws below stay inside these ranges and needn't reach their ends.
Inputs may be any that keep to these rules, and one draw needn't show every extreme that they name: `w_qkv`: the query, key and value projections of every head, side by side.
All inputs are finite; a program needn't handle non-finite values.
Results may differ from the reference program's by a relative error of at most 0.013.
The reference program's roundings to bfloat16 on the way count: a program that leaves them out, or rounds other values in their place, can miss the bound.
Values may be sent and summed in bfloat16 or wider, within the bound.
A program may use at most 256 MiB of HBM per device.

```python
import jax
import jax.numpy as jnp
from jax import lax

D = 1024
H = 16
HD = 64
FF = 4096
SEQ_LEN = 512
SEQS = 64


def draw_w_qkv(key, part):
    base_key = jax.random.fold_in(jax.random.fold_in(key, 17), 0)
    weights = jax.random.normal(base_key, (D, 3 * D), jnp.float32) * D ** (-0.5)
    return weights.astype(jnp.bfloat16)


def block_levels(stream_key, extent, pieces, smallest, largest):
    level, own = 1.0, jax.random.fold_in(stream_key, 6)
    for dim, parts in pieces:
        steps = jnp.exp(jax.random.uniform(jax.random.fold_in(own, dim), (parts,), jnp.float32, smallest / len(pieces), largest / len(pieces)))
        level = level * jnp.repeat(steps, extent[dim] // parts).reshape([-1 if axis == dim else 1 for axis in range(len(extent))])
    return level


def scatter_about(rng, dims, scale, limit, cuts=(), dtype=jnp.bfloat16):
    values = scale * jax.random.normal(rng, dims, jnp.float32)
    if cuts:
        values = values * block_levels(rng, dims, cuts, -0.22, 0.18)
    return jnp.clip(values, -limit, limit).astype(dtype)


def setup_inputs(seed: int = 0) -> dict:
    splits = jax.random.split(jax.random.key(seed), 16)
    block_input = scatter_about(splits[0], (SEQS, SEQ_LEN, D), 1.0, 6.0, ((0, 32),))
    w_qkv = draw_w_qkv(jax.random.fold_in(splits[15], 71), 0)
    w_out = scatter_about(splits[2], (D, D), (D // 64) ** -0.5, 1.5, ((0, 16),))
    w_up = scatter_about(splits[3], (D, FF), D ** -0.5, 0.1875, ((0, 16),))
    w_down = scatter_about(splits[4], (FF, D), FF ** -0.5, 0.09375, ((0, 16),))
    b_query = scatter_about(splits[5], (D,), 0.5, 3.0, ((0, 16),))
    b_value = scatter_about(splits[6], (D,), 0.5, 3.0, ((0, 16),))
    b_out = scatter_about(splits[7], (D,), 0.5, 3.0, ((0, 16),))
    b_up = scatter_about(splits[8], (FF,), 0.5, 3.0, ((0, 16),))
    b_down = scatter_about(splits[9], (D,), 0.5, 3.0, ((0, 16),))
    gain_one = jnp.clip(1.0 + 0.1 * jax.random.normal(splits[10], (D,), jnp.float32), 0.5, 1.5).astype(jnp.bfloat16)
    shift_one = scatter_about(splits[11], (D,), 0.3, 2.0, ((0, 16),))
    gain_two = jnp.clip(1.0 + 0.1 * jax.random.normal(splits[12], (D,), jnp.float32), 0.5, 1.5).astype(jnp.bfloat16)
    shift_two = scatter_about(splits[13], (D,), 0.3, 2.0, ((0, 16),))
    cotangent = scatter_about(splits[14], (SEQS, SEQ_LEN, D), 1.0, 6.0, ((0, 32),))
    return {"block_input": block_input, "w_qkv": w_qkv, "w_out": w_out, "w_up": w_up, "w_down": w_down, "b_query": b_query, "b_value": b_value, "b_out": b_out, "b_up": b_up, "b_down": b_down, "gain_one": gain_one, "shift_one": shift_one, "gain_two": gain_two, "shift_two": shift_two, "cotangent": cotangent}


@jax.custom_vjp
def low(v):
    return lax.optimization_barrier(v.astype(jnp.bfloat16)).astype(jnp.float32)

@jax.custom_vjp
def low_back(v):
    return v

def low_keep(v):
    return (low(v), None)

def low_pass(kept, grad):
    return (grad,)

def back_keep(v):
    return (v, None)

def back_low(kept, grad):
    return (low(grad),)
low.defvjp(low_keep, low_pass)
low_back.defvjp(back_keep, back_low)

def layer_norm(values, gain, shift):
    center = values - lax.optimization_barrier(jnp.mean(values, -1, keepdims=True))
    spread = lax.optimization_barrier(jnp.mean(center * center, -1, keepdims=True))
    return center * lax.rsqrt(spread + 1e-05) * gain + shift

def product(left, right):
    return jnp.dot(left, right, precision=lax.Precision.HIGHEST, preferred_element_type=jnp.float32)

def block_one(sequence, params):
    w_qkv, w_out, w_up, w_down, b_query, b_value, b_out, b_up, b_down, gain_one, shift_one, gain_two, shift_two = params
    length = sequence.shape[0]
    model_width = sequence.shape[1]
    normed_one = low(layer_norm(sequence, gain_one, shift_one))
    merged = product(normed_one, w_qkv)
    query = low(low_back(merged[:, :model_width] + b_query))
    keys = low(low_back(merged[:, model_width:2 * model_width]))
    values = low(low_back(merged[:, 2 * model_width:] + b_value))
    query_heads = query.reshape(length, H, HD)
    key_heads = keys.reshape(length, H, HD)
    value_heads = values.reshape(length, H, HD)
    scores = jnp.einsum('qhd,khd->hqk', query_heads, key_heads, precision=lax.Precision.HIGHEST) * 0.125
    scores = low_back(scores)
    position = jnp.arange(length)
    allowed = position[None, :] <= position[:, None]
    probs = jax.nn.softmax(jnp.where(allowed[None], scores, -1e+30), axis=-1)
    attended = jnp.einsum('hqk,khd->qhd', low(probs), value_heads, precision=lax.Precision.HIGHEST)
    attended = low(low_back(attended.reshape(length, model_width)))
    middle = sequence + low_back(product(attended, w_out) + b_out)
    normed_two = low(layer_norm(middle, gain_two, shift_two))
    hidden = low_back(product(normed_two, w_up) + b_up)
    activated = low(jax.nn.gelu(hidden, approximate=True))
    return middle + low_back(product(activated, w_down) + b_down)

def reference(block_input, w_qkv, w_out, w_up, w_down, b_query, b_value, b_out, b_up, b_down, gain_one, shift_one, gain_two, shift_two, cotangent):
    params = tuple((item.astype(jnp.float32) for item in (w_qkv, w_out, w_up, w_down, b_query, b_value, b_out, b_up, b_down, gain_one, shift_one, gain_two, shift_two)))

    def whole(inputs, weights):
        return lax.map(jax.checkpoint(lambda sequence: block_one(sequence, weights)), inputs)
    output, pullback = jax.vjp(whole, block_input.astype(jnp.float32), params)
    input_grad, grads = pullback(cotangent.astype(jnp.float32))
    return (output.astype(jnp.bfloat16), input_grad, grads[0], grads[1], grads[2], grads[3], grads[4], grads[5], grads[6], grads[7], grads[8], grads[9], grads[10], grads[11], grads[12])
```

```python
import jax
import jax.numpy as jnp
from jax import lax
from jax.experimental import pallas as pl
from jax.experimental.pallas import tpu as pltpu
from jax.sharding import PartitionSpec as P

EPSILON = 1e-05
NEG_LARGE = -1e30
MESH = pl.DeviceIdType.MESH
NN = (((1,), (0,)), ((), ()))
NT = (((1,), (1,)), ((), ()))
TN = (((0,), (0,)), ((), ()))
BF16 = jnp.bfloat16
F32 = jnp.float32
VMEM_LIMIT = 60 * 2**20


def dot(left, right, dims=NN):
    return lax.dot_general(left, right, dims, preferred_element_type=F32)


class Place:
    def __init__(self):
        f = lax.axis_index("fsdp")
        self.c = lax.axis_index("seq")
        self.z, self.y, self.x = f // 4, (f // 2) % 2, f % 2

    def block(self, z, y, x):
        return z * 4 + y * 2 + x

    def dev(self, z, y, x):
        return (self.block(z, y, x), self.c)

    @property
    def xn(self):
        return self.dev(self.z, self.y, 1 - self.x)

    @property
    def yn(self):
        return self.dev(self.z, 1 - self.y, self.x)

    @property
    def up(self):
        return self.dev(self.z + 1, self.y, self.x)

    @property
    def down(self):
        return self.dev(self.z - 1, self.y, self.x)

    @property
    def partner(self):
        return (self.block(self.z, self.y, self.x), 1 - self.c)


def greet(p):
    barrier = pltpu.get_barrier_semaphore()

    def signal(device):
        pl.semaphore_signal(barrier, inc=1, device_id=device, device_id_type=MESH)

    for device in (p.xn, p.yn, p.partner):
        signal(device)

    @pl.when(p.z < 3)
    def _():
        signal(p.up)

    @pl.when(p.z > 0)
    def _():
        signal(p.down)

    inner = jnp.logical_and(p.z > 0, p.z < 3)

    @pl.when(inner)
    def _():
        pl.semaphore_wait(barrier, 5)

    @pl.when(jnp.logical_not(inner))
    def _():
        pl.semaphore_wait(barrier, 4)


def remote(src, dst, send, recv, device):
    return pltpu.make_async_remote_copy(
        src_ref=src, dst_ref=dst, send_sem=send, recv_sem=recv, device_id=device, device_id_type=MESH
    )


def wait_bytes(ref, sem):
    pltpu.make_async_copy(ref, ref, sem).wait()


AG_SEMS = 24


class Gather:
    def __init__(self, p, src, dst, sems):
        self.p, self.src, self.dst, self.sems = p, src, dst, sems
        self.rz = [None] * 4
        self.send, self.zsend, self.local, self.rp = (sems.at[20], sems.at[21], sems.at[22], sems.at[23])

    def half(self, z, y, x):
        return self.dst.at[2 * self.p.block(z, y, x) + self.p.c]

    def to(self, src, dst, recv, device, send=None):
        remote(src, dst, self.send if send is None else send, self.sems.at[recv], device).start()

    def spread(self, src, z):
        p = self.p
        mine = self.half(z, p.y, p.x)
        self.to(src, mine, 4 + z, p.xn)
        self.to(src, mine, 8 + z, p.yn)

    def along(self, src, z, up):
        p = self.p
        mine = self.half(z, p.y, p.x)

        @pl.when(p.z < 3 if up else p.z > 0)
        def _():
            self.to(src, mine, z, p.up if up else p.down, self.zsend)

    def start(self):
        p = self.p
        own = self.src.at[p.c]
        self.along(own, p.z, True)
        self.along(own, p.z, False)
        self.spread(own, p.z)
        me = p.block(p.z, p.y, p.x)
        pltpu.make_async_copy(self.src, self.dst.at[pl.ds(2 * me, 2)], self.local).start()

    def at_distance(self, s, body):
        p = self.p
        if s == 0:
            body(p.z, None)
            return

        @pl.when(p.z - s >= 0)
        def _():
            body(p.z - s, True)

        @pl.when(p.z + s <= 3)
        def _():
            body(p.z + s, False)

    def z_step(self, s):
        p = self.p

        def body(z, up):
            mine = self.half(z, p.y, p.x)
            wait_bytes(mine, self.sems.at[z])
            self.along(mine, z, up)
            self.spread(mine, z)
            self.to(mine, mine, 23, p.partner)

        self.at_distance(s, body)

    def xy_step(self, s):
        p = self.p

        def body(z, up):
            a = self.half(z, p.y, 1 - p.x)
            wait_bytes(a, self.sems.at[4 + z])
            self.to(a.at[0], a.at[0], 12 + z, p.yn)
            self.to(a, a, 23, p.partner)
            b = self.half(z, 1 - p.y, p.x)
            wait_bytes(b, self.sems.at[8 + z])
            self.to(b.at[1], b.at[1], 16 + z, p.xn)
            self.to(b, b, 23, p.partner)

        self.at_distance(s, body)

    def diag_step(self, s):
        p = self.p

        def body(z, up):
            d = self.half(z, 1 - p.y, 1 - p.x)
            wait_bytes(d.at[0], self.sems.at[12 + z])
            wait_bytes(d.at[1], self.sems.at[16 + z])
            self.to(d, d, 23, p.partner)

        self.at_distance(s, body)

    def finish(self):
        p = self.p
        wait_bytes(self.dst.at[pl.ds(0, 15)], self.rp)
        wait_bytes(self.dst.at[pl.ds(0, 27)], self.send)
        wait_bytes(self.dst.at[pl.ds(0, 2)], self.local)
        inner = jnp.logical_and(p.z > 0, p.z < 3)

        @pl.when(inner)
        def _():
            wait_bytes(self.dst.at[pl.ds(0, 5)], self.zsend)

        @pl.when(jnp.logical_not(inner))
        def _():
            wait_bytes(self.dst.at[pl.ds(0, 1)], self.zsend)


def gather_program(gathers):
    steps = []
    n = len(gathers)
    for i in range(n + 1):
        if i < n:
            steps.append(gathers[i].start)
            for s in (1, 2, 3):
                steps.append(lambda g=gathers[i], s=s: g.z_step(s))
        if i >= 1:
            g = gathers[i - 1]
            for s in range(5):
                if s < 4:
                    steps.append(lambda g=g, s=s: g.xy_step(s))
                if s >= 1:
                    steps.append(lambda g=g, s=s: g.diag_step(s - 1))
    for g in gathers:
        steps.append(g.finish)
    return steps


def gather_all(shards, collective_id):
    n = len(shards)
    views = []
    for shard in shards:
        r, width = shard.shape
        views.append(shard.reshape(2, 2, r // 4, width))

    def kernel(*refs):
        p = Place()
        greet(p)
        gathers = [Gather(p, refs[i], refs[n + i], refs[2 * n].at[i]) for i in range(n)]
        for step in gather_program(gathers):
            step()

    outs = pl.pallas_call(
        kernel,
        in_specs=[pl.BlockSpec(memory_space=pltpu.VMEM)] * n,
        out_specs=[pl.BlockSpec(memory_space=pl.ANY)] * n,
        out_shape=[jax.ShapeDtypeStruct((32,) + v.shape[1:], v.dtype) for v in views],
        scratch_shapes=[pltpu.SemaphoreType.DMA((n, AG_SEMS))],
        compiler_params=pltpu.CompilerParams(
            collective_id=collective_id, has_side_effects=True, vmem_limit_bytes=VMEM_LIMIT
        ),
        name="gather",
    )(*views)
    return [out.reshape(16 * shard.shape[0], shard.shape[1]) for out, shard in zip(outs, shards)]


RS_SEMS = 4 * 8 + 8


class Scatter:
    def __init__(self, p, g, out, bufs, sems):
        self.p, self.g, self.out, self.sems = p, g, out, sems
        self.o, self.pr, self.x1, self.y1, self.x2, self.y2, self.u, self.d = bufs
        self.psend, self.zsend, self.fsend, self.frecv = (sems.at[36 + i] for i in range(4))

    @staticmethod
    def scratch(q, width, dtype):
        return [
            pltpu.VMEM((4, 2, 2, 2, q, width), dtype),
            pltpu.VMEM((4, 2, 2, 2, q, width), dtype),
            pltpu.VMEM((4, 2, q, width), dtype),
            pltpu.VMEM((4, 2, q, width), dtype),
            pltpu.VMEM((4, q, width), dtype),
            pltpu.VMEM((4, q, width), dtype),
            pltpu.VMEM((4, 2, q, width), dtype),
            pltpu.VMEM((4, 2, q, width), dtype),
        ]

    def level(self, i):
        z = self.p.z
        return jnp.where(z < 2, 3 - i, i)

    def sem(self, kind, i):
        return self.sems.at[4 * kind + i]

    def start(self):
        p = self.p
        for i in range(4):
            z = self.level(i)
            theirs = self.g.at[z, :, :, 1 - p.c]
            remote(theirs, self.pr.at[z], self.psend, self.sem(0, i), p.partner).start()
            pltpu.make_async_copy(self.g.at[z, :, :, p.c], self.o.at[z], self.sem(1, i)).start()

    def stage0(self, i):
        p = self.p
        z = self.level(i)
        wait_bytes(self.o.at[z], self.sem(1, i))
        wait_bytes(self.pr.at[z], self.sem(0, i))

        def add(j, carry):
            y, x, k = j // 4, (j // 2) % 2, j % 2
            self.o[z, y, x, k] = self.o[z, y, x, k] + self.pr[z, y, x, k]
            return carry

        lax.fori_loop(0, 8, add, 0)
        remote(self.o.at[z, :, 1 - p.x, 0], self.x1.at[z], self.sems.at[32], self.sem(2, i), p.xn).start()
        remote(self.o.at[z, 1 - p.y, :, 1], self.y1.at[z], self.sems.at[33], self.sem(3, i), p.yn).start()

    def stage1(self, i):
        p = self.p
        z = self.level(i)
        wait_bytes(self.x1.at[z], self.sem(2, i))
        for y in range(2):
            self.o[z, y, p.x, 0] = self.o[z, y, p.x, 0] + self.x1[z, y]
        remote(self.o.at[z, 1 - p.y, p.x, 0], self.y2.at[z], self.sems.at[35], self.sem(4, i), p.yn).start()
        wait_bytes(self.y1.at[z], self.sem(3, i))
        for x in range(2):
            self.o[z, p.y, x, 1] = self.o[z, p.y, x, 1] + self.y1[z, x]
        remote(self.o.at[z, p.y, 1 - p.x, 1], self.x2.at[z], self.sems.at[34], self.sem(5, i), p.xn).start()

    def stage2(self, i):
        p = self.p
        z = self.level(i)
        wait_bytes(self.y2.at[z], self.sem(4, i))
        wait_bytes(self.x2.at[z], self.sem(5, i))
        self.o[z, p.y, p.x, 0] = self.o[z, p.y, p.x, 0] + self.y2[z]
        self.o[z, p.y, p.x, 1] = self.o[z, p.y, p.x, 1] + self.x2[z]

    def chain(self, z, up):
        p = self.p
        buf = self.u if up else self.d
        kind = 6 if up else 7
        mine = self.o.at[z, p.y, p.x]

        @pl.when(p.z > 0 if up else p.z < 3)
        def _():
            wait_bytes(buf.at[z], self.sems.at[4 * kind + z])
            self.o[z, p.y, p.x] = self.o[z, p.y, p.x] + buf[z]

        remote(mine, buf.at[z], self.zsend, self.sems.at[4 * kind + z], p.up if up else p.down).start()

    def stage3(self, i):
        p = self.p
        z = self.level(i)

        @pl.when(z > p.z)
        def _():
            self.chain(z, True)

        @pl.when(z < p.z)
        def _():
            self.chain(z, False)

    def stage4(self):
        p = self.p
        z = p.z
        self.out[p.c] = self.o[z, p.y, p.x].astype(F32)

        @pl.when(z > 0)
        def _():
            wait_bytes(self.u.at[z], self.sems.at[24 + z])
            self.out[p.c] = self.out[p.c] + self.u[z].astype(F32)

        @pl.when(z < 3)
        def _():
            wait_bytes(self.d.at[z], self.sems.at[28 + z])
            self.out[p.c] = self.out[p.c] + self.d[z].astype(F32)

        remote(self.out.at[p.c], self.out.at[p.c], self.fsend, self.frecv, p.partner).start()

    def finish(self):
        p = self.p
        wait_bytes(self.out.at[1 - p.c], self.frecv)
        wait_bytes(self.out.at[p.c], self.fsend)
        wait_bytes(self.o, self.psend)
        for k, ref in enumerate((self.x1, self.y1, self.x2, self.y2)):
            wait_bytes(ref, self.sems.at[32 + k])
        wait_bytes(self.u.at[pl.ds(0, 3)], self.zsend)


def scatter_program(scatters):
    steps = []
    for s in scatters:
        steps.append(s.start)
    chunks = [(s, i) for s in scatters for i in range(4)]
    n = len(chunks)
    for t in range(n + 12):
        for lag, name in ((0, "stage0"), (3, "stage1"), (6, "stage2"), (6, "stage3")):
            k = t - lag
            if 0 <= k < n:
                s, i = chunks[k]
                steps.append(lambda s=s, i=i, name=name: getattr(s, name)(i))
        k = t - 12
        if 0 <= k < n and chunks[k][1] == 3:
            steps.append(chunks[k][0].stage4)
    for s in scatters:
        steps.append(s.finish)
    return steps


def scatter_all(grads, collective_id):
    n = len(grads)
    views = []
    for grad in grads:
        rows, width = grad.shape
        views.append(grad.reshape(4, 2, 2, 2, 2, rows // 64, width))
    scratch = []
    for v in views:
        scratch += Scatter.scratch(v.shape[5], v.shape[6], v.dtype)

    def kernel(*refs):
        p = Place()
        greet(p)
        bufs = refs[2 * n : 2 * n + 8 * n]
        sems = refs[10 * n]
        scatters = [Scatter(p, refs[i], refs[n + i], bufs[8 * i : 8 * i + 8], sems.at[i]) for i in range(n)]
        for step in scatter_program(scatters):
            step()

    outs = pl.pallas_call(
        kernel,
        in_specs=[pl.BlockSpec(memory_space=pl.ANY)] * n,
        out_specs=[pl.BlockSpec(memory_space=pltpu.VMEM)] * n,
        out_shape=[jax.ShapeDtypeStruct((2, 2) + v.shape[5:], F32) for v in views],
        scratch_shapes=scratch + [pltpu.SemaphoreType.DMA((n, RS_SEMS))],
        compiler_params=pltpu.CompilerParams(
            collective_id=collective_id, has_side_effects=True, vmem_limit_bytes=VMEM_LIMIT
        ),
        name="scatter",
    )(*views)
    return [out.reshape(grad.shape[0] // 16, grad.shape[1]) for out, grad in zip(outs, grads)]


def lane_masks(rows, width, dtype=BF16):
    lanes = lax.broadcasted_iota(jnp.int32,(rows,width),1)
    return lanes < width//2
def pick(h, low, v):
    z=jnp.zeros_like(v)
    return jnp.where(low, v, z) if h==0 else jnp.where(low, z, v)
def fwd_body(q_ref,k_ref,v_ref,o_ref,l_ref, B):
    S=q_ref.shape[0]
    low=lane_masks(S,128)
    q=q_ref[...]*BF16(0.125); k=k_ref[...]; v=v_ref[...]
    qs=[pick(h,low,q) for h in (0,1)]; vs=[pick(h,low,v) for h in (0,1)]
    for b in range(S//B):
        end=(b+1)*B
        acc=None
        for h in (0,1):
            st=dot(k[:end],qs[h][b*B:end],NT)
            key=lax.broadcasted_iota(jnp.int32,(B,B),0); qry=lax.broadcasted_iota(jnp.int32,(B,B),1)
            diag=jnp.where(key<=qry, st[b*B:end], NEG_LARGE)
            st=jnp.concatenate([st[:b*B],diag],0) if b else diag
            m=jnp.max(st,0,keepdims=True)
            p=jnp.exp(st-m)
            l=jnp.sum(p,0,keepdims=True)
            l_ref[h:h+1,b*B:end]=m+jnp.log(l)
            pt=(p*(1.0/l)).astype(BF16)
            o=dot(pt,vs[h][:end],TN)
            acc=o if acc is None else acc+o
        o_ref[b*B:end,:]=acc.astype(BF16)
def bwd_body(q_ref,k_ref,v_ref,g_ref,l_ref,dq_ref,dk_ref,dv_ref,dk_acc,dv_acc,B):
    S=q_ref.shape[0]
    low=lane_masks(S,128)
    q=q_ref[...]*BF16(0.125); k=k_ref[...]; v=v_ref[...]; g=g_ref[...]
    qs=[pick(h,low,q) for h in (0,1)]; gs=[pick(h,low,g) for h in (0,1)]; ks=[pick(h,low,k) for h in (0,1)]
    for b in reversed(range(S//B)):
        end=(b+1)*B
        dq=None; dk=None; dv=None
        for h in (0,1):
            qb=qs[h][b*B:end]; gb=gs[h][b*B:end]
            st=dot(k[:end],qb,NT)
            p=jnp.exp(st-l_ref[h:h+1,b*B:end])
            key=lax.broadcasted_iota(jnp.int32,(B,B),0); qry=lax.broadcasted_iota(jnp.int32,(B,B),1)
            diag=jnp.where(key<=qry, p[b*B:end], 0.0)
            p=jnp.concatenate([p[:b*B],diag],0) if b else diag
            dp=dot(v[:end],gb,NT)
            inner=jnp.sum(p*dp,0,keepdims=True)
            ds=(p*(dp-inner)).astype(BF16)
            pb=p.astype(BF16)
            dvh=dot(pb,gb,NN); dkh=dot(ds,qb,NN); dqh=dot(ds,ks[h][:end],TN)
            dq=dqh if dq is None else dq+dqh
            dk=dkh if dk is None else dk+dkh
            dv=dvh if dv is None else dv+dvh
        dq_ref[b*B:end,:]=(dq*0.125).astype(BF16)
        if b==S//B-1:
            dk_acc[...]=dk; dv_acc[...]=dv
        else:
            dk_acc[:end,:]+=dk; dv_acc[:end,:]+=dv
    dk_ref[...]=dk_acc[...].astype(BF16)
    dv_ref[...]=dv_acc[...].astype(BF16)
def attn_fwd(merged, S, B=256):
    T=merged.shape[0]; D=merged.shape[1]//3; n=D//128
    def body(q,k,v,o,l): fwd_body(q,k,v,o,l.at[0,0],B)
    sp=lambda off: pl.BlockSpec((S,128),lambda s,h: (s,off+h))
    return pl.pallas_call(body,grid=(T//S,n),in_specs=[sp(0),sp(n),sp(2*n)],
        out_specs=[pl.BlockSpec((S,128),lambda s,h:(s,h)),pl.BlockSpec((1,1,2,S),lambda s,h:(s,h,0,0))],
        out_shape=[jax.ShapeDtypeStruct((T,D),BF16),jax.ShapeDtypeStruct((T//S,n,2,S),F32)],
        name="attn_fwd",compiler_params=pltpu.CompilerParams(vmem_limit_bytes=40*2**20))(merged,merged,merged)
def attn_bwd(merged, g, lse, S, B=256):
    T=merged.shape[0]; D=merged.shape[1]//3; n=D//128
    def body(q,k,v,gr,l,d,dka,dva): bwd_body(q,k,v,gr,l.at[0,0],d.at[0],d.at[1],d.at[2],dka,dva,B)
    sp=lambda off: pl.BlockSpec((S,128),lambda s,h: (s,off+h))
    return pl.pallas_call(body,grid=(T//S,n),in_specs=[sp(0),sp(n),sp(2*n),sp(0),pl.BlockSpec((1,1,2,S),lambda s,h:(s,h,0,0))],
        out_specs=pl.BlockSpec((3,S,128),lambda s,h:(0,s,h)),
        out_shape=jax.ShapeDtypeStruct((3,T,D),BF16),
        scratch_shapes=[pltpu.VMEM((S,128),F32)]*2,
        name="attn_bwd",compiler_params=pltpu.CompilerParams(vmem_limit_bytes=40*2**20))(merged,merged,merged,g,lse)


def layer_norm(values, gain, shift):
    center = values - jnp.mean(values, -1, keepdims=True)
    spread = jnp.mean(center * center, -1, keepdims=True)
    return center * lax.rsqrt(spread + EPSILON) * gain + shift


def norm_back(values, gain, grad):
    center = values - jnp.mean(values, -1, keepdims=True)
    inverse = lax.rsqrt(jnp.mean(center * center, -1, keepdims=True) + EPSILON)
    unit = center * inverse
    scaled = grad * gain
    first = jnp.mean(scaled, -1, keepdims=True)
    second = jnp.mean(scaled * unit, -1, keepdims=True)
    return (inverse * (scaled - first - unit * second), jnp.sum(grad * unit, 0), jnp.sum(grad, 0))


def gelu_pair(u):
    a = 0.7978845608028654
    inner = jnp.tanh(a * (u + 0.044715 * u * u * u))
    half = 0.5 * (1.0 + inner)
    slope = half + 0.5 * u * (1.0 - inner * inner) * (a * (1.0 + 3.0 * 0.044715 * u * u))
    return u * half, slope


def up_project(normed, w_up, b_up):
    rows, depth = normed.shape
    width = w_up.shape[1]
    tile = 512

    def body(n_ref, w_ref, b_ref, a_ref, s_ref):
        value, slope = gelu_pair(dot(n_ref[...], w_ref[...]) + b_ref[...])
        a_ref[...] = value.astype(BF16)
        s_ref[...] = slope.astype(BF16)

    out = pl.BlockSpec((rows // 2, tile), lambda j, i: (i, j))
    return pl.pallas_call(
        body,
        grid=(width // tile, 2),
        in_specs=[
            pl.BlockSpec((rows // 2, depth), lambda j, i: (i, 0)),
            pl.BlockSpec((depth, tile), lambda j, i: (0, j)),
            pl.BlockSpec((1, tile), lambda j, i: (0, j)),
        ],
        out_specs=[out, out],
        out_shape=[jax.ShapeDtypeStruct((rows, width), BF16)] * 2,
        compiler_params=pltpu.CompilerParams(vmem_limit_bytes=VMEM_LIMIT),
        name="up_project",
    )(normed, w_up, b_up)


def compute(rows, upstream, weights, small):
    w_qkv, w_out, w_up, w_down = weights
    b_query, b_value, b_out, b_up, b_down, gain_one, shift_one, gain_two, shift_two = small
    length, width = rows.shape[1], rows.shape[2]
    tokens = rows.shape[0] * length
    x = rows.reshape(tokens, width)
    c = upstream.reshape(tokens, width)
    xf, cf = x.astype(F32), c.astype(F32)
    normed_one = layer_norm(xf, gain_one, shift_one).astype(BF16)
    qkv_bias = jnp.concatenate([b_query, jnp.zeros_like(b_query), b_value])
    merged = (dot(normed_one, w_qkv) + qkv_bias).astype(BF16)
    attended, logsum = attn_fwd(merged, length)
    middle = xf + (dot(attended, w_out) + b_out)
    normed_two = layer_norm(middle, gain_two, shift_two).astype(BF16)
    activated, slope = up_project(normed_two, w_up, b_up[None])
    output = (middle + (dot(activated, w_down) + b_down)).astype(BF16)

    grad_down_bias = jnp.sum(cf, 0)
    grad_down = dot(activated, c, TN).astype(BF16)
    hidden_grad = (dot(c, w_down, NT) * slope.astype(F32)).astype(BF16)
    grad_up_bias = jnp.sum(hidden_grad.astype(F32), 0)
    grad_up = dot(normed_two, hidden_grad, TN).astype(BF16)
    part, grad_gain_two, grad_shift_two = norm_back(middle, gain_two, dot(hidden_grad, w_up, NT))
    middle_grad = cf + part
    branch_grad = middle_grad.astype(BF16)
    grad_out_bias = jnp.sum(branch_grad.astype(F32), 0)
    grad_out = dot(attended, branch_grad, TN).astype(BF16)
    attended_grad = dot(branch_grad, w_out, NT).astype(BF16)
    back = attn_bwd(merged, attended_grad, logsum, length)
    grad_query_bias = jnp.sum(back[0].astype(F32), 0)
    grad_value_bias = jnp.sum(back[2].astype(F32), 0)
    grad_qkv = jnp.concatenate([dot(normed_one, back[j], TN).astype(BF16) for j in range(3)], 1)
    normed_one_grad = sum(dot(back[j], w_qkv[:, j * width : (j + 1) * width], NT) for j in range(3))
    part, grad_gain_one, grad_shift_one = norm_back(xf, gain_one, normed_one_grad)
    input_grad = middle_grad + part
    return (
        output.reshape(rows.shape),
        input_grad.reshape(rows.shape),
        (grad_qkv, grad_out, grad_up, grad_down),
        (
            grad_query_bias,
            grad_value_bias,
            grad_out_bias,
            grad_up_bias,
            grad_down_bias,
            grad_gain_one,
            grad_shift_one,
            grad_gain_two,
            grad_shift_two,
        ),
    )


def pack_shards(vectors):
    wide = vectors[3]
    narrow = jnp.stack([v for k, v in enumerate(vectors) if k != 3])
    zeros = jnp.zeros_like(narrow)
    odd = lax.axis_index("fsdp") % 2 == 1
    lanes = jnp.concatenate([jnp.where(odd, zeros, narrow), jnp.where(odd, narrow, zeros)], 1)
    rows = jnp.concatenate([lanes, wide.reshape(2, 128)], 0)
    return jnp.pad(rows, ((0, 64 - rows.shape[0]), (0, 0)))


def unpack_whole(packed):
    blocks = packed.reshape(8, 2, 64, 128)
    narrow = (blocks[:, 0, :8] + blocks[:, 1, :8]).astype(F32)
    narrow = jnp.moveaxis(narrow, 0, 1).reshape(8, 1024)
    wide = blocks[:, :, 8:10].astype(F32).reshape(4096)
    return tuple(narrow[j] for j in range(3)) + (wide,) + tuple(narrow[j] for j in range(3, 8))


def pack_grads(vectors):
    narrow = jnp.stack([v for k, v in enumerate(vectors) if k != 3]).reshape(8, 8, 128)
    narrow = jnp.repeat(jnp.moveaxis(narrow, 1, 0), 2, axis=0)
    wide = vectors[3].reshape(16, 2, 128)
    rows = jnp.concatenate([narrow, wide], 1)
    return jnp.pad(rows, ((0, 0), (0, 22), (0, 0))).reshape(16 * 32, 128)


def unpack_shard(packed):
    odd = lax.axis_index("fsdp") % 2 == 1
    narrow = jnp.where(odd, packed[:8, 64:], packed[:8, :64])
    wide = packed[8:10].reshape(256)
    return tuple(narrow[j] for j in range(3)) + (wide,) + tuple(narrow[j] for j in range(3, 8))


def local_ring(block_input, *rest):
    shards, cotangent = rest[:13], rest[13]
    w_qkv, w_out, w_up, w_down, packed = gather_all(shards[:4] + (pack_shards(shards[4:]),), 0)
    small = unpack_whole(packed)
    output, input_grad, mats, vecs = compute(block_input, cotangent, (w_qkv, w_out, w_up, w_down), small)
    grad_down, grad_up, grad_out, grad_qkv, vec = scatter_all(
        [mats[3], mats[2], mats[1], mats[0], pack_grads(vecs)], 1
    )
    return (output, input_grad, grad_qkv, grad_out, grad_up, grad_down) + unpack_shard(vec)


def local_any(block_input, *rest):
    shards, cotangent = rest[:13], rest[13]
    whole = [lax.all_gather(shard, "fsdp", axis=0, tiled=True) for shard in shards]
    small = tuple(v.astype(F32) for v in whole[4:])
    output, input_grad, mats, vecs = compute(block_input, cotangent, whole[:4], small)

    def reduce(grad):
        part = lax.psum_scatter(grad.astype(F32), "fsdp", scatter_dimension=0, tiled=True)
        return lax.psum(part, "seq")

    return (output, input_grad) + tuple(reduce(grad) for grad in mats + vecs)


def solution(mesh):
    split = P(("fsdp", "seq"), None, None)
    matrix, vector = P("fsdp", None), P("fsdp")
    in_specs = (split,) + (matrix,) * 4 + (vector,) * 9 + (split,)
    out_specs = (split, split) + (matrix,) * 4 + (vector,) * 9
    local = local_ring if (mesh.shape["fsdp"], mesh.shape["seq"]) == (16, 2) else local_any
    return jax.shard_map(local, mesh=mesh, in_specs=in_specs, out_specs=out_specs, check_vma=False)
```

```python
import jax
import jax.numpy as jnp
from jax import lax
from jax.experimental import pallas as pl
from jax.experimental.pallas import tpu as pltpu
from jax.sharding import PartitionSpec as P

EPSILON = 1e-05
NEG_LARGE = -1e30
MESH = pl.DeviceIdType.MESH
NN = (((1,), (0,)), ((), ()))
NT = (((1,), (1,)), ((), ()))
TN = (((0,), (0,)), ((), ()))
BF16 = jnp.bfloat16
F32 = jnp.float32
VMEM_LIMIT = 60 * 2**20


def dot(left, right, dims=NN):
    return lax.dot_general(left, right, dims, preferred_element_type=F32)


class Place:
    def __init__(self):
        f = lax.axis_index("fsdp")
        self.c = lax.axis_index("seq")
        self.z, self.y, self.x = f // 4, (f // 2) % 2, f % 2

    def block(self, z, y, x):
        return z * 4 + y * 2 + x

    def dev(self, z, y, x):
        return (self.block(z, y, x), self.c)

    @property
    def xn(self):
        return self.dev(self.z, self.y, 1 - self.x)

    @property
    def yn(self):
        return self.dev(self.z, 1 - self.y, self.x)

    @property
    def up(self):
        return self.dev(self.z + 1, self.y, self.x)

    @property
    def down(self):
        return self.dev(self.z - 1, self.y, self.x)

    @property
    def partner(self):
        return (self.block(self.z, self.y, self.x), 1 - self.c)


def greet(p):
    barrier = pltpu.get_barrier_semaphore()

    def signal(device):
        pl.semaphore_signal(barrier, inc=1, device_id=device, device_id_type=MESH)

    for device in (p.xn, p.yn, p.partner):
        signal(device)

    @pl.when(p.z < 3)
    def _():
        signal(p.up)

    @pl.when(p.z > 0)
    def _():
        signal(p.down)

    inner = jnp.logical_and(p.z > 0, p.z < 3)

    @pl.when(inner)
    def _():
        pl.semaphore_wait(barrier, 5)

    @pl.when(jnp.logical_not(inner))
    def _():
        pl.semaphore_wait(barrier, 4)


def remote(src, dst, send, recv, device):
    return pltpu.make_async_remote_copy(
        src_ref=src, dst_ref=dst, send_sem=send, recv_sem=recv, device_id=device, device_id_type=MESH
    )


def wait_bytes(ref, sem):
    pltpu.make_async_copy(ref, ref, sem).wait()


AG_SEMS = 24


class Gather:
    def __init__(self, p, src, dst, sems):
        self.p, self.src, self.dst, self.sems = p, src, dst, sems
        self.rz = [None] * 4
        self.send, self.zsend, self.local, self.rp = (sems.at[20], sems.at[21], sems.at[22], sems.at[23])

    def half(self, z, y, x):
        return self.dst.at[2 * self.p.block(z, y, x) + self.p.c]

    def to(self, src, dst, recv, device, send=None):
        remote(src, dst, self.send if send is None else send, self.sems.at[recv], device).start()

    def spread(self, src, z):
        p = self.p
        mine = self.half(z, p.y, p.x)
        self.to(src, mine, 4 + z, p.xn)
        self.to(src, mine, 8 + z, p.yn)

    def along(self, src, z, up):
        p = self.p
        mine = self.half(z, p.y, p.x)

        @pl.when(p.z < 3 if up else p.z > 0)
        def _():
            self.to(src, mine, z, p.up if up else p.down, self.zsend)

    def start(self):
        p = self.p
        own = self.src.at[p.c]
        self.along(own, p.z, True)
        self.along(own, p.z, False)
        self.spread(own, p.z)
        me = p.block(p.z, p.y, p.x)
        pltpu.make_async_copy(self.src, self.dst.at[pl.ds(2 * me, 2)], self.local).start()

    def at_distance(self, s, body):
        p = self.p
        if s == 0:
            body(p.z, None)
            return

        @pl.when(p.z - s >= 0)
        def _():
            body(p.z - s, True)

        @pl.when(p.z + s <= 3)
        def _():
            body(p.z + s, False)

    def z_step(self, s):
        p = self.p

        def body(z, up):
            mine = self.half(z, p.y, p.x)
            wait_bytes(mine, self.sems.at[z])
            self.along(mine, z, up)
            self.spread(mine, z)
            self.to(mine, mine, 23, p.partner)

        self.at_distance(s, body)

    def xy_step(self, s):
        p = self.p

        def body(z, up):
            a = self.half(z, p.y, 1 - p.x)
            wait_bytes(a, self.sems.at[4 + z])
            self.to(a.at[0], a.at[0], 12 + z, p.yn)
            self.to(a, a, 23, p.partner)
            b = self.half(z, 1 - p.y, p.x)
            wait_bytes(b, self.sems.at[8 + z])
            self.to(b.at[1], b.at[1], 16 + z, p.xn)
            self.to(b, b, 23, p.partner)

        self.at_distance(s, body)

    def diag_step(self, s):
        p = self.p

        def body(z, up):
            d = self.half(z, 1 - p.y, 1 - p.x)
            wait_bytes(d.at[0], self.sems.at[12 + z])
            wait_bytes(d.at[1], self.sems.at[16 + z])
            self.to(d, d, 23, p.partner)

        self.at_distance(s, body)

    def arrived(self):
        wait_bytes(self.dst.at[pl.ds(0, 15)], self.rp)
        wait_bytes(self.dst.at[pl.ds(0, 2)], self.local)

    def drain(self):
        p = self.p
        wait_bytes(self.dst.at[pl.ds(0, 27)], self.send)
        inner = jnp.logical_and(p.z > 0, p.z < 3)

        @pl.when(inner)
        def _():
            wait_bytes(self.dst.at[pl.ds(0, 5)], self.zsend)

        @pl.when(jnp.logical_not(inner))
        def _():
            wait_bytes(self.dst.at[pl.ds(0, 1)], self.zsend)


def z_steps(g):
    return [g.start] + [lambda s=s: g.z_step(s) for s in (1, 2, 3)]


def xy_steps(g):
    return [lambda s=s: g.xy_step(s) for s in range(4)]


def diag_steps(g):
    return [lambda s=s: g.diag_step(s) for s in range(4)]


def weave(*lists):
    return [item[k] for k in range(max(map(len, lists))) for item in lists if k < len(item)]


def hook(index, table):
    for k, steps in table.items():

        @pl.when(index == k)
        def _(steps=steps):
            for step in steps:
                step()


def spread(steps, slots):
    table = {}
    for k, step in enumerate(steps):
        table.setdefault(slots[min(k * len(slots) // len(steps), len(slots) - 1)], []).append(step)
    return table


RS_SEMS = 44


class Scatter:
    def __init__(self, p, g, out, pr, bufs, tmp, sems):
        self.p, self.g, self.out, self.pr, self.tmp, self.sems = p, g, out, pr, tmp, sems
        self.o, self.x1, self.y1, self.x2, self.y2, self.u, self.d = bufs
        self.psend, self.zsend, self.fsend, self.frecv = (sems.at[36 + i] for i in range(4))

    @staticmethod
    def scratch(q, width, dtype):
        shapes = [(4, 2, 2, 2), (4, 2), (4, 2), (4,), (4,), (4, 2), (4, 2)]
        return [pltpu.VMEM(shape + (q, width), dtype) for shape in shapes]

    def level(self, i):
        z = self.p.z
        return jnp.where(z < 2, 3 - i, i)

    def sem(self, kind, i):
        return self.sems.at[4 * kind + i]

    def start(self):
        p = self.p
        for i in range(4):
            z = self.level(i)
            theirs = self.g.at[z, :, :, 1 - p.c]
            remote(theirs, self.pr.at[z], self.psend, self.sem(0, i), p.partner).start()
            pltpu.make_async_copy(self.g.at[z, :, :, p.c], self.o.at[z], self.sem(1, i)).start()

    def fetch(self, i):
        z = self.level(i)
        wait_bytes(self.pr.at[z], self.sem(0, i))
        pltpu.make_async_copy(self.pr.at[z], self.tmp.at[i % 2], self.sems.at[40 + i]).start()

    def stage0(self, i):
        p = self.p
        z = self.level(i)
        wait_bytes(self.o.at[z], self.sem(1, i))
        wait_bytes(self.tmp.at[i % 2], self.sems.at[40 + i])

        def add(j, carry):
            y, x, k = j // 4, (j // 2) % 2, j % 2
            self.o[z, y, x, k] = self.o[z, y, x, k] + self.tmp[i % 2, y, x, k]
            return carry

        lax.fori_loop(0, 8, add, 0)
        remote(self.o.at[z, :, 1 - p.x, 0], self.x1.at[z], self.sems.at[32], self.sem(2, i), p.xn).start()
        remote(self.o.at[z, 1 - p.y, :, 1], self.y1.at[z], self.sems.at[33], self.sem(3, i), p.yn).start()

    def stage1(self, i):
        p = self.p
        z = self.level(i)
        wait_bytes(self.x1.at[z], self.sem(2, i))
        for y in range(2):
            self.o[z, y, p.x, 0] = self.o[z, y, p.x, 0] + self.x1[z, y]
        remote(self.o.at[z, 1 - p.y, p.x, 0], self.y2.at[z], self.sems.at[35], self.sem(4, i), p.yn).start()
        wait_bytes(self.y1.at[z], self.sem(3, i))
        for x in range(2):
            self.o[z, p.y, x, 1] = self.o[z, p.y, x, 1] + self.y1[z, x]
        remote(self.o.at[z, p.y, 1 - p.x, 1], self.x2.at[z], self.sems.at[34], self.sem(5, i), p.xn).start()

    def along(self, z, up):
        p = self.p
        buf, kind = (self.u, 6) if up else (self.d, 7)
        remote(
            self.o.at[z, p.y, p.x], buf.at[z], self.zsend, self.sems.at[4 * kind + z], p.up if up else p.down
        ).start()

    def chain(self, z, up):
        p = self.p
        buf, kind = (self.u, 6) if up else (self.d, 7)
        wait_bytes(buf.at[z], self.sems.at[4 * kind + z])
        self.o[z, p.y, p.x] = self.o[z, p.y, p.x] + buf[z]
        self.along(z, up)

    def stage2(self, i):
        p = self.p
        z = self.level(i)
        wait_bytes(self.y2.at[z], self.sem(4, i))
        wait_bytes(self.x2.at[z], self.sem(5, i))
        self.o[z, p.y, p.x, 0] = self.o[z, p.y, p.x, 0] + self.y2[z]
        self.o[z, p.y, p.x, 1] = self.o[z, p.y, p.x, 1] + self.x2[z]

        @pl.when(jnp.logical_and(p.z == 0, z > 0))
        def _():
            self.along(z, True)

        @pl.when(jnp.logical_and(p.z == 3, z < 3))
        def _():
            self.along(z, False)

    def stage3(self, i):
        p = self.p
        z = self.level(i)
        inner = jnp.logical_and(p.z > 0, p.z < 3)

        @pl.when(jnp.logical_and(inner, z > p.z))
        def _():
            self.chain(z, True)

        @pl.when(jnp.logical_and(inner, z < p.z))
        def _():
            self.chain(z, False)

    def stage4(self, i=0):
        p = self.p
        z = p.z
        self.out[p.c] = self.o[z, p.y, p.x].astype(F32)

        @pl.when(z > 0)
        def _():
            wait_bytes(self.u.at[z], self.sems.at[24 + z])
            self.out[p.c] = self.out[p.c] + self.u[z].astype(F32)

        @pl.when(z < 3)
        def _():
            wait_bytes(self.d.at[z], self.sems.at[28 + z])
            self.out[p.c] = self.out[p.c] + self.d[z].astype(F32)

        remote(self.out.at[p.c], self.out.at[p.c], self.fsend, self.frecv, p.partner).start()

    def finish(self):
        p = self.p
        wait_bytes(self.out.at[1 - p.c], self.frecv)
        wait_bytes(self.out.at[p.c], self.fsend)
        wait_bytes(self.o, self.psend)
        for k, ref in enumerate((self.x1, self.y1, self.x2, self.y2)):
            wait_bytes(ref, self.sems.at[32 + k])
        wait_bytes(self.u.at[pl.ds(0, 3)], self.zsend)


def lane_masks(rows, width, dtype=BF16):
    lanes = lax.broadcasted_iota(jnp.int32,(rows,width),1)
    return lanes < width//2
def pick(h, low, v):
    z=jnp.zeros_like(v)
    return jnp.where(low, v, z) if h==0 else jnp.where(low, z, v)
def fwd_body(q_ref,k_ref,v_ref,o_ref,l_ref, B):
    S=q_ref.shape[0]
    low=lane_masks(S,128)
    q=q_ref[...]*BF16(0.125); k=k_ref[...]; v=v_ref[...]
    qs=[pick(h,low,q) for h in (0,1)]; vs=[pick(h,low,v) for h in (0,1)]
    for b in range(S//B):
        end=(b+1)*B
        acc=None
        for h in (0,1):
            st=dot(k[:end],qs[h][b*B:end],NT)
            key=lax.broadcasted_iota(jnp.int32,(B,B),0); qry=lax.broadcasted_iota(jnp.int32,(B,B),1)
            diag=jnp.where(key<=qry, st[b*B:end], NEG_LARGE)
            st=jnp.concatenate([st[:b*B],diag],0) if b else diag
            m=jnp.max(st,0,keepdims=True)
            p=jnp.exp(st-m)
            l=jnp.sum(p,0,keepdims=True)
            l_ref[h:h+1,b*B:end]=m+jnp.log(l)
            pt=(p*(1.0/l)).astype(BF16)
            o=dot(pt,vs[h][:end],TN)
            acc=o if acc is None else acc+o
        o_ref[b*B:end,:]=acc.astype(BF16)
def bwd_body(q_ref,k_ref,v_ref,g_ref,l_ref,dq_ref,dk_ref,dv_ref,dk_acc,dv_acc,B):
    S=q_ref.shape[0]
    low=lane_masks(S,128)
    q=q_ref[...]*BF16(0.125); k=k_ref[...]; v=v_ref[...]; g=g_ref[...]
    qs=[pick(h,low,q) for h in (0,1)]; gs=[pick(h,low,g) for h in (0,1)]; ks=[pick(h,low,k) for h in (0,1)]
    for b in reversed(range(S//B)):
        end=(b+1)*B
        dq=None; dk=None; dv=None
        for h in (0,1):
            qb=qs[h][b*B:end]; gb=gs[h][b*B:end]
            st=dot(k[:end],qb,NT)
            p=jnp.exp(st-l_ref[h:h+1,b*B:end])
            key=lax.broadcasted_iota(jnp.int32,(B,B),0); qry=lax.broadcasted_iota(jnp.int32,(B,B),1)
            diag=jnp.where(key<=qry, p[b*B:end], 0.0)
            p=jnp.concatenate([p[:b*B],diag],0) if b else diag
            dp=dot(v[:end],gb,NT)
            inner=jnp.sum(p*dp,0,keepdims=True)
            ds=(p*(dp-inner)).astype(BF16)
            pb=p.astype(BF16)
            dvh=dot(pb,gb,NN); dkh=dot(ds,qb,NN); dqh=dot(ds,ks[h][:end],TN)
            dq=dqh if dq is None else dq+dqh
            dk=dkh if dk is None else dk+dkh
            dv=dvh if dv is None else dv+dvh
        dq_ref[b*B:end,:]=(dq*0.125).astype(BF16)
        if b==S//B-1:
            dk_acc[...]=dk; dv_acc[...]=dv
        else:
            dk_acc[:end,:]+=dk; dv_acc[:end,:]+=dv
    dk_ref[...]=dk_acc[...].astype(BF16)
    dv_ref[...]=dv_acc[...].astype(BF16)
def attn_fwd(merged, S, B=256):
    T=merged.shape[0]; D=merged.shape[1]//3; n=D//128
    def body(q,k,v,o,l): fwd_body(q,k,v,o,l.at[0,0],B)
    sp=lambda off: pl.BlockSpec((S,128),lambda s,h: (s,off+h))
    return pl.pallas_call(body,grid=(T//S,n),in_specs=[sp(0),sp(n),sp(2*n)],
        out_specs=[pl.BlockSpec((S,128),lambda s,h:(s,h)),pl.BlockSpec((1,1,2,S),lambda s,h:(s,h,0,0))],
        out_shape=[jax.ShapeDtypeStruct((T,D),BF16),jax.ShapeDtypeStruct((T//S,n,2,S),F32)],
        name="attn_fwd",compiler_params=pltpu.CompilerParams(vmem_limit_bytes=40*2**20))(merged,merged,merged)
def attn_bwd(merged, g, lse, S, B=256):
    T=merged.shape[0]; D=merged.shape[1]//3; n=D//128
    def body(q,k,v,gr,l,d,dka,dva): bwd_body(q,k,v,gr,l.at[0,0],d.at[0],d.at[1],d.at[2],dka,dva,B)
    sp=lambda off: pl.BlockSpec((S,128),lambda s,h: (s,off+h))
    return pl.pallas_call(body,grid=(T//S,n),in_specs=[sp(0),sp(n),sp(2*n),sp(0),pl.BlockSpec((1,1,2,S),lambda s,h:(s,h,0,0))],
        out_specs=pl.BlockSpec((3,S,128),lambda s,h:(0,s,h)),
        out_shape=jax.ShapeDtypeStruct((3,T,D),BF16),
        scratch_shapes=[pltpu.VMEM((S,128),F32)]*2,
        name="attn_bwd",compiler_params=pltpu.CompilerParams(vmem_limit_bytes=40*2**20))(merged,merged,merged,g,lse)


def layer_norm(values, gain, shift):
    center = values - jnp.mean(values, -1, keepdims=True)
    spread = jnp.mean(center * center, -1, keepdims=True)
    return center * lax.rsqrt(spread + EPSILON) * gain + shift


def norm_back(values, gain, grad):
    center = values - jnp.mean(values, -1, keepdims=True)
    inverse = lax.rsqrt(jnp.mean(center * center, -1, keepdims=True) + EPSILON)
    unit = center * inverse
    scaled = grad * gain
    first = jnp.mean(scaled, -1, keepdims=True)
    second = jnp.mean(scaled * unit, -1, keepdims=True)
    return (inverse * (scaled - first - unit * second), jnp.sum(grad * unit, 0), jnp.sum(grad, 0))


def gelu_pair(u):
    a = 0.7978845608028654
    square = u * u
    half = 0.5 + 0.5 * jnp.tanh(u * (a + (a * 0.044715) * square))
    value = u * half
    slope = half + value * (1.0 - half) * (2.0 * a + (6.0 * a * 0.044715) * square)
    return value, slope


def whole_spec(ref, tile=None):
    n, two, q, width = ref.shape
    if tile is None:
        return pl.BlockSpec((n, two, q, width), lambda j: (0, 0, 0, 0))
    return pl.BlockSpec((n, two, q, tile), lambda j: (0, 0, 0, j))


def rows_of(block):
    value = block[...]
    return value.reshape(-1, value.shape[-1])


def forward_kernel(length, *refs):
    (shards, refs) = (refs[:5], refs[5:])
    x_ref, c_ref = refs[:2]
    (wholes, refs) = (refs[2:7], refs[7:])
    n1_ref, merged, logsum, attended, middle, n2_ref, act, slope, grad_down, small, refs = refs[:10] + (refs[10:],)
    b_up, qkv_bias, vec, hidden, sems, vsem = refs
    tokens, width = x_ref.shape
    p = Place()
    greet(p)
    order = [4, 0, 1, 2, 3]
    g_vec, g_qkv, g_out, g_up, g_down = [Gather(p, shards[i], wholes[i], sems.at[i]) for i in order]
    head = z_steps(g_vec) + weave(z_steps(g_qkv), xy_steps(g_vec))
    head += weave(z_steps(g_out), xy_steps(g_qkv), diag_steps(g_vec))
    for step in head:
        step()
    g_vec.arrived()
    load = pltpu.make_async_copy(wholes[4], vec, vsem)
    load.start()
    load.wait()
    for k in range(8):
        small[:, pl.ds(128 * k, 128)] = (vec[4 * k, 0, :8] + vec[4 * k + 2, 0, :8]).astype(F32)
    for k in range(16):
        for i in range(2):
            b_up[:, pl.ds(256 * k + 128 * i, 128)] = vec[2 * k, 0, 8 + i : 9 + i].astype(F32)
    qkv_bias[:, :width] = small[0:1]
    qkv_bias[:, width : 2 * width] = jnp.zeros_like(small[0:1])
    qkv_bias[:, 2 * width :] = small[1:2]

    def norm_rows(i, carry):
        rows = pl.ds(i * 128, 128)
        n1_ref[rows, :] = layer_norm(x_ref[rows, :].astype(F32), small[4:5], small[5:6]).astype(BF16)
        return carry

    lax.fori_loop(0, tokens // 128, norm_rows, 0)
    for step in weave(z_steps(g_up), diag_steps(g_qkv)):
        step()
    g_qkv.arrived()

    rest = weave(xy_steps(g_out), z_steps(g_down)) + diag_steps(g_out) + xy_steps(g_up)
    n_qkv, tile = 3 * width // 512, 512
    table = spread(rest[:8], range(n_qkv))

    def qkv_body(w_ref, o_ref):
        j = pl.program_id(0)
        hook(j, table)
        bias = qkv_bias[:, pl.ds(pl.multiple_of(j * tile, tile), tile)]
        o_ref[...] = (dot(n1_ref[...], rows_of(w_ref)) + bias).astype(BF16)

    pltpu.emit_pipeline(
        qkv_body,
        grid=(n_qkv,),
        in_specs=[whole_spec(wholes[0], tile)],
        out_specs=[pl.BlockSpec((tokens, tile), lambda j: (0, j))],
    )(wholes[0], merged)

    pairs = width // 128
    attend_table = spread(rest[8:], range(0, (tokens // length) * pairs, 2))

    def attend_body(q, k, v, o, l):
        s, h = pl.program_id(0), pl.program_id(1)
        hook(s * pairs + h, attend_table)
        fwd_body(q, k, v, o, l.at[0, 0], 256)

    def head_spec(off):
        return pl.BlockSpec((length, 128), lambda s, h: (s, off + h))

    pltpu.emit_pipeline(
        attend_body,
        grid=(tokens // length, pairs),
        in_specs=[head_spec(0), head_spec(pairs), head_spec(2 * pairs)],
        out_specs=[head_spec(0), pl.BlockSpec((1, 1, 2, length), lambda s, h: (s, h, 0, 0))],
    )(merged, merged, merged, attended, logsum)

    g_out.arrived()
    out_table = spread(diag_steps(g_up), range(tokens // 256))

    def out_body(a_ref, w_ref, m_ref):
        i = pl.program_id(0)
        hook(i, out_table)
        rows = pl.ds(pl.multiple_of(i * 256, 256), 256)
        value = x_ref[rows, :].astype(F32) + (dot(a_ref[...], rows_of(w_ref)) + small[2:3])
        m_ref[...] = value
        n2_ref[rows, :] = layer_norm(value, small[6:7], small[7:8]).astype(BF16)

    pltpu.emit_pipeline(
        out_body,
        grid=(tokens // 256,),
        in_specs=[pl.BlockSpec((256, width), lambda i: (i, 0)), whole_spec(wholes[1])],
        out_specs=[pl.BlockSpec((256, width), lambda i: (i, 0))],
    )(attended, wholes[1], middle)

    g_up.arrived()
    n_up = act.shape[1] // tile
    up_table = spread(xy_steps(g_down), range(1, n_up, 2))

    def gelu_tile(j, a_ref, s_ref):
        bias = b_up[:, pl.ds(pl.multiple_of(j * tile, tile), tile)]

        value, grad = gelu_pair(hidden[j % 2] + bias)
        a_ref[...] = value.astype(BF16)
        s_ref[...] = grad.astype(BF16)

    def up_body(w_ref, a_ref, s_ref):
        j = pl.program_id(0)
        hook(j, up_table)

        @pl.when(j == 0)
        def _():
            hidden[0] = dot(n2_ref[...], rows_of(w_ref))

        @pl.when(jnp.logical_and(j > 0, j < n_up))
        def _():
            gelu_tile(j - 1, a_ref, s_ref)
            hidden[j % 2] = dot(n2_ref[...], rows_of(w_ref))

        @pl.when(j == n_up)
        def _():
            gelu_tile(j - 1, a_ref, s_ref)

    n, two, q, _ = wholes[2].shape
    late = pl.BlockSpec((tokens, tile), lambda j: (0, jnp.maximum(j - 1, 0)))
    pltpu.emit_pipeline(
        up_body,
        grid=(n_up + 1,),
        in_specs=[pl.BlockSpec((n, two, q, tile), lambda j: (0, 0, 0, jnp.minimum(j, n_up - 1)))],
        out_specs=[late, late],
    )(wholes[2], act, slope)

    down_table = spread(diag_steps(g_down), range(1, n_up, 2))

    def grad_body(a_ref, o_ref):
        hook(pl.program_id(0), down_table)
        o_ref[...] = dot(a_ref[...], c_ref[...], TN).astype(BF16)

    pltpu.emit_pipeline(
        grad_body,
        grid=(n_up,),
        in_specs=[pl.BlockSpec((tokens, tile), lambda j: (0, j))],
        out_specs=[pl.BlockSpec((tile, width), lambda j: (j, 0))],
    )(act, grad_down)
    g_down.arrived()
    for g in (g_vec, g_qkv, g_out, g_up, g_down):
        g.drain()


def forward_call(shards, x, c, length):
    tokens, width = x.shape
    hidden = 16 * shards[3].shape[0]
    views = [s.reshape(2, 2, s.shape[0] // 4, s.shape[1]) for s in shards]
    whole = [jax.ShapeDtypeStruct((32,) + v.shape[1:], v.dtype) for v in views]
    vmem, any_space = pl.BlockSpec(memory_space=pltpu.VMEM), pl.BlockSpec(memory_space=pl.ANY)
    low = lambda *shape: jax.ShapeDtypeStruct(shape, BF16)
    outs = pl.pallas_call(
        lambda *refs: forward_kernel(length, *refs),
        in_specs=[vmem] * 7,
        out_specs=[any_space] * 5 + [vmem] + [any_space] * 4 + [vmem] + [any_space] * 3 + [vmem],
        out_shape=whole
        + [
            low(tokens, width),
            low(tokens, 3 * width),
            jax.ShapeDtypeStruct((tokens // length, width // 128, 2, length), F32),
            low(tokens, width),
            jax.ShapeDtypeStruct((tokens, width), F32),
            low(tokens, width),
            low(tokens, hidden),
            low(tokens, hidden),
            low(hidden, width),
            jax.ShapeDtypeStruct((8, width), F32),
        ],
        scratch_shapes=[
            pltpu.VMEM((1, hidden), F32),
            pltpu.VMEM((1, 3 * width), F32),
            pltpu.VMEM(whole[4].shape, BF16),
            pltpu.VMEM((2, tokens, 512), F32),
            pltpu.SemaphoreType.DMA((5, AG_SEMS)),
            pltpu.SemaphoreType.DMA,
        ],
        compiler_params=pltpu.CompilerParams(collective_id=0, has_side_effects=True, vmem_limit_bytes=VMEM_LIMIT),
        name="forward",
    )(*views, x, c)
    return outs[:4], outs[5:]


PLAN = (
    (4, 0, 0, 0), (5, 1, 0, 0), (5, 0, 0, 1), (6, 1, 0, 1), (7, 0, 0, 2), (8, 1, 0, 2), (8, 2, 0, 0), (8, 0, 0, 3),
    (9, 1, 0, 3), (11, 2, 0, 1), (14, 2, 0, 2), (16, 3, 0, 0), (17, 0, 1, 0), (18, 1, 1, 0), (18, 0, 1, 1), (19, 2, 0, 3),
    (19, 1, 1, 1), (19, 0, 1, 2), (20, 4, 0, 0), (20, 3, 0, 1), (20, 1, 1, 2), (20, 0, 1, 3), (21, 3, 0, 2), (21, 4, 0, 2),
    (21, 1, 1, 3), (22, 2, 1, 0), (24, 4, 0, 1), (24, 3, 0, 3), (24, 4, 0, 3), (27, 2, 1, 1), (28, 0, 2, 0), (30, 2, 1, 2),
    (30, 1, 2, 0), (30, 0, 2, 1), (32, 5, 0, 0), (32, 2, 1, 3), (32, 1, 2, 1), (32, 0, 2, 2), (33, 3, 1, 0), (33, 3, 1, 1),
    (33, 1, 2, 2), (33, 0, 2, 3), (34, 3, 1, 2), (34, 4, 1, 2), (34, 1, 2, 3), (35, 4, 1, 0), (35, 2, 2, 0), (36, 3, 1, 3),
    (37, 4, 1, 1), (37, 2, 2, 1), (37, 4, 1, 3), (37, 0, 3, 0), (38, 2, 2, 2), (38, 1, 3, 0), (38, 0, 3, 1), (38, 0, 3, 2),
    (39, 5, 1, 0), (39, 2, 2, 3), (39, 1, 3, 1), (39, 1, 3, 2), (39, 3, 2, 0), (39, 0, 3, 3), (40, 3, 2, 1), (40, 1, 3, 3),
    (40, 3, 2, 2), (40, 4, 2, 2), (41, 4, 2, 0), (41, 2, 3, 0), (42, 4, 2, 1), (42, 3, 2, 3), (42, 2, 3, 1), (43, 4, 2, 3),
    (43, 2, 3, 2), (43, 2, 3, 3), (43, 3, 3, 0), (44, 3, 3, 1), (44, 3, 3, 2), (44, 4, 3, 2), (44, 3, 3, 3), (45, 5, 2, 0),
    (45, 4, 3, 0), (45, 4, 3, 1), (47, 4, 3, 3), (49, 5, 3, 0), (57, 0, 4, 0), (57, 0, 4, 1), (58, 1, 4, 0), (58, 1, 4, 1),
    (58, 0, 4, 2), (58, 0, 4, 3), (59, 1, 4, 2), (59, 1, 4, 3), (59, 2, 4, 0), (59, 0, 5, 0), (59, 0, 5, 1), (60, 2, 4, 1),
    (60, 1, 5, 0), (60, 1, 5, 1), (60, 2, 4, 2), (60, 0, 5, 2), (60, 0, 5, 3), (60, 0, 6, 0), (60, 0, 6, 1), (61, 3, 4, 0),
    (61, 2, 4, 3), (61, 1, 5, 2), (61, 3, 4, 1), (61, 1, 5, 3), (61, 1, 6, 0), (61, 1, 6, 1), (61, 2, 5, 0), (61, 0, 6, 2),
    (61, 0, 6, 3), (62, 4, 4, 0), (62, 3, 4, 2), (62, 4, 4, 1), (62, 4, 4, 2), (62, 3, 4, 3), (62, 2, 5, 1), (62, 1, 6, 2),
    (62, 1, 6, 3), (63, 4, 4, 3), (63, 2, 5, 2), (63, 2, 5, 3), (64, 2, 6, 0), (65, 5, 4, 0), (65, 3, 5, 0), (65, 2, 6, 1),
    (66, 3, 5, 1), (67, 2, 6, 2), (68, 4, 5, 0), (68, 2, 6, 3), (69, 4, 5, 1), (69, 3, 5, 2), (69, 4, 5, 2), (69, 3, 5, 3),
    (70, 3, 6, 0), (71, 4, 5, 3), (71, 3, 6, 1), (71, 3, 6, 2), (71, 4, 6, 2), (72, 3, 6, 3), (73, 5, 5, 0), (73, 4, 6, 0),
    (73, 0, 7, 0), (73, 4, 6, 1), (73, 0, 7, 1), (74, 1, 7, 0), (74, 1, 7, 1), (74, 0, 7, 2), (74, 0, 7, 3), (75, 4, 6, 3),
    (75, 2, 7, 0), (75, 2, 7, 1), (75, 1, 7, 2), (75, 1, 7, 3), (76, 3, 7, 0), (76, 3, 7, 1), (76, 2, 7, 2), (76, 2, 7, 3),
    (76, 5, 6, 0), (77, 4, 7, 0), (77, 4, 7, 1), (77, 3, 7, 2), (77, 4, 7, 2), (77, 3, 7, 3), (78, 4, 7, 3), (79, 5, 7, 0),
)

PRE, S0, S1, S2, S3, S4 = range(6)
STAGES = ("fetch", "stage0", "stage1", "stage2", "stage3", "stage4")


def column_sum(ref, at, value):
    ref[at] = ref[at] + jnp.sum(value, 0, keepdims=True)


def backward_kernel(length, plan, n_up_parts, *refs):
    (w_qkv, w_out, w_up, w_down), refs = refs[:4], refs[4:]
    x, c, n1, merged, logsum, attended, middle, n2, act, slope, g_down, small, refs = refs[:12] + (refs[12:],)
    output, input_grad, f_qkv, f_out, f_up, f_down, f_vec, g_qkv, g_out, g_up, mid_grad, ag, back, refs = refs[:13] + (
        refs[13:],
    )
    landing, refs = refs[:8], refs[8:]
    sets, refs = refs[: 8 * 7], refs[8 * 7 :]
    tmps, refs = refs[:8], refs[8:]
    (g_vec, narrow, wide, left, right, acc, branch, dk_acc, dv_acc, sems, csem) = refs
    tokens, width = x.shape
    hidden = act.shape[1]
    tile = 512
    pairs = width // 128
    p = Place()
    greet(p)
    sets = [sets[7 * i : 7 * i + 7] for i in range(8)]
    half = hidden // n_up_parts
    entries = [
        (g_down, f_down),
        (g_up.at[0], f_up.at[:, :, :, pl.ds(0, half)]),
        (g_up.at[1], f_up.at[:, :, :, pl.ds(half, half)]),
        (g_out, f_out),
        (g_qkv.at[0], f_qkv.at[:, :, :, pl.ds(0, width)]),
        (g_qkv.at[1], f_qkv.at[:, :, :, pl.ds(width, width)]),
        (g_qkv.at[2], f_qkv.at[:, :, :, pl.ds(2 * width, width)]),
        (g_vec, f_vec),
    ]
    rs = [Scatter(p, g, f, landing[k], sets[k], tmps[k], sems.at[k]) for k, (g, f) in enumerate(entries)]

    def turn(slot, first, count):
        table = {}
        for at, stage, k, i in plan:
            if first <= at < first + count:
                table.setdefault(at, []).append(lambda stage=stage, k=k, i=i: getattr(rs[k], STAGES[stage])(i))
        hook(slot, table)

    loads = [
        pltpu.make_async_copy(c, left, csem.at[0]),
        pltpu.make_async_copy(n2, right, csem.at[1]),
    ]
    for load in loads:
        load.start()
    rs[0].start()
    narrow[...] = jnp.zeros_like(narrow)
    wide[...] = jnp.zeros_like(wide)
    g_vec[...] = jnp.zeros_like(g_vec)
    acc[...] = jnp.zeros_like(acc)
    for load in loads:
        load.wait()

    n_up = hidden // tile

    def ffn_body(wd, s, wu, g):
        j = pl.program_id(0)

        @pl.when(j == n_up // 2 + 1)
        def _():
            rs[1].start()

        turn(3 * j, 0, 3 * n_up)
        grad = (dot(left[...], rows_of(wd), NT) * s[...].astype(F32)).astype(BF16)
        at = pl.ds(pl.multiple_of(j * tile, tile), tile)
        wide[:, at] = jnp.sum(grad.astype(F32), 0, keepdims=True)
        turn(3 * j + 1, 0, 3 * n_up)
        g[0] = dot(right[...], grad, TN).astype(BF16).reshape(g.shape[1:])
        turn(3 * j + 2, 0, 3 * n_up)
        acc[...] += dot(grad, rows_of(wu), NT)

    per = n_up // n_up_parts
    q_down = w_down.shape[2]
    blocks = tile // (2 * q_down)
    shape = g_up.shape[1:7]
    pltpu.emit_pipeline(
        ffn_body,
        grid=(n_up,),
        in_specs=[
            pl.BlockSpec((blocks, 2, q_down, width), lambda j: (j, 0, 0, 0)),
            pl.BlockSpec((tokens, tile), lambda j: (0, j)),
            whole_spec(w_up, tile),
        ],
        out_specs=[pl.BlockSpec((1,) + shape + (tile,), lambda j: (j // per, 0, 0, 0, 0, 0, 0, j % per))],
    )(w_down, slope, w_up, g_up)
    rs[2].start()
    load = pltpu.make_async_copy(n1, right, csem.at[1])
    load.start()
    base = 3 * n_up

    step = 128
    n_rows = tokens // step

    def norm_two_body(m, o):
        i = pl.program_id(0)
        turn(base + i, base, n_rows)
        rows = pl.ds(pl.multiple_of(i * step, step), step)
        upstream = left[rows, :].astype(F32)
        part, gain, shift = norm_back(m[...], small[6:7], acc[rows, :])
        total = upstream + part
        o[...] = total
        low = total.astype(BF16)
        branch[rows, :] = low
        narrow[2:3] += jnp.sum(low.astype(F32), 0, keepdims=True)
        narrow[3:4] += jnp.sum(upstream, 0, keepdims=True)
        narrow[6:7] += gain[None]
        narrow[7:8] += shift[None]

    row_spec = pl.BlockSpec((step, width), lambda i: (i, 0))
    pltpu.emit_pipeline(norm_two_body, grid=(n_rows,), in_specs=[row_spec], out_specs=[row_spec])(middle, mid_grad)
    base += n_rows

    n_out = width // 256
    first_out = base

    def out_body(a, w, g, o):
        i = pl.program_id(0)
        turn(first_out + i, first_out, n_out)
        g[...] = dot(a[...], branch[...], TN).astype(BF16).reshape(g.shape)
        rows = pl.ds(pl.multiple_of(i * 256, 256), 256)
        o[...] = dot(branch[rows, :], rows_of(w), NT).astype(BF16)

    q = g_out.shape[5]
    levels = 256 // (16 * q)
    assert levels == 1
    pltpu.emit_pipeline(
        out_body,
        grid=(n_out,),
        in_specs=[pl.BlockSpec((tokens, 256), lambda i: (0, i)), whole_spec(w_out)],
        out_specs=[
            pl.BlockSpec((1, 2, 2, 2, 2, q, width), lambda i: (i, 0, 0, 0, 0, 0, 0)),
            pl.BlockSpec((256, width), lambda i: (i, 0)),
        ],
    )(attended, w_out, g_out, ag)
    rs[3].start()
    base += n_out

    first_attend = base
    n_attend = (tokens // length) * pairs

    def attend_body(q, k, v, g, l, d):
        s, h = pl.program_id(0), pl.program_id(1)
        turn(first_attend + s * pairs + h, first_attend, n_attend)
        bwd_body(q, k, v, g, l.at[0, 0], d.at[0], d.at[1], d.at[2], dk_acc, dv_acc, 256)
        at = pl.ds(pl.multiple_of(h * 128, 128), 128)
        narrow[0:1, at] += jnp.sum(d[0].astype(F32), 0, keepdims=True)
        narrow[1:2, at] += jnp.sum(d[2].astype(F32), 0, keepdims=True)

    def head_spec(off):
        return pl.BlockSpec((length, 128), lambda s, h: (s, off + h))

    pltpu.emit_pipeline(
        attend_body,
        grid=(tokens // length, pairs),
        in_specs=[head_spec(0), head_spec(pairs), head_spec(2 * pairs), head_spec(0)]
        + [pl.BlockSpec((1, 1, 2, length), lambda s, h: (s, h, 0, 0))],
        out_specs=[pl.BlockSpec((3, length, 128), lambda s, h: (0, s, h))],
    )(merged, merged, merged, ag, logsum, back)
    base += n_attend
    load.wait()

    first_qkv = base
    n_qkv = 3 * width // tile
    per_part = width // tile

    def grad_body(d, g):
        j = pl.program_id(0)
        for k in (1, 2):

            @pl.when(j == k * per_part + 1)
            def _(k=k):
                rs[3 + k].start()

        turn(first_qkv + j, first_qkv, n_qkv)
        g[0] = dot(right[...], d[0], TN).astype(BF16).reshape(g.shape[1:])

    shape = g_qkv.shape[1:7]
    back_spec = pl.BlockSpec((1, tokens, tile), lambda j: (j // per_part, 0, j % per_part))
    pltpu.emit_pipeline(
        grad_body,
        grid=(n_qkv,),
        in_specs=[back_spec],
        out_specs=[
            pl.BlockSpec((1,) + shape + (tile,), lambda j: (j // per_part, 0, 0, 0, 0, 0, 0, j % per_part))
        ],
    )(back, g_qkv)
    rs[6].start()
    base += n_qkv
    first_in = base
    acc[...] = jnp.zeros_like(acc)

    def in_body(d, w):
        j = pl.program_id(0)
        turn(first_in + j, first_in, n_qkv)
        acc[...] += dot(d[0], rows_of(w), NT)

    pltpu.emit_pipeline(in_body, grid=(n_qkv,), in_specs=[back_spec, whole_spec(w_qkv, tile)])(back, w_qkv)
    base += n_qkv

    first_one = base

    def norm_one_body(v, m, o):
        i = pl.program_id(0)
        turn(first_one + i, first_one, n_rows)
        rows = pl.ds(pl.multiple_of(i * step, step), step)
        part, gain, shift = norm_back(v[...].astype(F32), small[4:5], acc[rows, :])
        o[...] = m[...] + part
        narrow[4:5] += gain[None]
        narrow[5:6] += shift[None]

    pltpu.emit_pipeline(norm_one_body, grid=(n_rows,), in_specs=[row_spec] * 2, out_specs=[row_spec])(
        x, mid_grad, input_grad
    )
    base += n_rows
    for k in range(16):
        z, y, xx = k // 4, (k // 2) % 2, k % 2
        g_vec[z, y, xx, 0, 0] = narrow[:, 128 * (k // 2) : 128 * (k // 2) + 128]
        for i in range(2):
            g_vec[z, y, xx, 0, 1, i : i + 1] = wide[:, 256 * k + 128 * i : 256 * k + 128 * i + 128]
    rs[7].start()
    acc[...] = jnp.zeros_like(acc)

    first_down = base

    def down_body(a, w):
        j = pl.program_id(0)
        turn(first_down + j, first_down, n_up)
        acc[...] += dot(a[...], rows_of(w))

    pltpu.emit_pipeline(
        down_body,
        grid=(n_up,),
        in_specs=[
            pl.BlockSpec((tokens, tile), lambda j: (0, j)),
            pl.BlockSpec((blocks, 2, q_down, width), lambda j: (j, 0, 0, 0)),
        ],
    )(act, w_down)
    base += n_up
    first_last = base

    def last_body(m, o):
        i = pl.program_id(0)
        turn(first_last + i, first_last, n_rows)
        rows = pl.ds(pl.multiple_of(i * step, step), step)
        o[...] = (m[...] + (acc[rows, :] + small[3:4])).astype(BF16)

    pltpu.emit_pipeline(last_body, grid=(n_rows,), in_specs=[row_spec], out_specs=[row_spec])(middle, output)
    base += n_rows
    for at, stage, k, i in plan:
        if at >= base:
            getattr(rs[k], STAGES[stage])(i)
    for r in rs:
        r.finish()


def backward_call(weights, x, c, kept, length):
    n1, merged, logsum, attended, middle, n2, act, slope, g_down, small = kept
    tokens, width = x.shape
    hidden = act.shape[1]
    q, q_down = width // 64, hidden // 64
    parts = 2
    low = lambda *shape: jax.ShapeDtypeStruct(shape, BF16)
    full = lambda *shape: jax.ShapeDtypeStruct(shape, F32)
    vmem, any_space = pl.BlockSpec(memory_space=pltpu.VMEM), pl.BlockSpec(memory_space=pl.ANY)
    kinds = [(q_down, width, BF16)] + [(q, hidden // parts, BF16)] * 2 + [(q, width, BF16)] * 4 + [(8, 128, F32)]
    scratch = []
    for kind in kinds:
        scratch += Scatter.scratch(*kind)
    scratch += [pltpu.VMEM((2, 2, 2, 2) + kind[:2], kind[2]) for kind in kinds]
    scratch += [
        pltpu.VMEM((4, 2, 2, 2, 2, 8, 128), F32),
        pltpu.VMEM((8, width), F32),
        pltpu.VMEM((1, hidden), F32),
        pltpu.VMEM((tokens, width), BF16),
        pltpu.VMEM((tokens, width), BF16),
        pltpu.VMEM((tokens, width), F32),
        pltpu.VMEM((tokens, width), BF16),
        pltpu.VMEM((length, 128), F32),
        pltpu.VMEM((length, 128), F32),
        pltpu.SemaphoreType.DMA((8, RS_SEMS)),
        pltpu.SemaphoreType.DMA((2,)),
    ]
    shards = [full(2, 2, q, 3 * width), full(2, 2, q, width), full(2, 2, q, hidden), full(2, 2, q_down, width)]
    outs = pl.pallas_call(
        lambda *refs: backward_kernel(length, PLAN, parts, *refs),
        in_specs=[any_space] * 15 + [vmem],
        out_specs=[any_space] * 2 + [vmem] * 5 + [any_space] * 14,
        out_shape=[low(tokens, width), full(tokens, width)]
        + shards
        + [full(2, 2, 8, 128)]
        + [
            low(3, 4, 2, 2, 2, 2, q, width),
            low(4, 2, 2, 2, 2, q, width),
            low(parts, 4, 2, 2, 2, 2, q, hidden // parts),
            full(tokens, width),
            low(tokens, width),
            low(3, tokens, width),
        ]
        + [jax.ShapeDtypeStruct((4, 2, 2, 2) + kind[:2], kind[2]) for kind in kinds],
        scratch_shapes=scratch,
        compiler_params=pltpu.CompilerParams(
            collective_id=1, has_side_effects=True, vmem_limit_bytes=66 * 10**6
        ),
        name="backward",
    )(*weights, x, c, n1, merged, logsum, attended, middle, n2, act, slope, g_down.reshape(4, 2, 2, 2, 2, q_down, width), small)
    grads = [o.reshape(-1, o.shape[-1]) for o in outs[2:6]]
    return outs[0], outs[1], grads, outs[6].reshape(32, 128)


def forward_plain(x, weights, small, length):
    w_qkv, w_out, w_up, w_down = weights
    b_query, b_value, b_out, b_up, b_down, gain_one, shift_one, gain_two, shift_two = small
    xf = x.astype(F32)
    normed_one = layer_norm(xf, gain_one, shift_one).astype(BF16)
    qkv_bias = jnp.concatenate([b_query, jnp.zeros_like(b_query), b_value])
    merged = (dot(normed_one, w_qkv) + qkv_bias).astype(BF16)
    attended, logsum = attn_fwd(merged, length)
    middle = xf + (dot(attended, w_out) + b_out)
    normed_two = layer_norm(middle, gain_two, shift_two).astype(BF16)
    activated, slope = gelu_pair(dot(normed_two, w_up) + b_up)
    return normed_one, merged, logsum, attended, middle, normed_two, activated.astype(BF16), slope.astype(BF16)


def backward(x, c, weights, small, kept, length):
    w_qkv, w_out, w_up, w_down = weights
    b_down, gain_one, gain_two = small
    normed_one, merged, logsum, attended, middle, normed_two, activated, slope = kept
    width = x.shape[1]
    xf, cf = x.astype(F32), c.astype(F32)
    output = (middle + (dot(activated, w_down) + b_down)).astype(BF16)

    grad_down_bias = jnp.sum(cf, 0)
    hidden_grad = (dot(c, w_down, NT) * slope.astype(F32)).astype(BF16)
    grad_up_bias = jnp.sum(hidden_grad.astype(F32), 0)
    grad_up = dot(normed_two, hidden_grad, TN).astype(BF16)
    part, grad_gain_two, grad_shift_two = norm_back(middle, gain_two, dot(hidden_grad, w_up, NT))
    middle_grad = cf + part
    branch_grad = middle_grad.astype(BF16)
    grad_out_bias = jnp.sum(branch_grad.astype(F32), 0)
    grad_out = dot(attended, branch_grad, TN).astype(BF16)
    attended_grad = dot(branch_grad, w_out, NT).astype(BF16)
    back = attn_bwd(merged, attended_grad, logsum, length)
    grad_query_bias = jnp.sum(back[0].astype(F32), 0)
    grad_value_bias = jnp.sum(back[2].astype(F32), 0)
    grad_qkv = jnp.concatenate([dot(normed_one, back[j], TN).astype(BF16) for j in range(3)], 1)
    normed_one_grad = sum(dot(back[j], w_qkv[:, j * width : (j + 1) * width], NT) for j in range(3))
    part, grad_gain_one, grad_shift_one = norm_back(xf, gain_one, normed_one_grad)
    input_grad = middle_grad + part
    return (
        output,
        input_grad,
        (grad_qkv, grad_out, grad_up),
        (
            grad_query_bias,
            grad_value_bias,
            grad_out_bias,
            grad_up_bias,
            grad_down_bias,
            grad_gain_one,
            grad_shift_one,
            grad_gain_two,
            grad_shift_two,
        ),
    )


def pack_shards(vectors):
    wide = vectors[3]
    narrow = jnp.stack([v for k, v in enumerate(vectors) if k != 3])
    zeros = jnp.zeros_like(narrow)
    odd = lax.axis_index("fsdp") % 2 == 1
    lanes = jnp.concatenate([jnp.where(odd, zeros, narrow), jnp.where(odd, narrow, zeros)], 1)
    rows = jnp.concatenate([lanes, wide.reshape(2, 128)], 0)
    return jnp.pad(rows, ((0, 64 - rows.shape[0]), (0, 0)))


def unpack_shard(packed):
    odd = lax.axis_index("fsdp") % 2 == 1
    narrow = jnp.where(odd, packed[:8, 64:], packed[:8, :64])
    wide = packed[8:10].reshape(256)
    return tuple(narrow[j] for j in range(3)) + (wide,) + tuple(narrow[j] for j in range(3, 8))


def local_ring(block_input, *rest):
    shards, cotangent = rest[:13], rest[13]
    length, width = block_input.shape[1:]
    x, c = block_input.reshape(-1, width), cotangent.reshape(-1, width)
    weights, kept = forward_call(shards[:4] + (pack_shards(shards[4:]),), x, c, length)
    output, input_grad, grads, vec = backward_call(weights, x, c, kept, length)
    whole = (output.reshape(block_input.shape), input_grad.reshape(block_input.shape))
    return whole + tuple(grads) + unpack_shard(vec)


def local_any(block_input, *rest):
    shards, cotangent = rest[:13], rest[13]
    length, width = block_input.shape[1:]
    x, c = block_input.reshape(-1, width), cotangent.reshape(-1, width)
    gathered = [lax.all_gather(shard, "fsdp", axis=0, tiled=True) for shard in shards]
    weights, small = gathered[:4], tuple(v.astype(F32) for v in gathered[4:])
    kept = forward_plain(x, weights, small, length)
    output, input_grad, mats, vecs = backward(x, c, weights, (small[4], small[5], small[7]), kept, length)
    mats += (dot(kept[6], c, TN),)

    def reduce(grad):
        part = lax.psum_scatter(grad.astype(F32), "fsdp", scatter_dimension=0, tiled=True)
        return lax.psum(part, "seq")

    whole = (output.reshape(block_input.shape), input_grad.reshape(block_input.shape))
    return whole + tuple(reduce(grad) for grad in mats + vecs)


def solution(mesh):
    split = P(("fsdp", "seq"), None, None)
    matrix, vector = P("fsdp", None), P("fsdp")
    in_specs = (split,) + (matrix,) * 4 + (vector,) * 9 + (split,)
    out_specs = (split, split) + (matrix,) * 4 + (vector,) * 9
    local = local_ring if (mesh.shape["fsdp"], mesh.shape["seq"]) == (16, 2) else local_any
    return jax.shard_map(local, mesh=mesh, in_specs=in_specs, out_specs=out_specs, check_vma=False)
```

```python
import jax
import jax.numpy as jnp
from jax import lax
from jax.experimental import pallas as pl
from jax.experimental.pallas import tpu as pltpu
from jax.sharding import PartitionSpec as P

EPSILON = 1e-05
NEG_LARGE = -1e30
MESH = pl.DeviceIdType.MESH
NN = (((1,), (0,)), ((), ()))
NT = (((1,), (1,)), ((), ()))
TN = (((0,), (0,)), ((), ()))
BF16 = jnp.bfloat16
F32 = jnp.float32
VMEM_LIMIT = 60 * 2**20


def dot(left, right, dims=NN):
    return lax.dot_general(left, right, dims, preferred_element_type=F32)


class Place:
    def __init__(self):
        f = lax.axis_index("fsdp")
        self.c = lax.axis_index("seq")
        self.z, self.y, self.x = f // 4, (f // 2) % 2, f % 2

    def block(self, z, y, x):
        return z * 4 + y * 2 + x

    def dev(self, z, y, x):
        return (self.block(z, y, x), self.c)

    @property
    def xn(self):
        return self.dev(self.z, self.y, 1 - self.x)

    @property
    def yn(self):
        return self.dev(self.z, 1 - self.y, self.x)

    @property
    def up(self):
        return self.dev(self.z + 1, self.y, self.x)

    @property
    def down(self):
        return self.dev(self.z - 1, self.y, self.x)

    @property
    def partner(self):
        return (self.block(self.z, self.y, self.x), 1 - self.c)


def greet(p):
    barrier = pltpu.get_barrier_semaphore()

    def signal(device):
        pl.semaphore_signal(barrier, inc=1, device_id=device, device_id_type=MESH)

    for device in (p.xn, p.yn, p.partner):
        signal(device)

    @pl.when(p.z < 3)
    def _():
        signal(p.up)

    @pl.when(p.z > 0)
    def _():
        signal(p.down)

    inner = jnp.logical_and(p.z > 0, p.z < 3)

    @pl.when(inner)
    def _():
        pl.semaphore_wait(barrier, 5)

    @pl.when(jnp.logical_not(inner))
    def _():
        pl.semaphore_wait(barrier, 4)


def remote(src, dst, send, recv, device):
    return pltpu.make_async_remote_copy(
        src_ref=src, dst_ref=dst, send_sem=send, recv_sem=recv, device_id=device, device_id_type=MESH
    )


def wait_bytes(ref, sem):
    pltpu.make_async_copy(ref, ref, sem).wait()


AG_SEMS = 24


class Gather:
    def __init__(self, p, src, dst, sems):
        self.p, self.src, self.dst, self.sems = p, src, dst, sems
        self.rz = [None] * 4
        self.send, self.zsend, self.local, self.rp = (sems.at[20], sems.at[21], sems.at[22], sems.at[23])

    def half(self, z, y, x):
        return self.dst.at[2 * self.p.block(z, y, x) + self.p.c]

    def to(self, src, dst, recv, device, send=None):
        remote(src, dst, self.send if send is None else send, self.sems.at[recv], device).start()

    def spread(self, src, z):
        p = self.p
        mine = self.half(z, p.y, p.x)
        self.to(src, mine, 4 + z, p.xn)
        self.to(src, mine, 8 + z, p.yn)

    def along(self, src, z, up):
        p = self.p
        mine = self.half(z, p.y, p.x)

        @pl.when(p.z < 3 if up else p.z > 0)
        def _():
            self.to(src, mine, z, p.up if up else p.down, self.zsend)

    def start(self):
        p = self.p
        own = self.src.at[p.c]
        self.along(own, p.z, True)
        self.along(own, p.z, False)
        me = p.block(p.z, p.y, p.x)
        pltpu.make_async_copy(self.src, self.dst.at[pl.ds(2 * me, 2)], self.local).start()

    def at_distance(self, s, body):
        p = self.p
        if s == 0:
            body(p.z, None)
            return

        @pl.when(p.z - s >= 0)
        def _():
            body(p.z - s, True)

        @pl.when(p.z + s <= 3)
        def _():
            body(p.z + s, False)

    def z_step(self, s):
        p = self.p
        if s == 0:
            self.start()
            return

        def body(z, up):
            mine = self.half(z, p.y, p.x)
            wait_bytes(mine, self.sems.at[z])
            self.along(mine, z, up)
            self.to(mine, mine, 23, p.partner)

        self.at_distance(s, body)

    def spread_step(self, s):
        p = self.p

        def body(z, up):
            self.spread(self.src.at[p.c] if s == 0 else self.half(z, p.y, p.x), z)

        self.at_distance(s, body)

    def xy_step(self, s):
        p = self.p

        def body(z, up):
            a = self.half(z, p.y, 1 - p.x)
            wait_bytes(a, self.sems.at[4 + z])
            self.to(a.at[0], a.at[0], 12 + z, p.yn)
            self.to(a, a, 23, p.partner)
            b = self.half(z, 1 - p.y, p.x)
            wait_bytes(b, self.sems.at[8 + z])
            self.to(b.at[1], b.at[1], 16 + z, p.xn)
            self.to(b, b, 23, p.partner)

        self.at_distance(s, body)

    def diag_step(self, s):
        p = self.p

        def body(z, up):
            d = self.half(z, 1 - p.y, 1 - p.x)
            wait_bytes(d.at[0], self.sems.at[12 + z])
            wait_bytes(d.at[1], self.sems.at[16 + z])
            self.to(d, d, 23, p.partner)

        self.at_distance(s, body)

    def arrived(self):
        wait_bytes(self.dst.at[pl.ds(0, 15)], self.rp)
        wait_bytes(self.dst.at[pl.ds(0, 2)], self.local)

    def drain(self):
        p = self.p
        wait_bytes(self.dst.at[pl.ds(0, 27)], self.send)
        inner = jnp.logical_and(p.z > 0, p.z < 3)

        @pl.when(inner)
        def _():
            wait_bytes(self.dst.at[pl.ds(0, 5)], self.zsend)

        @pl.when(jnp.logical_not(inner))
        def _():
            wait_bytes(self.dst.at[pl.ds(0, 1)], self.zsend)


GATHER_STAGES = ("z_step", "spread_step", "xy_step", "diag_step")


def hook(index, table):
    for k, steps in table.items():

        @pl.when(index == k)
        def _(steps=steps):
            for step in steps:
                step()


RS_SEMS = 44


class Scatter:
    def __init__(self, p, g, out, pr, bufs, tmp, sems):
        self.p, self.g, self.out, self.pr, self.tmp, self.sems = p, g, out, pr, tmp, sems
        self.o, self.x1, self.y1, self.x2, self.y2, self.u, self.d = bufs
        self.psend, self.zsend, self.fsend, self.frecv = (sems.at[36 + i] for i in range(4))

    @staticmethod
    def scratch(q, width, dtype):
        shapes = [(4, 2, 2, 2), (4, 2), (4, 2), (4,), (4,), (4, 2), (4, 2)]
        return [pltpu.VMEM(shape + (q, width), dtype) for shape in shapes]

    def level(self, i):
        z = self.p.z
        return jnp.where(z < 2, 3 - i, i)

    def sem(self, kind, i):
        return self.sems.at[4 * kind + i]

    def start(self):
        p = self.p
        for i in range(4):
            z = self.level(i)
            theirs = self.g.at[z, :, :, 1 - p.c]
            remote(theirs, self.pr.at[z], self.psend, self.sem(0, i), p.partner).start()
            pltpu.make_async_copy(self.g.at[z, :, :, p.c], self.o.at[z], self.sem(1, i)).start()

    def fetch(self, i):
        z = self.level(i)
        wait_bytes(self.pr.at[z], self.sem(0, i))
        pltpu.make_async_copy(self.pr.at[z], self.tmp.at[i % 2], self.sems.at[40 + i]).start()

    def stage0(self, i):
        p = self.p
        z = self.level(i)
        wait_bytes(self.o.at[z], self.sem(1, i))
        wait_bytes(self.tmp.at[i % 2], self.sems.at[40 + i])

        def add(j, carry):
            y, x, k = j // 4, (j // 2) % 2, j % 2
            self.o[z, y, x, k] = self.o[z, y, x, k] + self.tmp[i % 2, y, x, k]
            return carry

        lax.fori_loop(0, 8, add, 0)
        remote(self.o.at[z, :, 1 - p.x, 0], self.x1.at[z], self.sems.at[32], self.sem(2, i), p.xn).start()
        remote(self.o.at[z, 1 - p.y, :, 1], self.y1.at[z], self.sems.at[33], self.sem(3, i), p.yn).start()

    def stage1(self, i):
        p = self.p
        z = self.level(i)
        wait_bytes(self.x1.at[z], self.sem(2, i))
        for y in range(2):
            self.o[z, y, p.x, 0] = self.o[z, y, p.x, 0] + self.x1[z, y]
        remote(self.o.at[z, 1 - p.y, p.x, 0], self.y2.at[z], self.sems.at[35], self.sem(4, i), p.yn).start()
        wait_bytes(self.y1.at[z], self.sem(3, i))
        for x in range(2):
            self.o[z, p.y, x, 1] = self.o[z, p.y, x, 1] + self.y1[z, x]
        remote(self.o.at[z, p.y, 1 - p.x, 1], self.x2.at[z], self.sems.at[34], self.sem(5, i), p.xn).start()

    def along(self, z, up):
        p = self.p
        buf, kind = (self.u, 6) if up else (self.d, 7)
        remote(
            self.o.at[z, p.y, p.x], buf.at[z], self.zsend, self.sems.at[4 * kind + z], p.up if up else p.down
        ).start()

    def chain(self, z, up):
        p = self.p
        buf, kind = (self.u, 6) if up else (self.d, 7)
        wait_bytes(buf.at[z], self.sems.at[4 * kind + z])
        self.o[z, p.y, p.x] = self.o[z, p.y, p.x] + buf[z]
        self.along(z, up)

    def stage2(self, i):
        p = self.p
        z = self.level(i)
        wait_bytes(self.y2.at[z], self.sem(4, i))
        wait_bytes(self.x2.at[z], self.sem(5, i))
        self.o[z, p.y, p.x, 0] = self.o[z, p.y, p.x, 0] + self.y2[z]
        self.o[z, p.y, p.x, 1] = self.o[z, p.y, p.x, 1] + self.x2[z]

        @pl.when(jnp.logical_and(p.z == 0, z > 0))
        def _():
            self.along(z, True)

        @pl.when(jnp.logical_and(p.z == 3, z < 3))
        def _():
            self.along(z, False)

    def stage3(self, i):
        p = self.p
        z = self.level(i)
        inner = jnp.logical_and(p.z > 0, p.z < 3)

        @pl.when(jnp.logical_and(inner, z > p.z))
        def _():
            self.chain(z, True)

        @pl.when(jnp.logical_and(inner, z < p.z))
        def _():
            self.chain(z, False)

    def stage4(self, i=0):
        p = self.p
        z = p.z
        self.out[p.c] = self.o[z, p.y, p.x].astype(F32)

        @pl.when(z > 0)
        def _():
            wait_bytes(self.u.at[z], self.sems.at[24 + z])
            self.out[p.c] = self.out[p.c] + self.u[z].astype(F32)

        @pl.when(z < 3)
        def _():
            wait_bytes(self.d.at[z], self.sems.at[28 + z])
            self.out[p.c] = self.out[p.c] + self.d[z].astype(F32)

        remote(self.out.at[p.c], self.out.at[p.c], self.fsend, self.frecv, p.partner).start()

    def finish(self):
        p = self.p
        wait_bytes(self.out.at[1 - p.c], self.frecv)
        wait_bytes(self.out.at[p.c], self.fsend)
        wait_bytes(self.o, self.psend)
        for k, ref in enumerate((self.x1, self.y1, self.x2, self.y2)):
            wait_bytes(ref, self.sems.at[32 + k])
        wait_bytes(self.u.at[pl.ds(0, 3)], self.zsend)


def lane_masks(rows, width, dtype=BF16):
    lanes = lax.broadcasted_iota(jnp.int32,(rows,width),1)
    return lanes < width//2
def pick(h, low, v):
    z=jnp.zeros_like(v)
    return jnp.where(low, v, z) if h==0 else jnp.where(low, z, v)
def fwd_body(q_ref,k_ref,v_ref,o_ref,l_ref, B):
    S=q_ref.shape[0]
    low=lane_masks(S,128)
    q=q_ref[...]*BF16(0.125); k=k_ref[...]; v=v_ref[...]
    qs=[pick(h,low,q) for h in (0,1)]; vs=[pick(h,low,v) for h in (0,1)]
    for b in range(S//B):
        end=(b+1)*B
        acc=None
        for h in (0,1):
            st=dot(k[:end],qs[h][b*B:end],NT)
            key=lax.broadcasted_iota(jnp.int32,(B,B),0); qry=lax.broadcasted_iota(jnp.int32,(B,B),1)
            diag=jnp.where(key<=qry, st[b*B:end], NEG_LARGE)
            st=jnp.concatenate([st[:b*B],diag],0) if b else diag
            m=jnp.max(st,0,keepdims=True)
            p=jnp.exp(st-m)
            l=jnp.sum(p,0,keepdims=True)
            l_ref[h:h+1,b*B:end]=m+jnp.log(l)
            pt=(p*(1.0/l)).astype(BF16)
            o=dot(pt,vs[h][:end],TN)
            acc=o if acc is None else acc+o
        o_ref[b*B:end,:]=acc.astype(BF16)
def bwd_body(q_ref,k_ref,v_ref,g_ref,l_ref,dq_ref,dk_ref,dv_ref,dk_acc,dv_acc,B):
    S=q_ref.shape[0]
    low=lane_masks(S,128)
    q=q_ref[...]*BF16(0.125); k=k_ref[...]; v=v_ref[...]; g=g_ref[...]
    qs=[pick(h,low,q) for h in (0,1)]; gs=[pick(h,low,g) for h in (0,1)]; ks=[pick(h,low,k) for h in (0,1)]
    for b in reversed(range(S//B)):
        end=(b+1)*B
        dq=None; dk=None; dv=None
        for h in (0,1):
            qb=qs[h][b*B:end]; gb=gs[h][b*B:end]
            st=dot(k[:end],qb,NT)
            p=jnp.exp(st-l_ref[h:h+1,b*B:end])
            key=lax.broadcasted_iota(jnp.int32,(B,B),0); qry=lax.broadcasted_iota(jnp.int32,(B,B),1)
            diag=jnp.where(key<=qry, p[b*B:end], 0.0)
            p=jnp.concatenate([p[:b*B],diag],0) if b else diag
            dp=dot(v[:end],gb,NT)
            inner=jnp.sum(p*dp,0,keepdims=True)
            ds=(p*(dp-inner)).astype(BF16)
            pb=p.astype(BF16)
            dvh=dot(pb,gb,NN); dkh=dot(ds,qb,NN); dqh=dot(ds,ks[h][:end],TN)
            dq=dqh if dq is None else dq+dqh
            dk=dkh if dk is None else dk+dkh
            dv=dvh if dv is None else dv+dvh
        dq_ref[b*B:end,:]=(dq*0.125).astype(BF16)
        if b==S//B-1:
            dk_acc[...]=dk; dv_acc[...]=dv
        else:
            dk_acc[:end,:]+=dk; dv_acc[:end,:]+=dv
    dk_ref[...]=dk_acc[...].astype(BF16)
    dv_ref[...]=dv_acc[...].astype(BF16)
def attn_fwd(merged, S, B=256):
    T=merged.shape[0]; D=merged.shape[1]//3; n=D//128
    def body(q,k,v,o,l): fwd_body(q,k,v,o,l.at[0,0],B)
    sp=lambda off: pl.BlockSpec((S,128),lambda s,h: (s,off+h))
    return pl.pallas_call(body,grid=(T//S,n),in_specs=[sp(0),sp(n),sp(2*n)],
        out_specs=[pl.BlockSpec((S,128),lambda s,h:(s,h)),pl.BlockSpec((1,1,2,S),lambda s,h:(s,h,0,0))],
        out_shape=[jax.ShapeDtypeStruct((T,D),BF16),jax.ShapeDtypeStruct((T//S,n,2,S),F32)],
        name="attn_fwd",compiler_params=pltpu.CompilerParams(vmem_limit_bytes=40*2**20))(merged,merged,merged)
def attn_bwd(merged, g, lse, S, B=256):
    T=merged.shape[0]; D=merged.shape[1]//3; n=D//128
    def body(q,k,v,gr,l,d,dka,dva): bwd_body(q,k,v,gr,l.at[0,0],d.at[0],d.at[1],d.at[2],dka,dva,B)
    sp=lambda off: pl.BlockSpec((S,128),lambda s,h: (s,off+h))
    return pl.pallas_call(body,grid=(T//S,n),in_specs=[sp(0),sp(n),sp(2*n),sp(0),pl.BlockSpec((1,1,2,S),lambda s,h:(s,h,0,0))],
        out_specs=pl.BlockSpec((3,S,128),lambda s,h:(0,s,h)),
        out_shape=jax.ShapeDtypeStruct((3,T,D),BF16),
        scratch_shapes=[pltpu.VMEM((S,128),F32)]*2,
        name="attn_bwd",compiler_params=pltpu.CompilerParams(vmem_limit_bytes=40*2**20))(merged,merged,merged,g,lse)


def layer_norm(values, gain, shift):
    center = values - jnp.mean(values, -1, keepdims=True)
    spread = jnp.mean(center * center, -1, keepdims=True)
    return center * lax.rsqrt(spread + EPSILON) * gain + shift


def norm_back(values, gain, grad):
    center = values - jnp.mean(values, -1, keepdims=True)
    inverse = lax.rsqrt(jnp.mean(center * center, -1, keepdims=True) + EPSILON)
    unit = center * inverse
    scaled = grad * gain
    first = jnp.mean(scaled, -1, keepdims=True)
    second = jnp.mean(scaled * unit, -1, keepdims=True)
    return (inverse * (scaled - first - unit * second), jnp.sum(grad * unit, 0), jnp.sum(grad, 0))


def gelu_pair(u):
    a = 0.7978845608028654
    square = u * u
    half = 0.5 + 0.5 * jnp.tanh(u * (a + (a * 0.044715) * square))
    value = u * half
    slope = half + value * (1.0 - half) * (2.0 * a + (6.0 * a * 0.044715) * square)
    return value, slope


def whole_spec(ref, tile=None):
    n, two, q, width = ref.shape
    if tile is None:
        return pl.BlockSpec((n, two, q, width), lambda j: (0, 0, 0, 0))
    return pl.BlockSpec((n, two, q, tile), lambda j: (0, 0, 0, j))


def rows_of(block):
    value = block[...]
    return value.reshape(-1, value.shape[-1])


GATHER_PLAN = (
    (0, 0, 0, 0), (0, 0, 1, 0), (0, 1, 0, 0), (0, 1, 1, 0), (0, 0, 0, 1), (0, 0, 2, 0), (0, 2, 0, 0), (0, 1, 2, 0),
    (0, 1, 0, 1), (0, 0, 1, 1), (0, 1, 1, 1), (0, 2, 1, 0), (0, 2, 0, 1), (0, 0, 0, 2), (0, 0, 1, 2), (0, 1, 0, 2),
    (0, 0, 0, 3), (0, 1, 1, 2), (0, 0, 3, 0), (0, 0, 2, 1), (0, 1, 0, 3), (0, 2, 0, 2), (0, 2, 1, 1), (0, 3, 1, 0),
    (0, 0, 1, 3), (0, 1, 1, 3), (0, 3, 0, 1), (0, 2, 0, 3), (0, 2, 1, 2), (0, 3, 0, 2), (0, 2, 1, 3), (0, 2, 2, 0),
    (0, 0, 2, 2), (0, 0, 2, 3), (0, 3, 0, 0), (0, 1, 3, 0), (0, 1, 2, 2), (0, 3, 0, 3), (0, 3, 1, 1), (0, 1, 2, 1),
    (0, 1, 2, 3), (0, 0, 3, 1), (0, 1, 3, 1), (0, 0, 4, 0), (0, 3, 1, 2), (0, 3, 1, 3), (4, 0, 3, 2), (5, 2, 3, 0),
    (5, 2, 2, 2), (9, 2, 2, 1), (9, 0, 4, 1), (10, 3, 2, 0), (10, 1, 3, 2), (10, 0, 3, 3), (11, 1, 3, 3), (15, 2, 2, 3),
    (15, 2, 3, 1), (16, 3, 2, 2), (18, 3, 3, 0), (18, 0, 4, 2), (18, 3, 2, 1), (20, 2, 3, 2), (21, 3, 2, 3), (22, 2, 3, 3),
    (23, 1, 4, 2), (24, 0, 4, 3), (24, 1, 4, 3), (24, 3, 3, 1), (24, 1, 4, 0), (24, 1, 4, 1), (25, 3, 3, 2), (25, 3, 3, 3),
    (29, 2, 4, 2), (33, 2, 4, 0), (33, 2, 4, 3), (36, 2, 4, 1), (38, 3, 4, 0), (40, 3, 4, 3), (41, 3, 4, 1), (41, 3, 4, 2),
)


def forward_kernel(length, plan, *refs):
    (shards, refs) = (refs[:5], refs[5:])
    x, c = refs[:2]
    (wholes, refs) = (refs[2:7], refs[7:])
    n1, merged, logsum, attended, middle, n2, act, slope, grad_down, small, refs = refs[:10] + (refs[10:],)
    b_up, qkv_bias, vec, hidden, x_ref, c_ref, n1_ref, n2_ref, sems, local = refs
    tokens, width = x_ref.shape
    p = Place()
    greet(p)
    order = [4, 0, 1, 2, 3]
    gathers = [Gather(p, shards[i], wholes[i], sems.at[i]) for i in order]
    g_vec, g_qkv, g_out, g_up, g_down = gathers

    def steps(at):
        return [
            lambda stage=stage, w=w, s=s: getattr(gathers[w], GATHER_STAGES[stage])(s)
            for when, stage, w, s in plan
            if when == at
        ]

    def run(at):
        for step in steps(at):
            step()

    def turn(index, first, count, skip=0):
        hook(index, {k: steps(first + k) for k in range(skip, count) if steps(first + k)})

    loads = [pltpu.make_async_copy(x, x_ref, local.at[0]), pltpu.make_async_copy(c, c_ref, local.at[1])]
    for load in loads:
        load.start()
    run(0)
    g_vec.arrived()
    load = pltpu.make_async_copy(wholes[4], vec, local.at[2])
    load.start()
    load.wait()
    for load in loads:
        load.wait()
    for k in range(8):
        small[:, pl.ds(128 * k, 128)] = (vec[4 * k, 0, :8] + vec[4 * k + 2, 0, :8]).astype(F32)
    for k in range(16):
        for i in range(2):
            b_up[:, pl.ds(256 * k + 128 * i, 128)] = vec[2 * k, 0, 8 + i : 9 + i].astype(F32)
    qkv_bias[:, :width] = small[0:1]
    qkv_bias[:, width : 2 * width] = jnp.zeros_like(small[0:1])
    qkv_bias[:, 2 * width :] = small[1:2]

    def norm_rows(i, carry):
        rows = pl.ds(i * 128, 128)
        n1_ref[rows, :] = layer_norm(x_ref[rows, :].astype(F32), small[4:5], small[5:6]).astype(BF16)
        return carry

    lax.fori_loop(0, tokens // 128, norm_rows, 0)
    store_n1 = pltpu.make_async_copy(n1_ref, n1, local.at[0])
    store_n1.start()
    base = 1
    run(base)
    g_qkv.arrived()

    n_qkv, tile = 3 * width // 512, 512
    first_qkv = base

    def qkv_body(w_ref, o_ref):
        j = pl.program_id(0)
        turn(j, first_qkv, n_qkv, 1)
        bias = qkv_bias[:, pl.ds(pl.multiple_of(j * tile, tile), tile)]
        o_ref[...] = (dot(n1_ref[...], rows_of(w_ref)) + bias).astype(BF16)

    pltpu.emit_pipeline(
        qkv_body,
        grid=(n_qkv,),
        in_specs=[whole_spec(wholes[0], tile)],
        out_specs=[pl.BlockSpec((tokens, tile), lambda j: (0, j))],
    )(wholes[0], merged)

    pairs = width // 128
    base += n_qkv
    n_attend = (tokens // length) * pairs
    first_attend = base

    def attend_body(q, k, v, o, l):
        s, h = pl.program_id(0), pl.program_id(1)
        turn(s * pairs + h, first_attend, n_attend)
        fwd_body(q, k, v, o, l.at[0, 0], 256)

    def head_spec(off):
        return pl.BlockSpec((length, 128), lambda s, h: (s, off + h))

    pltpu.emit_pipeline(
        attend_body,
        grid=(tokens // length, pairs),
        in_specs=[head_spec(0), head_spec(pairs), head_spec(2 * pairs)],
        out_specs=[head_spec(0), pl.BlockSpec((1, 1, 2, length), lambda s, h: (s, h, 0, 0))],
    )(merged, merged, merged, attended, logsum)

    base += n_attend
    run(base)
    g_out.arrived()
    n_out, first_out = tokens // 256, base

    def out_body(a_ref, w_ref, m_ref):
        i = pl.program_id(0)
        turn(i, first_out, n_out, 1)
        rows = pl.ds(pl.multiple_of(i * 256, 256), 256)
        value = x_ref[rows, :].astype(F32) + (dot(a_ref[...], rows_of(w_ref)) + small[2:3])
        m_ref[...] = value
        n2_ref[rows, :] = layer_norm(value, small[6:7], small[7:8]).astype(BF16)

    pltpu.emit_pipeline(
        out_body,
        grid=(tokens // 256,),
        in_specs=[pl.BlockSpec((256, width), lambda i: (i, 0)), whole_spec(wholes[1])],
        out_specs=[pl.BlockSpec((256, width), lambda i: (i, 0))],
    )(attended, wholes[1], middle)

    store_n2 = pltpu.make_async_copy(n2_ref, n2, local.at[1])
    store_n2.start()
    base += n_out
    run(base)
    g_up.arrived()
    n_up, first_up = act.shape[1] // tile, base

    def gelu_tile(j, a_ref, s_ref):
        bias = b_up[:, pl.ds(pl.multiple_of(j * tile, tile), tile)]

        value, grad = gelu_pair(hidden[j % 2] + bias)
        a_ref[...] = value.astype(BF16)
        s_ref[...] = grad.astype(BF16)

    def up_body(w_ref, a_ref, s_ref):
        j = pl.program_id(0)
        turn(j, first_up, n_up + 1, 1)

        @pl.when(j == 0)
        def _():
            hidden[0] = dot(n2_ref[...], rows_of(w_ref))

        @pl.when(jnp.logical_and(j > 0, j < n_up))
        def _():
            gelu_tile(j - 1, a_ref, s_ref)
            hidden[j % 2] = dot(n2_ref[...], rows_of(w_ref))

        @pl.when(j == n_up)
        def _():
            gelu_tile(j - 1, a_ref, s_ref)

    n, two, q, _ = wholes[2].shape
    late = pl.BlockSpec((tokens, tile), lambda j: (0, jnp.maximum(j - 1, 0)))
    pltpu.emit_pipeline(
        up_body,
        grid=(n_up + 1,),
        in_specs=[pl.BlockSpec((n, two, q, tile), lambda j: (0, 0, 0, jnp.minimum(j, n_up - 1)))],
        out_specs=[late, late],
    )(wholes[2], act, slope)

    base += n_up + 1
    first_grad = base

    def grad_body(a_ref, o_ref):
        turn(pl.program_id(0), first_grad, n_up)
        o_ref[...] = dot(a_ref[...], c_ref[...], TN).astype(BF16)

    pltpu.emit_pipeline(
        grad_body,
        grid=(n_up,),
        in_specs=[pl.BlockSpec((tokens, tile), lambda j: (0, j))],
        out_specs=[pl.BlockSpec((tile, width), lambda j: (j, 0))],
    )(act, grad_down)
    run(base + n_up)
    g_down.arrived()
    for g in gathers:
        g.drain()
    store_n1.wait()
    store_n2.wait()


def forward_call(shards, x, c, length):
    tokens, width = x.shape
    hidden = 16 * shards[3].shape[0]
    views = [s.reshape(2, 2, s.shape[0] // 4, s.shape[1]) for s in shards]
    whole = [jax.ShapeDtypeStruct((32,) + v.shape[1:], v.dtype) for v in views]
    vmem, any_space = pl.BlockSpec(memory_space=pltpu.VMEM), pl.BlockSpec(memory_space=pl.ANY)
    low = lambda *shape: jax.ShapeDtypeStruct(shape, BF16)
    outs = pl.pallas_call(
        lambda *refs: forward_kernel(length, GATHER_PLAN, *refs),
        in_specs=[vmem] * 5 + [any_space] * 2,
        out_specs=[any_space] * 14 + [vmem],
        out_shape=whole
        + [
            low(tokens, width),
            low(tokens, 3 * width),
            jax.ShapeDtypeStruct((tokens // length, width // 128, 2, length), F32),
            low(tokens, width),
            jax.ShapeDtypeStruct((tokens, width), F32),
            low(tokens, width),
            low(tokens, hidden),
            low(tokens, hidden),
            low(hidden, width),
            jax.ShapeDtypeStruct((8, width), F32),
        ],
        scratch_shapes=[
            pltpu.VMEM((1, hidden), F32),
            pltpu.VMEM((1, 3 * width), F32),
            pltpu.VMEM(whole[4].shape, BF16),
            pltpu.VMEM((2, tokens, 512), F32),
            pltpu.VMEM((tokens, width), BF16),
            pltpu.VMEM((tokens, width), BF16),
            pltpu.VMEM((tokens, width), BF16),
            pltpu.VMEM((tokens, width), BF16),
            pltpu.SemaphoreType.DMA((5, AG_SEMS)),
            pltpu.SemaphoreType.DMA((3,)),
        ],
        compiler_params=pltpu.CompilerParams(collective_id=0, has_side_effects=True, vmem_limit_bytes=VMEM_LIMIT),
        name="forward",
    )(*views, x, c)
    return outs[:4], outs[5:]


PLAN = (
    (5, 0, 0, 0), (7, 1, 0, 0), (7, 0, 0, 1), (9, 1, 0, 1), (9, 0, 0, 2), (11, 1, 0, 2), (11, 0, 0, 3), (12, 2, 0, 0),
    (13, 1, 0, 3), (16, 2, 0, 1), (18, 0, 1, 0), (19, 2, 0, 2), (19, 0, 1, 1), (20, 1, 1, 0), (21, 3, 0, 0), (21, 1, 1, 1),
    (21, 0, 1, 2), (22, 0, 1, 3), (23, 1, 1, 2), (24, 2, 0, 3), (24, 1, 1, 3), (27, 3, 0, 1), (28, 4, 0, 0), (30, 0, 2, 0),
    (30, 3, 0, 2), (30, 4, 0, 2), (32, 0, 2, 1), (33, 2, 1, 0), (33, 1, 2, 0), (33, 1, 2, 1), (33, 0, 2, 2), (34, 4, 0, 1),
    (34, 2, 1, 1), (34, 1, 2, 2), (34, 0, 2, 3), (35, 2, 1, 2), (35, 1, 2, 3), (36, 3, 0, 3), (36, 4, 0, 3), (38, 2, 1, 3),
    (39, 3, 1, 0), (39, 0, 3, 0), (39, 0, 3, 1), (40, 2, 2, 0), (41, 5, 0, 0), (41, 1, 3, 0), (41, 1, 3, 1), (41, 0, 3, 2),
    (41, 0, 3, 3), (42, 4, 1, 0), (42, 3, 1, 1), (42, 2, 2, 1), (43, 1, 3, 2), (43, 1, 3, 3), (44, 2, 2, 2), (45, 3, 1, 2),
    (45, 4, 1, 2), (46, 4, 1, 1), (46, 2, 2, 3), (47, 3, 1, 3), (47, 4, 1, 3), (48, 3, 2, 0), (49, 2, 3, 0), (50, 3, 2, 1),
    (50, 2, 3, 1), (51, 5, 1, 0), (51, 2, 3, 2), (52, 4, 2, 0), (52, 2, 3, 3), (53, 4, 2, 1), (53, 3, 2, 2), (53, 4, 2, 2),
    (53, 3, 2, 3), (54, 3, 3, 0), (54, 3, 3, 1), (54, 3, 3, 2), (54, 4, 3, 2), (55, 4, 2, 3), (55, 3, 3, 3), (57, 4, 3, 0),
    (57, 0, 4, 0), (58, 5, 2, 0), (58, 4, 3, 1), (58, 1, 4, 0), (58, 0, 4, 1), (58, 0, 4, 2), (59, 0, 5, 0), (60, 4, 3, 3),
    (60, 1, 4, 1), (60, 1, 4, 2), (60, 0, 4, 3), (60, 0, 5, 1), (61, 2, 4, 0), (61, 1, 5, 0), (61, 0, 5, 2), (62, 1, 4, 3),
    (62, 1, 5, 1), (62, 0, 5, 3), (62, 0, 6, 0), (62, 0, 6, 1), (63, 5, 3, 0), (63, 2, 4, 1), (63, 2, 4, 2), (63, 1, 5, 2),
    (64, 3, 4, 0), (64, 1, 5, 3), (64, 1, 6, 0), (64, 1, 6, 1), (64, 0, 6, 2), (64, 0, 6, 3), (64, 2, 5, 0), (66, 2, 4, 3),
    (66, 1, 6, 2), (66, 1, 6, 3), (67, 4, 4, 0), (67, 3, 4, 1), (67, 2, 5, 1), (68, 3, 4, 2), (68, 4, 4, 2), (69, 2, 5, 2),
    (70, 2, 5, 3), (71, 4, 4, 1), (71, 2, 6, 0), (72, 2, 6, 1), (73, 3, 4, 3), (73, 4, 4, 3), (73, 3, 5, 0), (74, 2, 6, 2),
    (74, 0, 7, 0), (74, 0, 7, 1), (75, 3, 5, 1), (75, 2, 6, 3), (76, 5, 4, 0), (76, 4, 5, 0), (76, 3, 5, 2), (76, 4, 5, 2),
    (76, 3, 5, 3), (76, 1, 7, 0), (76, 3, 6, 0), (76, 1, 7, 1), (76, 0, 7, 2), (76, 0, 7, 3), (77, 3, 6, 1), (77, 3, 6, 2),
    (77, 4, 6, 2), (78, 4, 5, 1), (78, 3, 6, 3), (78, 2, 7, 0), (78, 2, 7, 1), (78, 1, 7, 2), (78, 1, 7, 3), (79, 4, 5, 3),
    (80, 4, 6, 0), (80, 3, 7, 0), (80, 3, 7, 1), (80, 2, 7, 2), (80, 2, 7, 3), (81, 4, 6, 1), (83, 5, 5, 0), (83, 4, 7, 0),
    (83, 4, 7, 1), (83, 3, 7, 2), (83, 4, 7, 2), (83, 3, 7, 3), (84, 4, 6, 3), (86, 4, 7, 3), (88, 5, 6, 0), (88, 5, 7, 0),
)

PRE, S0, S1, S2, S3, S4 = range(6)
STAGES = ("fetch", "stage0", "stage1", "stage2", "stage3", "stage4")


def column_sum(ref, at, value):
    ref[at] = ref[at] + jnp.sum(value, 0, keepdims=True)


def backward_kernel(length, plan, n_up_parts, *refs):
    (w_qkv, w_out, w_up, w_down), refs = refs[:4], refs[4:]
    x, c, n1, merged, logsum, attended, middle, n2, act, slope, g_down, small, refs = refs[:12] + (refs[12:],)
    output, input_grad, f_qkv, f_out, f_up, f_down, f_vec, g_qkv, g_out, g_up, mid_grad, ag, back, refs = refs[:13] + (
        refs[13:],
    )
    landing, refs = refs[:8], refs[8:]
    sets, refs = refs[: 8 * 7], refs[8 * 7 :]
    tmps, refs = refs[:8], refs[8:]
    (g_vec, narrow, wide, left, right, acc, branch, dk_acc, dv_acc, sems, csem) = refs
    tokens, width = x.shape
    hidden = act.shape[1]
    tile = 512
    pairs = width // 128
    p = Place()
    greet(p)
    sets = [sets[7 * i : 7 * i + 7] for i in range(8)]
    half = hidden // n_up_parts
    entries = [
        (g_down, f_down),
        (g_up.at[0], f_up.at[:, :, :, pl.ds(0, half)]),
        (g_up.at[1], f_up.at[:, :, :, pl.ds(half, half)]),
        (g_out, f_out),
        (g_qkv.at[0], f_qkv.at[:, :, :, pl.ds(0, width)]),
        (g_qkv.at[1], f_qkv.at[:, :, :, pl.ds(width, width)]),
        (g_qkv.at[2], f_qkv.at[:, :, :, pl.ds(2 * width, width)]),
        (g_vec, f_vec),
    ]
    rs = [Scatter(p, g, f, landing[k], sets[k], tmps[k], sems.at[k]) for k, (g, f) in enumerate(entries)]

    def turn(slot, first, count):
        table = {}
        for at, stage, k, i in plan:
            if first <= at < first + count:
                table.setdefault(at, []).append(lambda stage=stage, k=k, i=i: getattr(rs[k], STAGES[stage])(i))
        hook(slot, table)

    loads = [
        pltpu.make_async_copy(c, left, csem.at[0]),
        pltpu.make_async_copy(n2, right, csem.at[1]),
    ]
    for load in loads:
        load.start()
    rs[0].start()
    narrow[...] = jnp.zeros_like(narrow)
    wide[...] = jnp.zeros_like(wide)
    g_vec[...] = jnp.zeros_like(g_vec)
    acc[...] = jnp.zeros_like(acc)
    for load in loads:
        load.wait()

    n_up = hidden // tile

    def ffn_body(wd, s, wu, g):
        j = pl.program_id(0)

        @pl.when(j == n_up // 2 + 1)
        def _():
            rs[1].start()

        turn(3 * j, 0, 3 * n_up)
        grad = (dot(left[...], rows_of(wd), NT) * s[...].astype(F32)).astype(BF16)
        at = pl.ds(pl.multiple_of(j * tile, tile), tile)
        wide[:, at] = jnp.sum(grad.astype(F32), 0, keepdims=True)
        turn(3 * j + 1, 0, 3 * n_up)
        g[0] = dot(right[...], grad, TN).astype(BF16).reshape(g.shape[1:])
        turn(3 * j + 2, 0, 3 * n_up)
        acc[...] += dot(grad, rows_of(wu), NT)

    per = n_up // n_up_parts
    q_down = w_down.shape[2]
    blocks = tile // (2 * q_down)
    shape = g_up.shape[1:7]
    pltpu.emit_pipeline(
        ffn_body,
        grid=(n_up,),
        in_specs=[
            pl.BlockSpec((blocks, 2, q_down, width), lambda j: (j, 0, 0, 0)),
            pl.BlockSpec((tokens, tile), lambda j: (0, j)),
            whole_spec(w_up, tile),
        ],
        out_specs=[pl.BlockSpec((1,) + shape + (tile,), lambda j: (j // per, 0, 0, 0, 0, 0, 0, j % per))],
    )(w_down, slope, w_up, g_up)
    rs[2].start()
    load = pltpu.make_async_copy(n1, right, csem.at[1])
    load.start()
    base = 3 * n_up

    step = 128
    n_rows = tokens // step

    def norm_two_body(m, o):
        i = pl.program_id(0)
        turn(base + i, base, n_rows)
        rows = pl.ds(pl.multiple_of(i * step, step), step)
        upstream = left[rows, :].astype(F32)
        part, gain, shift = norm_back(m[...], small[6:7], acc[rows, :])
        total = upstream + part
        o[...] = total
        low = total.astype(BF16)
        branch[rows, :] = low
        narrow[2:3] += jnp.sum(low.astype(F32), 0, keepdims=True)
        narrow[3:4] += jnp.sum(upstream, 0, keepdims=True)
        narrow[6:7] += gain[None]
        narrow[7:8] += shift[None]

    row_spec = pl.BlockSpec((step, width), lambda i: (i, 0))
    pltpu.emit_pipeline(norm_two_body, grid=(n_rows,), in_specs=[row_spec], out_specs=[row_spec])(middle, mid_grad)
    base += n_rows

    n_out = width // 256
    first_out = base

    def out_body(a, w, g, o):
        i = pl.program_id(0)
        turn(first_out + i, first_out, n_out)
        g[...] = dot(a[...], branch[...], TN).astype(BF16).reshape(g.shape)
        rows = pl.ds(pl.multiple_of(i * 256, 256), 256)
        o[...] = dot(branch[rows, :], rows_of(w), NT).astype(BF16)

    q = g_out.shape[5]
    levels = 256 // (16 * q)
    assert levels == 1
    pltpu.emit_pipeline(
        out_body,
        grid=(n_out,),
        in_specs=[pl.BlockSpec((tokens, 256), lambda i: (0, i)), whole_spec(w_out)],
        out_specs=[
            pl.BlockSpec((1, 2, 2, 2, 2, q, width), lambda i: (i, 0, 0, 0, 0, 0, 0)),
            pl.BlockSpec((256, width), lambda i: (i, 0)),
        ],
    )(attended, w_out, g_out, ag)
    rs[3].start()
    base += n_out

    first_attend = base
    n_attend = (tokens // length) * pairs

    def attend_body(q, k, v, g, l, d):
        s, h = pl.program_id(0), pl.program_id(1)
        turn(first_attend + s * pairs + h, first_attend, n_attend)
        bwd_body(q, k, v, g, l.at[0, 0], d.at[0], d.at[1], d.at[2], dk_acc, dv_acc, 256)
        at = pl.ds(pl.multiple_of(h * 128, 128), 128)
        narrow[0:1, at] += jnp.sum(d[0].astype(F32), 0, keepdims=True)
        narrow[1:2, at] += jnp.sum(d[2].astype(F32), 0, keepdims=True)

    def head_spec(off):
        return pl.BlockSpec((length, 128), lambda s, h: (s, off + h))

    pltpu.emit_pipeline(
        attend_body,
        grid=(tokens // length, pairs),
        in_specs=[head_spec(0), head_spec(pairs), head_spec(2 * pairs), head_spec(0)]
        + [pl.BlockSpec((1, 1, 2, length), lambda s, h: (s, h, 0, 0))],
        out_specs=[pl.BlockSpec((3, length, 128), lambda s, h: (0, s, h))],
    )(merged, merged, merged, ag, logsum, back)
    base += n_attend
    load.wait()

    first_qkv = base
    n_qkv = 3 * width // tile
    per_part = width // tile

    def grad_body(d, g):
        j = pl.program_id(0)
        for k in (1, 2):

            @pl.when(j == k * per_part + 1)
            def _(k=k):
                rs[3 + k].start()

        turn(first_qkv + j, first_qkv, n_qkv)
        g[0] = dot(right[...], d[0], TN).astype(BF16).reshape(g.shape[1:])

    shape = g_qkv.shape[1:7]
    back_spec = pl.BlockSpec((1, tokens, tile), lambda j: (j // per_part, 0, j % per_part))
    pltpu.emit_pipeline(
        grad_body,
        grid=(n_qkv,),
        in_specs=[back_spec],
        out_specs=[
            pl.BlockSpec((1,) + shape + (tile,), lambda j: (j // per_part, 0, 0, 0, 0, 0, 0, j % per_part))
        ],
    )(back, g_qkv)
    rs[6].start()
    base += n_qkv
    first_in = base
    acc[...] = jnp.zeros_like(acc)

    def in_body(d, w):
        j = pl.program_id(0)
        turn(first_in + j, first_in, n_qkv)
        acc[...] += dot(d[0], rows_of(w), NT)

    pltpu.emit_pipeline(in_body, grid=(n_qkv,), in_specs=[back_spec, whole_spec(w_qkv, tile)])(back, w_qkv)
    base += n_qkv

    first_one = base

    def norm_one_body(v, m, o):
        i = pl.program_id(0)
        turn(first_one + i, first_one, n_rows)
        rows = pl.ds(pl.multiple_of(i * step, step), step)
        part, gain, shift = norm_back(v[...].astype(F32), small[4:5], acc[rows, :])
        o[...] = m[...] + part
        narrow[4:5] += gain[None]
        narrow[5:6] += shift[None]

    pltpu.emit_pipeline(norm_one_body, grid=(n_rows,), in_specs=[row_spec] * 2, out_specs=[row_spec])(
        x, mid_grad, input_grad
    )
    base += n_rows
    for k in range(16):
        z, y, xx = k // 4, (k // 2) % 2, k % 2
        g_vec[z, y, xx, 0, 0] = narrow[:, 128 * (k // 2) : 128 * (k // 2) + 128]
        for i in range(2):
            g_vec[z, y, xx, 0, 1, i : i + 1] = wide[:, 256 * k + 128 * i : 256 * k + 128 * i + 128]
    rs[7].start()
    acc[...] = jnp.zeros_like(acc)

    first_down = base

    def down_body(a, w):
        j = pl.program_id(0)
        turn(first_down + j, first_down, n_up)
        acc[...] += dot(a[...], rows_of(w))

    pltpu.emit_pipeline(
        down_body,
        grid=(n_up,),
        in_specs=[
            pl.BlockSpec((tokens, tile), lambda j: (0, j)),
            pl.BlockSpec((blocks, 2, q_down, width), lambda j: (j, 0, 0, 0)),
        ],
    )(act, w_down)
    base += n_up
    first_last = base

    def last_body(m, o):
        i = pl.program_id(0)
        turn(first_last + i, first_last, n_rows)
        rows = pl.ds(pl.multiple_of(i * step, step), step)
        o[...] = (m[...] + (acc[rows, :] + small[3:4])).astype(BF16)

    pltpu.emit_pipeline(last_body, grid=(n_rows,), in_specs=[row_spec], out_specs=[row_spec])(middle, output)
    base += n_rows
    for at, stage, k, i in plan:
        if at >= base:
            getattr(rs[k], STAGES[stage])(i)
    for r in rs:
        r.finish()


def backward_call(weights, x, c, kept, length):
    n1, merged, logsum, attended, middle, n2, act, slope, g_down, small = kept
    tokens, width = x.shape
    hidden = act.shape[1]
    q, q_down = width // 64, hidden // 64
    parts = 2
    low = lambda *shape: jax.ShapeDtypeStruct(shape, BF16)
    full = lambda *shape: jax.ShapeDtypeStruct(shape, F32)
    vmem, any_space = pl.BlockSpec(memory_space=pltpu.VMEM), pl.BlockSpec(memory_space=pl.ANY)
    kinds = [(q_down, width, BF16)] + [(q, hidden // parts, BF16)] * 2 + [(q, width, BF16)] * 4 + [(8, 128, F32)]
    scratch = []
    for kind in kinds:
        scratch += Scatter.scratch(*kind)
    scratch += [pltpu.VMEM((2, 2, 2, 2) + kind[:2], kind[2]) for kind in kinds]
    scratch += [
        pltpu.VMEM((4, 2, 2, 2, 2, 8, 128), F32),
        pltpu.VMEM((8, width), F32),
        pltpu.VMEM((1, hidden), F32),
        pltpu.VMEM((tokens, width), BF16),
        pltpu.VMEM((tokens, width), BF16),
        pltpu.VMEM((tokens, width), F32),
        pltpu.VMEM((tokens, width), BF16),
        pltpu.VMEM((length, 128), F32),
        pltpu.VMEM((length, 128), F32),
        pltpu.SemaphoreType.DMA((8, RS_SEMS)),
        pltpu.SemaphoreType.DMA((2,)),
    ]
    shards = [full(2, 2, q, 3 * width), full(2, 2, q, width), full(2, 2, q, hidden), full(2, 2, q_down, width)]
    outs = pl.pallas_call(
        lambda *refs: backward_kernel(length, PLAN, parts, *refs),
        in_specs=[any_space] * 15 + [vmem],
        out_specs=[any_space] * 2 + [vmem] * 5 + [any_space] * 14,
        out_shape=[low(tokens, width), full(tokens, width)]
        + shards
        + [full(2, 2, 8, 128)]
        + [
            low(3, 4, 2, 2, 2, 2, q, width),
            low(4, 2, 2, 2, 2, q, width),
            low(parts, 4, 2, 2, 2, 2, q, hidden // parts),
            full(tokens, width),
            low(tokens, width),
            low(3, tokens, width),
        ]
        + [jax.ShapeDtypeStruct((4, 2, 2, 2) + kind[:2], kind[2]) for kind in kinds],
        scratch_shapes=scratch,
        compiler_params=pltpu.CompilerParams(
            collective_id=1, has_side_effects=True, vmem_limit_bytes=66 * 10**6
        ),
        name="backward",
    )(*weights, x, c, n1, merged, logsum, attended, middle, n2, act, slope, g_down.reshape(4, 2, 2, 2, 2, q_down, width), small)
    grads = [o.reshape(-1, o.shape[-1]) for o in outs[2:6]]
    return outs[0], outs[1], grads, outs[6].reshape(32, 128)


def forward_plain(x, weights, small, length):
    w_qkv, w_out, w_up, w_down = weights
    b_query, b_value, b_out, b_up, b_down, gain_one, shift_one, gain_two, shift_two = small
    xf = x.astype(F32)
    normed_one = layer_norm(xf, gain_one, shift_one).astype(BF16)
    qkv_bias = jnp.concatenate([b_query, jnp.zeros_like(b_query), b_value])
    merged = (dot(normed_one, w_qkv) + qkv_bias).astype(BF16)
    attended, logsum = attn_fwd(merged, length)
    middle = xf + (dot(attended, w_out) + b_out)
    normed_two = layer_norm(middle, gain_two, shift_two).astype(BF16)
    activated, slope = gelu_pair(dot(normed_two, w_up) + b_up)
    return normed_one, merged, logsum, attended, middle, normed_two, activated.astype(BF16), slope.astype(BF16)


def backward(x, c, weights, small, kept, length):
    w_qkv, w_out, w_up, w_down = weights
    b_down, gain_one, gain_two = small
    normed_one, merged, logsum, attended, middle, normed_two, activated, slope = kept
    width = x.shape[1]
    xf, cf = x.astype(F32), c.astype(F32)
    output = (middle + (dot(activated, w_down) + b_down)).astype(BF16)

    grad_down_bias = jnp.sum(cf, 0)
    hidden_grad = (dot(c, w_down, NT) * slope.astype(F32)).astype(BF16)
    grad_up_bias = jnp.sum(hidden_grad.astype(F32), 0)
    grad_up = dot(normed_two, hidden_grad, TN).astype(BF16)
    part, grad_gain_two, grad_shift_two = norm_back(middle, gain_two, dot(hidden_grad, w_up, NT))
    middle_grad = cf + part
    branch_grad = middle_grad.astype(BF16)
    grad_out_bias = jnp.sum(branch_grad.astype(F32), 0)
    grad_out = dot(attended, branch_grad, TN).astype(BF16)
    attended_grad = dot(branch_grad, w_out, NT).astype(BF16)
    back = attn_bwd(merged, attended_grad, logsum, length)
    grad_query_bias = jnp.sum(back[0].astype(F32), 0)
    grad_value_bias = jnp.sum(back[2].astype(F32), 0)
    grad_qkv = jnp.concatenate([dot(normed_one, back[j], TN).astype(BF16) for j in range(3)], 1)
    normed_one_grad = sum(dot(back[j], w_qkv[:, j * width : (j + 1) * width], NT) for j in range(3))
    part, grad_gain_one, grad_shift_one = norm_back(xf, gain_one, normed_one_grad)
    input_grad = middle_grad + part
    return (
        output,
        input_grad,
        (grad_qkv, grad_out, grad_up),
        (
            grad_query_bias,
            grad_value_bias,
            grad_out_bias,
            grad_up_bias,
            grad_down_bias,
            grad_gain_one,
            grad_shift_one,
            grad_gain_two,
            grad_shift_two,
        ),
    )


def pack_shards(vectors):
    wide = vectors[3]
    narrow = jnp.stack([v for k, v in enumerate(vectors) if k != 3])
    zeros = jnp.zeros_like(narrow)
    odd = lax.axis_index("fsdp") % 2 == 1
    lanes = jnp.concatenate([jnp.where(odd, zeros, narrow), jnp.where(odd, narrow, zeros)], 1)
    rows = jnp.concatenate([lanes, wide.reshape(2, 128)], 0)
    return jnp.pad(rows, ((0, 64 - rows.shape[0]), (0, 0)))


def unpack_shard(packed):
    odd = lax.axis_index("fsdp") % 2 == 1
    narrow = jnp.where(odd, packed[:8, 64:], packed[:8, :64])
    wide = packed[8:10].reshape(256)
    return tuple(narrow[j] for j in range(3)) + (wide,) + tuple(narrow[j] for j in range(3, 8))


def local_ring(block_input, *rest):
    shards, cotangent = rest[:13], rest[13]
    length, width = block_input.shape[1:]
    x, c = block_input.reshape(-1, width), cotangent.reshape(-1, width)
    weights, kept = forward_call(shards[:4] + (pack_shards(shards[4:]),), x, c, length)
    output, input_grad, grads, vec = backward_call(weights, x, c, kept, length)
    whole = (output.reshape(block_input.shape), input_grad.reshape(block_input.shape))
    return whole + tuple(grads) + unpack_shard(vec)


def local_any(block_input, *rest):
    shards, cotangent = rest[:13], rest[13]
    length, width = block_input.shape[1:]
    x, c = block_input.reshape(-1, width), cotangent.reshape(-1, width)
    gathered = [lax.all_gather(shard, "fsdp", axis=0, tiled=True) for shard in shards]
    weights, small = gathered[:4], tuple(v.astype(F32) for v in gathered[4:])
    kept = forward_plain(x, weights, small, length)
    output, input_grad, mats, vecs = backward(x, c, weights, (small[4], small[5], small[7]), kept, length)
    mats += (dot(kept[6], c, TN),)

    def reduce(grad):
        part = lax.psum_scatter(grad.astype(F32), "fsdp", scatter_dimension=0, tiled=True)
        return lax.psum(part, "seq")

    whole = (output.reshape(block_input.shape), input_grad.reshape(block_input.shape))
    return whole + tuple(reduce(grad) for grad in mats + vecs)


def solution(mesh):
    split = P(("fsdp", "seq"), None, None)
    matrix, vector = P("fsdp", None), P("fsdp")
    in_specs = (split,) + (matrix,) * 4 + (vector,) * 9 + (split,)
    out_specs = (split, split) + (matrix,) * 4 + (vector,) * 9
    local = local_ring if (mesh.shape["fsdp"], mesh.shape["seq"]) == (16, 2) else local_any
    return jax.shard_map(local, mesh=mesh, in_specs=in_specs, out_specs=out_specs, check_vma=False)
```

```python
import jax
import jax.numpy as jnp
from jax import lax
from jax.experimental import pallas as pl
from jax.experimental.pallas import tpu as pltpu
from jax.sharding import PartitionSpec as P

EPSILON = 1e-05
NEG_LARGE = -1e30
MESH = pl.DeviceIdType.MESH
NN = (((1,), (0,)), ((), ()))
NT = (((1,), (1,)), ((), ()))
TN = (((0,), (0,)), ((), ()))
BF16 = jnp.bfloat16
F32 = jnp.float32
VMEM_LIMIT = 60 * 2**20


def dot(left, right, dims=NN):
    return lax.dot_general(left, right, dims, preferred_element_type=F32)


class Place:
    def __init__(self):
        f = lax.axis_index("fsdp")
        self.c = lax.axis_index("seq")
        self.z, self.y, self.x = f // 4, (f // 2) % 2, f % 2

    def block(self, z, y, x):
        return z * 4 + y * 2 + x

    def dev(self, z, y, x):
        return (self.block(z, y, x), self.c)

    @property
    def xn(self):
        return self.dev(self.z, self.y, 1 - self.x)

    @property
    def yn(self):
        return self.dev(self.z, 1 - self.y, self.x)

    @property
    def up(self):
        return self.dev(self.z + 1, self.y, self.x)

    @property
    def down(self):
        return self.dev(self.z - 1, self.y, self.x)

    @property
    def partner(self):
        return (self.block(self.z, self.y, self.x), 1 - self.c)


def greet(p):
    barrier = pltpu.get_barrier_semaphore()

    def signal(device):
        pl.semaphore_signal(barrier, inc=1, device_id=device, device_id_type=MESH)

    for device in (p.xn, p.yn, p.partner):
        signal(device)

    @pl.when(p.z < 3)
    def _():
        signal(p.up)

    @pl.when(p.z > 0)
    def _():
        signal(p.down)

    inner = jnp.logical_and(p.z > 0, p.z < 3)

    @pl.when(inner)
    def _():
        pl.semaphore_wait(barrier, 5)

    @pl.when(jnp.logical_not(inner))
    def _():
        pl.semaphore_wait(barrier, 4)


def greet_column(p):
    barrier = pltpu.get_barrier_semaphore()
    column = [p.dev((p.z + k) % 4, p.y, p.x) for k in (1, 2, 3)]
    for device in [p.xn, p.yn, p.partner] + column:
        pl.semaphore_signal(barrier, inc=1, device_id=device, device_id_type=MESH)
    pl.semaphore_wait(barrier, 6)


def remote(src, dst, send, recv, device):
    return pltpu.make_async_remote_copy(
        src_ref=src, dst_ref=dst, send_sem=send, recv_sem=recv, device_id=device, device_id_type=MESH
    )


def wait_bytes(ref, sem):
    pltpu.make_async_copy(ref, ref, sem).wait()


AG_SEMS = 24


class Gather:
    def __init__(self, p, src, dst, sems):
        self.p, self.src, self.dst, self.sems = p, src, dst, sems
        self.rz = [None] * 4
        self.send, self.zsend, self.local, self.rp = (sems.at[20], sems.at[21], sems.at[22], sems.at[23])

    def half(self, z, y, x):
        return self.dst.at[2 * self.p.block(z, y, x) + self.p.c]

    def to(self, src, dst, recv, device, send=None):
        remote(src, dst, self.send if send is None else send, self.sems.at[recv], device).start()

    def spread(self, src, z):
        p = self.p
        mine = self.half(z, p.y, p.x)
        self.to(src, mine, 4 + z, p.xn)
        self.to(src, mine, 8 + z, p.yn)

    def along(self, src, z, up):
        p = self.p
        mine = self.half(z, p.y, p.x)

        @pl.when(p.z < 3 if up else p.z > 0)
        def _():
            self.to(src, mine, z, p.up if up else p.down, self.zsend)

    def start(self):
        p = self.p
        own = self.src.at[p.c]
        self.along(own, p.z, True)
        self.along(own, p.z, False)
        me = p.block(p.z, p.y, p.x)
        pltpu.make_async_copy(self.src, self.dst.at[pl.ds(2 * me, 2)], self.local).start()

    def at_distance(self, s, body):
        p = self.p
        if s == 0:
            body(p.z, None)
            return

        @pl.when(p.z - s >= 0)
        def _():
            body(p.z - s, True)

        @pl.when(p.z + s <= 3)
        def _():
            body(p.z + s, False)

    def z_step(self, s):
        p = self.p
        if s == 0:
            self.start()
            return

        def body(z, up):
            mine = self.half(z, p.y, p.x)
            wait_bytes(mine, self.sems.at[z])
            self.along(mine, z, up)
            self.to(mine, mine, 23, p.partner)

        self.at_distance(s, body)

    def spread_step(self, s):
        p = self.p

        def body(z, up):
            self.spread(self.src.at[p.c] if s == 0 else self.half(z, p.y, p.x), z)

        self.at_distance(s, body)

    def xy_step(self, s):
        p = self.p

        def body(z, up):
            a = self.half(z, p.y, 1 - p.x)
            wait_bytes(a, self.sems.at[4 + z])
            self.to(a.at[0], a.at[0], 12 + z, p.yn)
            self.to(a, a, 23, p.partner)
            b = self.half(z, 1 - p.y, p.x)
            wait_bytes(b, self.sems.at[8 + z])
            self.to(b.at[1], b.at[1], 16 + z, p.xn)
            self.to(b, b, 23, p.partner)

        self.at_distance(s, body)

    def diag_step(self, s):
        p = self.p

        def body(z, up):
            d = self.half(z, 1 - p.y, 1 - p.x)
            wait_bytes(d.at[0], self.sems.at[12 + z])
            wait_bytes(d.at[1], self.sems.at[16 + z])
            self.to(d, d, 23, p.partner)

        self.at_distance(s, body)

    def arrived(self):
        wait_bytes(self.dst.at[pl.ds(0, 15)], self.rp)
        wait_bytes(self.dst.at[pl.ds(0, 2)], self.local)

    def drain(self):
        p = self.p
        wait_bytes(self.dst.at[pl.ds(0, 27)], self.send)
        inner = jnp.logical_and(p.z > 0, p.z < 3)

        @pl.when(inner)
        def _():
            wait_bytes(self.dst.at[pl.ds(0, 5)], self.zsend)

        @pl.when(jnp.logical_not(inner))
        def _():
            wait_bytes(self.dst.at[pl.ds(0, 1)], self.zsend)


GATHER_STAGES = ("z_step", "spread_step", "xy_step", "diag_step")


def hook(index, table):
    for k, steps in table.items():

        @pl.when(index == k)
        def _(steps=steps):
            for step in steps:
                step()


RS_SEMS = 44


class Scatter:
    def __init__(self, p, g, out, pr, bufs, tmp, sems):
        self.p, self.g, self.out, self.pr, self.tmp, self.sems = p, g, out, pr, tmp, sems
        self.o, self.x1, self.y1, self.x2, self.y2, self.u, self.d = bufs
        self.psend, self.zsend, self.fsend, self.frecv = (sems.at[36 + i] for i in range(4))

    @staticmethod
    def scratch(q, width, dtype):
        shapes = [(4, 2, 2, 2), (4, 2), (4, 2), (4,), (4,), (4, 2), (4, 2)]
        return [pltpu.VMEM(shape + (q, width), dtype) for shape in shapes]

    def level(self, i):
        z = self.p.z
        return jnp.where(z < 2, 3 - i, i)

    def sem(self, kind, i):
        return self.sems.at[4 * kind + i]

    def start(self):
        p = self.p
        for i in range(4):
            z = self.level(i)
            theirs = self.g.at[z, :, :, 1 - p.c]
            remote(theirs, self.pr.at[z], self.psend, self.sem(0, i), p.partner).start()
            pltpu.make_async_copy(self.g.at[z, :, :, p.c], self.o.at[z], self.sem(1, i)).start()

    def fetch(self, i):
        z = self.level(i)
        wait_bytes(self.pr.at[z], self.sem(0, i))
        pltpu.make_async_copy(self.pr.at[z], self.tmp.at[i % 2], self.sems.at[40 + i]).start()

    def stage0(self, i):
        p = self.p
        z = self.level(i)
        wait_bytes(self.o.at[z], self.sem(1, i))
        wait_bytes(self.tmp.at[i % 2], self.sems.at[40 + i])

        def add(j, carry):
            y, x, k = j // 4, (j // 2) % 2, j % 2
            self.o[z, y, x, k] = self.o[z, y, x, k] + self.tmp[i % 2, y, x, k]
            return carry

        lax.fori_loop(0, 8, add, 0)
        remote(self.o.at[z, :, 1 - p.x, 0], self.x1.at[z], self.sems.at[32], self.sem(2, i), p.xn).start()
        remote(self.o.at[z, 1 - p.y, :, 1], self.y1.at[z], self.sems.at[33], self.sem(3, i), p.yn).start()

    def stage1(self, i):
        p = self.p
        z = self.level(i)
        wait_bytes(self.x1.at[z], self.sem(2, i))
        for y in range(2):
            self.o[z, y, p.x, 0] = self.o[z, y, p.x, 0] + self.x1[z, y]
        remote(self.o.at[z, 1 - p.y, p.x, 0], self.y2.at[z], self.sems.at[35], self.sem(4, i), p.yn).start()
        wait_bytes(self.y1.at[z], self.sem(3, i))
        for x in range(2):
            self.o[z, p.y, x, 1] = self.o[z, p.y, x, 1] + self.y1[z, x]
        remote(self.o.at[z, p.y, 1 - p.x, 1], self.x2.at[z], self.sems.at[34], self.sem(5, i), p.xn).start()

    def along(self, z, up):
        p = self.p
        buf, kind = (self.u, 6) if up else (self.d, 7)
        remote(
            self.o.at[z, p.y, p.x], buf.at[z], self.zsend, self.sems.at[4 * kind + z], p.up if up else p.down
        ).start()

    def chain(self, z, up):
        p = self.p
        buf, kind = (self.u, 6) if up else (self.d, 7)
        wait_bytes(buf.at[z], self.sems.at[4 * kind + z])
        self.o[z, p.y, p.x] = self.o[z, p.y, p.x] + buf[z]
        self.along(z, up)

    def stage2(self, i):
        p = self.p
        z = self.level(i)
        wait_bytes(self.y2.at[z], self.sem(4, i))
        wait_bytes(self.x2.at[z], self.sem(5, i))
        self.o[z, p.y, p.x, 0] = self.o[z, p.y, p.x, 0] + self.y2[z]
        self.o[z, p.y, p.x, 1] = self.o[z, p.y, p.x, 1] + self.x2[z]

        @pl.when(jnp.logical_and(p.z == 0, z > 0))
        def _():
            self.along(z, True)

        @pl.when(jnp.logical_and(p.z == 3, z < 3))
        def _():
            self.along(z, False)

    def stage3(self, i):
        p = self.p
        z = self.level(i)
        inner = jnp.logical_and(p.z > 0, p.z < 3)

        @pl.when(jnp.logical_and(inner, z > p.z))
        def _():
            self.chain(z, True)

        @pl.when(jnp.logical_and(inner, z < p.z))
        def _():
            self.chain(z, False)

    def stage4(self, i=0):
        p = self.p
        z = p.z
        self.out[p.c] = self.o[z, p.y, p.x].astype(F32)

        @pl.when(z > 0)
        def _():
            wait_bytes(self.u.at[z], self.sems.at[24 + z])
            self.out[p.c] = self.out[p.c] + self.u[z].astype(F32)

        @pl.when(z < 3)
        def _():
            wait_bytes(self.d.at[z], self.sems.at[28 + z])
            self.out[p.c] = self.out[p.c] + self.d[z].astype(F32)

        remote(self.out.at[p.c], self.out.at[p.c], self.fsend, self.frecv, p.partner).start()

    def finish(self):
        p = self.p
        wait_bytes(self.out.at[1 - p.c], self.frecv)
        wait_bytes(self.out.at[p.c], self.fsend)
        wait_bytes(self.o, self.psend)
        for k, ref in enumerate((self.x1, self.y1, self.x2, self.y2)):
            wait_bytes(ref, self.sems.at[32 + k])
        wait_bytes(self.u.at[pl.ds(0, 3)], self.zsend)


class VectorScatter:
    def __init__(self, p, g, out, bufs, sems):
        self.p, self.g, self.out, self.sems = p, g, out, sems
        self.pv, self.xv, self.yv, self.zv, self.t1, self.t2, self.t3 = bufs

    @staticmethod
    def scratch():
        shapes = [(4, 2, 2), (4, 2), (4,), (4,), (4, 2, 2), (4, 2), (4,)]
        return [pltpu.VMEM(shape + (16, 128), F32) for shape in shapes]

    def start(self):
        remote(self.g, self.pv, self.sems.at[0], self.sems.at[1], self.p.partner).start()

    def cores(self):
        p = self.p
        wait_bytes(self.pv, self.sems.at[1])
        self.t1[...] = self.g[...] + self.pv[...]
        remote(self.t1.at[:, :, 1 - p.x], self.xv, self.sems.at[2], self.sems.at[3], p.xn).start()

    def over_x(self):
        p = self.p
        wait_bytes(self.xv, self.sems.at[3])
        self.t2[...] = self.t1[:, :, p.x] + self.xv[...]
        remote(self.t2.at[:, 1 - p.y], self.yv, self.sems.at[4], self.sems.at[5], p.yn).start()

    def over_y(self):
        p = self.p
        wait_bytes(self.yv, self.sems.at[5])
        self.t3[...] = self.t2[:, p.y] + self.yv[...]
        for k in (1, 2, 3):
            z = (p.z + k) % 4
            there = p.dev(z, p.y, p.x)
            remote(self.t3.at[z], self.zv.at[p.z], self.sems.at[6], self.sems.at[8 + p.z], there).start()

    def over_z(self):
        p = self.p
        total = self.t3[p.z]
        for k in (1, 2, 3):
            z = (p.z + k) % 4
            wait_bytes(self.zv.at[z], self.sems.at[8 + z])
            total = total + self.zv[z]
        self.out[...] = total

    def finish(self):
        wait_bytes(self.g, self.sems.at[0])
        wait_bytes(self.xv, self.sems.at[2])
        wait_bytes(self.yv, self.sems.at[4])
        wait_bytes(self.zv.at[pl.ds(0, 3)], self.sems.at[6])


def lane_masks(rows, width, dtype=BF16):
    lanes = lax.broadcasted_iota(jnp.int32,(rows,width),1)
    return lanes < width//2
def pick(h, low, v):
    z=jnp.zeros_like(v)
    return jnp.where(low, v, z) if h==0 else jnp.where(low, z, v)
def fwd_body(q_ref,k_ref,v_ref,o_ref,l_ref, B):
    S=q_ref.shape[0]
    low=lane_masks(S,128)
    q=q_ref[...]*BF16(0.125); k=k_ref[...]; v=v_ref[...]
    qs=[pick(h,low,q) for h in (0,1)]; vs=[pick(h,low,v) for h in (0,1)]
    for b in range(S//B):
        end=(b+1)*B
        acc=None
        for h in (0,1):
            st=dot(k[:end],qs[h][b*B:end],NT)
            key=lax.broadcasted_iota(jnp.int32,(B,B),0); qry=lax.broadcasted_iota(jnp.int32,(B,B),1)
            diag=jnp.where(key<=qry, st[b*B:end], NEG_LARGE)
            st=jnp.concatenate([st[:b*B],diag],0) if b else diag
            m=jnp.max(st,0,keepdims=True)
            p=jnp.exp(st-m)
            l=jnp.sum(p,0,keepdims=True)
            l_ref[h:h+1,b*B:end]=m+jnp.log(l)
            pt=(p*(1.0/l)).astype(BF16)
            o=dot(pt,vs[h][:end],TN)
            acc=o if acc is None else acc+o
        o_ref[b*B:end,:]=acc.astype(BF16)
def bwd_body(q_ref, k_ref, v_ref, g_ref, l_ref, dq_ref, dk_ref, dv_ref, dk_acc, dv_acc, B):
    S = q_ref.shape[0]
    low = lane_masks(S, 128)
    q = q_ref[...] * BF16(0.125)
    k, v, g = k_ref[...], v_ref[...], g_ref[...]
    qs, gs, ks = ([pick(h, low, t) for h in (0, 1)] for t in (q, g, k))
    key = lax.broadcasted_iota(jnp.int32, (B, B), 0)
    query = lax.broadcasted_iota(jnp.int32, (B, B), 1)
    blocks = list(reversed(range(S // B)))
    scores, grads = {}, {}
    for b in blocks:
        end = (b + 1) * B
        for h in (0, 1):
            scores[b, h] = dot(k[:end], qs[h][b * B : end], NT)
            grads[b, h] = dot(v[:end], gs[h][b * B : end], NT)
    for b in blocks:
        end = (b + 1) * B
        dq = dk = dv = None
        for h in (0, 1):
            qb, gb = qs[h][b * B : end], gs[h][b * B : end]
            p = jnp.exp(scores[b, h] - l_ref[h : h + 1, b * B : end])
            diag = jnp.where(key <= query, p[b * B : end], 0.0)
            p = jnp.concatenate([p[: b * B], diag], 0) if b else diag
            inner = jnp.sum(p * grads[b, h], 0, keepdims=True)
            ds = (p * (grads[b, h] - inner)).astype(BF16)
            parts = dot(ds, ks[h][:end], TN), dot(ds, qb, NN), dot(p.astype(BF16), gb, NN)
            dq, dk, dv = parts if h == 0 else (dq + parts[0], dk + parts[1], dv + parts[2])
        dq_ref[b * B : end, :] = (dq * 0.125).astype(BF16)
        if b == S // B - 1:
            dk_acc[...] = dk
            dv_acc[...] = dv
        else:
            dk_acc[:end, :] += dk
            dv_acc[:end, :] += dv
    dk_ref[...] = dk_acc[...].astype(BF16)
    dv_ref[...] = dv_acc[...].astype(BF16)


def attn_fwd(merged, S, B=256):
    T=merged.shape[0]; D=merged.shape[1]//3; n=D//128
    def body(q,k,v,o,l): fwd_body(q,k,v,o,l.at[0,0],B)
    sp=lambda off: pl.BlockSpec((S,128),lambda s,h: (s,off+h))
    return pl.pallas_call(body,grid=(T//S,n),in_specs=[sp(0),sp(n),sp(2*n)],
        out_specs=[pl.BlockSpec((S,128),lambda s,h:(s,h)),pl.BlockSpec((1,1,2,S),lambda s,h:(s,h,0,0))],
        out_shape=[jax.ShapeDtypeStruct((T,D),BF16),jax.ShapeDtypeStruct((T//S,n,2,S),F32)],
        name="attn_fwd",compiler_params=pltpu.CompilerParams(vmem_limit_bytes=40*2**20))(merged,merged,merged)
def attn_bwd(merged, g, lse, S, B=256):
    T=merged.shape[0]; D=merged.shape[1]//3; n=D//128
    def body(q,k,v,gr,l,d,dka,dva): bwd_body(q,k,v,gr,l.at[0,0],d.at[0],d.at[1],d.at[2],dka,dva,B)
    sp=lambda off: pl.BlockSpec((S,128),lambda s,h: (s,off+h))
    return pl.pallas_call(body,grid=(T//S,n),in_specs=[sp(0),sp(n),sp(2*n),sp(0),pl.BlockSpec((1,1,2,S),lambda s,h:(s,h,0,0))],
        out_specs=pl.BlockSpec((3,S,128),lambda s,h:(0,s,h)),
        out_shape=jax.ShapeDtypeStruct((3,T,D),BF16),
        scratch_shapes=[pltpu.VMEM((S,128),F32)]*2,
        name="attn_bwd",compiler_params=pltpu.CompilerParams(vmem_limit_bytes=40*2**20))(merged,merged,merged,g,lse)


def layer_norm(values, gain, shift):
    center = values - jnp.mean(values, -1, keepdims=True)
    spread = jnp.mean(center * center, -1, keepdims=True)
    return center * lax.rsqrt(spread + EPSILON) * gain + shift


def norm_back(values, gain, grad):
    center = values - jnp.mean(values, -1, keepdims=True)
    inverse = lax.rsqrt(jnp.mean(center * center, -1, keepdims=True) + EPSILON)
    unit = center * inverse
    scaled = grad * gain
    first = jnp.mean(scaled, -1, keepdims=True)
    second = jnp.mean(scaled * unit, -1, keepdims=True)
    return (inverse * (scaled - first - unit * second), jnp.sum(grad * unit, 0), jnp.sum(grad, 0))


def gelu_pair(u):
    a = 0.7978845608028654
    square = u * u
    half = 0.5 + 0.5 * jnp.tanh(u * (a + (a * 0.044715) * square))
    value = u * half
    slope = half + value * (1.0 - half) * (2.0 * a + (6.0 * a * 0.044715) * square)
    return value, slope


def whole_spec(ref, tile=None):
    n, two, q, width = ref.shape
    if tile is None:
        return pl.BlockSpec((n, two, q, width), lambda j: (0, 0, 0, 0))
    return pl.BlockSpec((n, two, q, tile), lambda j: (0, 0, 0, j))


def rows_of(block):
    value = block[...]
    return value.reshape(-1, value.shape[-1])


GATHER_PLAN = (
    (0, 0, 1, 0), (0, 1, 1, 0), (0, 0, 0, 0), (0, 0, 2, 0), (0, 1, 0, 0), (0, 1, 2, 0), (0, 0, 0, 1), (0, 2, 1, 0),
    (0, 0, 1, 1), (0, 2, 0, 0), (0, 1, 0, 1), (0, 1, 1, 1), (0, 0, 2, 1), (0, 2, 2, 0), (0, 0, 0, 2), (0, 1, 0, 2),
    (0, 0, 1, 2), (0, 1, 1, 2), (0, 2, 0, 1), (0, 0, 3, 0), (0, 3, 0, 0), (0, 0, 0, 3), (0, 0, 2, 2), (0, 2, 0, 2),
    (0, 1, 2, 2), (0, 0, 1, 3), (0, 1, 0, 3), (0, 3, 1, 0), (0, 2, 1, 2), (0, 1, 1, 3), (0, 0, 5, 0), (0, 3, 0, 1),
    (0, 3, 0, 2), (0, 0, 3, 1), (0, 2, 0, 3), (0, 0, 2, 3), (0, 1, 2, 3), (0, 3, 0, 3), (0, 2, 1, 1), (0, 2, 1, 3),
    (0, 1, 3, 0), (0, 1, 2, 1), (0, 0, 4, 0), (0, 1, 3, 1), (0, 0, 6, 0), (1, 3, 1, 1), (1, 3, 1, 3), (1, 1, 5, 0),
    (1, 3, 1, 2), (1, 2, 2, 3), (1, 0, 3, 2), (1, 2, 2, 2), (1, 2, 3, 0), (2, 0, 4, 1), (2, 1, 3, 2), (3, 2, 2, 1),
    (5, 1, 4, 0), (6, 2, 3, 1), (6, 0, 5, 1), (6, 0, 4, 2), (7, 3, 2, 2), (7, 1, 4, 1), (9, 2, 5, 0), (9, 3, 2, 3),
    (10, 1, 4, 2), (10, 3, 2, 0), (10, 0, 5, 2), (10, 3, 2, 1), (10, 3, 3, 0), (11, 0, 6, 1), (11, 2, 3, 2), (11, 0, 3, 3),
    (12, 1, 3, 3), (12, 0, 4, 3), (12, 1, 4, 3), (12, 1, 5, 2), (14, 0, 5, 3), (16, 0, 6, 2), (16, 2, 4, 0), (17, 2, 4, 3),
    (17, 2, 3, 3), (18, 1, 5, 1), (19, 2, 4, 2), (20, 2, 4, 1), (20, 3, 3, 2), (21, 3, 3, 3), (21, 3, 3, 1), (22, 1, 5, 3),
    (22, 2, 5, 2), (22, 0, 6, 3), (24, 3, 4, 0), (25, 2, 5, 1), (25, 3, 4, 3), (25, 1, 6, 1), (25, 2, 5, 3), (26, 3, 4, 2),
    (26, 1, 6, 3), (26, 3, 4, 1), (26, 1, 6, 0), (27, 3, 5, 2), (29, 3, 5, 3), (29, 3, 5, 1), (29, 1, 6, 2), (30, 3, 5, 0),
    (34, 2, 6, 0), (36, 2, 6, 1), (36, 2, 6, 2), (36, 2, 6, 3), (38, 3, 6, 0), (41, 3, 6, 1), (42, 3, 6, 2), (42, 3, 6, 3),
)


def forward_kernel(length, plan, *refs):
    (s_qkv, s_out, s_up, s_down, s_vec), refs = refs[:5], refs[5:]
    x, c = refs[:2]
    (wholes, refs) = (refs[2:9], refs[9:])
    n1, merged, logsum, attended, middle, n2, act, slope, grad_down, small, refs = refs[:10] + (refs[10:],)
    b_up, qkv_bias, vec, x_ref, c_ref, n1_ref, n2_ref, first_half, second_half, sems, local = refs
    tokens, width = x_ref.shape
    p = Place()
    for part, half in enumerate((first_half, second_half)):
        for k in range(3):
            columns = pl.ds(k * width + part * width // 2, width // 2)
            half[:, :, :, pl.ds(k * width // 2, width // 2)] = s_qkv[:, :, :, columns]
    greet(p)
    n_half = s_up.shape[3] // 2
    lows, highs = (s_up.at[:, :, :, pl.ds(k * n_half, n_half)] for k in (0, 1))
    sources = (first_half, second_half, s_out, lows, highs, s_down, s_vec)
    order = [6, 0, 1, 2, 3, 4, 5]
    gathers = [Gather(p, sources[i], wholes[i], sems.at[i]) for i in order]
    g_vec, g_first, g_second, g_out, g_low, g_high, g_down = gathers

    def steps(at):
        return [
            lambda stage=stage, w=w, s=s: getattr(gathers[w], GATHER_STAGES[stage])(s)
            for when, stage, w, s in plan
            if when == at
        ]

    def run(at):
        for step in steps(at):
            step()

    def turn(index, first, count, skip=0):
        hook(index, {k: steps(first + k) for k in range(skip, count) if steps(first + k)})

    loads = [pltpu.make_async_copy(x, x_ref, local.at[0]), pltpu.make_async_copy(c, c_ref, local.at[1])]
    for load in loads:
        load.start()
    run(0)
    g_vec.arrived()
    load = pltpu.make_async_copy(wholes[6], vec, local.at[2])
    load.start()
    load.wait()
    for load in loads:
        load.wait()
    for k in range(8):
        small[:, pl.ds(128 * k, 128)] = (vec[4 * k, 0, :8] + vec[4 * k + 2, 0, :8]).astype(F32)
    for k in range(16):
        for i in range(2):
            b_up[:, pl.ds(256 * k + 128 * i, 128)] = vec[2 * k, 0, 8 + i : 9 + i].astype(F32)
    qkv_bias[:, :width] = small[0:1]
    qkv_bias[:, width : 2 * width] = jnp.zeros_like(small[0:1])
    qkv_bias[:, 2 * width :] = small[1:2]

    def norm_rows(i, carry):
        rows = pl.ds(i * 128, 128)
        n1_ref[rows, :] = layer_norm(x_ref[rows, :].astype(F32), small[4:5], small[5:6]).astype(BF16)
        return carry

    lax.fori_loop(0, tokens // 128, norm_rows, 0)
    store_n1 = pltpu.make_async_copy(n1_ref, n1, local.at[0])
    store_n1.start()
    base = 1
    tile = 512

    halves = width // tile
    pairs = width // 128 // halves
    n_attend = (tokens // length) * pairs

    def head_spec(off):
        return pl.BlockSpec((length, 128), lambda s, h: (s, off + h))

    for part, (g, whole) in enumerate(((g_first, wholes[0]), (g_second, wholes[1]))):
        run(base)
        g.arrived()

        def qkv_body(w_ref, o_ref, first=base, part=part):
            j = pl.program_id(0)
            turn(j, first, 3, 1)
            at = pl.ds(pl.multiple_of((j * halves + part) * tile, tile), tile)
            o_ref[...] = (dot(n1_ref[...], rows_of(w_ref)) + qkv_bias[:, at]).astype(BF16)

        pltpu.emit_pipeline(
            qkv_body,
            grid=(3,),
            in_specs=[whole_spec(whole, tile)],
            out_specs=[pl.BlockSpec((tokens, tile), lambda j, part=part: (0, j * halves + part))],
        )(whole, merged)
        base += 3

        def attend_body(q, k, v, o, l, first=base):
            s, h = pl.program_id(0), pl.program_id(1)
            turn(s * pairs + h, first, n_attend)
            fwd_body(q, k, v, o, l.at[0, 0], 256)

        off = part * pairs
        third = width // 128
        pltpu.emit_pipeline(
            attend_body,
            grid=(tokens // length, pairs),
            in_specs=[head_spec(off), head_spec(third + off), head_spec(2 * third + off)],
            out_specs=[
                head_spec(off),
                pl.BlockSpec((1, 1, 2, length), lambda s, h, off=off: (s, off + h, 0, 0)),
            ],
        )(merged, merged, merged, attended, logsum)
        base += n_attend

    run(base)
    g_out.arrived()
    n_out, first_out = tokens // 256, base

    def out_body(a_ref, w_ref, m_ref):
        i = pl.program_id(0)
        turn(i, first_out, n_out, 1)
        rows = pl.ds(pl.multiple_of(i * 256, 256), 256)
        value = x_ref[rows, :].astype(F32) + (dot(a_ref[...], rows_of(w_ref)) + small[2:3])
        m_ref[...] = value
        n2_ref[rows, :] = layer_norm(value, small[6:7], small[7:8]).astype(BF16)

    pltpu.emit_pipeline(
        out_body,
        grid=(tokens // 256,),
        in_specs=[pl.BlockSpec((256, width), lambda i: (i, 0)), whole_spec(wholes[2])],
        out_specs=[pl.BlockSpec((256, width), lambda i: (i, 0))],
    )(attended, wholes[2], middle)

    store_n2 = pltpu.make_async_copy(n2_ref, n2, local.at[1])
    store_n2.start()
    base += n_out
    n_up = act.shape[1] // tile
    n_part = n_up // 2
    for part, (g, whole) in enumerate(((g_low, wholes[3]), (g_high, wholes[4]))):
        run(base)
        g.arrived()

        def up_body(w_ref, a_ref, s_ref, first=base, part=part):
            j = pl.program_id(0)
            turn(j, first, n_part, 1)
            bias = b_up[:, pl.ds(pl.multiple_of((part * n_part + j) * tile, tile), tile)]
            value, grad = gelu_pair(dot(n2_ref[...], rows_of(w_ref)) + bias)
            a_ref[...] = value.astype(BF16)
            s_ref[...] = grad.astype(BF16)

        column_spec = pl.BlockSpec((tokens, tile), lambda j, part=part: (0, part * n_part + j))
        pltpu.emit_pipeline(
            up_body,
            grid=(n_part,),
            in_specs=[whole_spec(whole, tile)],
            out_specs=[column_spec, column_spec],
        )(whole, act, slope)
        base += n_part

    first_grad = base

    def grad_body(a_ref, o_ref):
        turn(pl.program_id(0), first_grad, n_up)
        o_ref[...] = dot(a_ref[...], c_ref[...], TN).astype(BF16)

    pltpu.emit_pipeline(
        grad_body,
        grid=(n_up,),
        in_specs=[pl.BlockSpec((tokens, tile), lambda j: (0, j))],
        out_specs=[pl.BlockSpec((tile, width), lambda j: (j, 0))],
    )(act, grad_down)
    run(base + n_up)
    g_down.arrived()
    for g in gathers:
        g.drain()
    store_n1.wait()
    store_n2.wait()


def forward_call(shards, x, c, length):
    tokens, width = x.shape
    hidden = 16 * shards[3].shape[0]
    views = [s.reshape(2, 2, s.shape[0] // 4, s.shape[1]) for s in shards]
    q = views[0].shape[2]
    columns = [3 * width // 2] * 2 + [width] + [hidden // 2] * 2
    whole = [jax.ShapeDtypeStruct((32, 2, q, n), BF16) for n in columns]
    whole += [jax.ShapeDtypeStruct((32,) + v.shape[1:], BF16) for v in views[3:]]
    vmem, any_space = pl.BlockSpec(memory_space=pltpu.VMEM), pl.BlockSpec(memory_space=pl.ANY)
    low = lambda *shape: jax.ShapeDtypeStruct(shape, BF16)
    outs = pl.pallas_call(
        lambda *refs: forward_kernel(length, GATHER_PLAN, *refs),
        in_specs=[vmem] * 5 + [any_space] * 2,
        out_specs=[any_space] * 16 + [vmem],
        out_shape=whole
        + [
            low(tokens, width),
            low(tokens, 3 * width),
            jax.ShapeDtypeStruct((tokens // length, width // 128, 2, length), F32),
            low(tokens, width),
            jax.ShapeDtypeStruct((tokens, width), F32),
            low(tokens, width),
            low(tokens, hidden),
            low(tokens, hidden),
            low(hidden, width),
            jax.ShapeDtypeStruct((8, width), F32),
        ],
        scratch_shapes=[
            pltpu.VMEM((1, hidden), F32),
            pltpu.VMEM((1, 3 * width), F32),
            pltpu.VMEM(whole[6].shape, BF16),
            pltpu.VMEM((tokens, width), BF16),
            pltpu.VMEM((tokens, width), BF16),
            pltpu.VMEM((tokens, width), BF16),
            pltpu.VMEM((tokens, width), BF16),
            pltpu.VMEM((2, 2, q, 3 * width // 2), BF16),
            pltpu.VMEM((2, 2, q, 3 * width // 2), BF16),
            pltpu.SemaphoreType.DMA((7, AG_SEMS)),
            pltpu.SemaphoreType.DMA((3,)),
        ],
        compiler_params=pltpu.CompilerParams(collective_id=0, has_side_effects=True, vmem_limit_bytes=VMEM_LIMIT),
        name="forward",
    )(*views, x, c)
    return outs[:6], outs[7:]


PLAN = (
    (4, 0, 0, 0), (6, 1, 0, 0), (10, 0, 0, 1), (13, 1, 0, 1), (14, 2, 0, 0), (18, 0, 0, 2), (18, 0, 1, 0), (19, 0, 1, 1),
    (20, 1, 0, 2), (22, 0, 0, 3), (24, 1, 1, 0), (25, 1, 1, 1), (25, 1, 0, 3), (28, 0, 2, 0), (30, 1, 2, 0), (31, 0, 2, 2),
    (33, 3, 0, 0), (33, 1, 2, 2), (33, 2, 1, 1), (33, 2, 0, 1), (34, 0, 2, 1), (36, 2, 2, 0), (36, 2, 0, 2), (36, 1, 2, 1),
    (36, 0, 1, 3), (38, 2, 1, 0), (39, 1, 1, 3), (39, 0, 3, 1), (39, 0, 3, 0), (41, 2, 0, 3), (42, 0, 2, 3), (43, 0, 1, 2),
    (44, 3, 1, 1), (44, 3, 0, 1), (44, 2, 2, 1), (44, 1, 3, 1), (46, 2, 1, 3), (46, 1, 2, 3), (47, 1, 1, 2), (49, 1, 3, 0),
    (49, 0, 3, 2), (50, 2, 3, 1), (50, 0, 3, 3), (51, 1, 3, 3), (51, 3, 0, 2), (51, 3, 1, 0), (51, 3, 2, 1), (51, 1, 3, 2),
    (54, 4, 0, 0), (54, 3, 2, 0), (54, 2, 3, 0), (55, 2, 3, 3), (55, 2, 2, 2), (55, 2, 1, 2), (56, 2, 3, 2), (57, 2, 2, 3),
    (57, 3, 3, 1), (57, 0, 4, 1), (57, 4, 0, 1), (57, 0, 4, 0), (58, 1, 4, 0), (58, 1, 4, 1), (58, 0, 4, 3), (58, 3, 1, 2),
    (58, 0, 5, 0), (58, 3, 3, 0), (58, 4, 1, 2), (59, 1, 5, 0), (59, 0, 5, 1), (60, 1, 5, 1), (60, 4, 2, 0), (60, 3, 2, 2),
    (60, 0, 6, 0), (60, 2, 4, 0), (61, 0, 5, 2), (61, 3, 0, 3), (61, 2, 4, 1), (61, 0, 6, 1), (61, 4, 2, 2), (61, 1, 6, 0),
    (61, 2, 5, 0), (62, 4, 1, 0), (62, 2, 5, 1), (62, 3, 4, 0), (62, 4, 1, 1), (62, 1, 6, 1), (62, 4, 0, 3), (62, 0, 6, 3),
    (62, 3, 2, 3), (62, 1, 4, 3), (62, 4, 2, 1), (62, 0, 6, 2), (63, 1, 5, 2), (63, 2, 6, 0), (63, 3, 1, 3), (63, 3, 3, 2),
    (63, 0, 5, 3), (63, 1, 6, 2), (63, 3, 3, 3), (63, 0, 4, 2), (63, 4, 3, 0), (64, 3, 5, 0), (64, 2, 6, 1), (64, 1, 5, 3),
    (64, 4, 3, 1), (64, 4, 2, 3), (64, 3, 5, 1), (64, 1, 6, 3), (64, 4, 1, 3), (65, 1, 4, 2), (65, 4, 4, 0), (66, 3, 6, 0),
    (66, 2, 4, 3), (67, 2, 6, 2), (67, 4, 5, 0), (67, 4, 0, 2), (67, 2, 5, 2), (67, 3, 6, 1), (67, 2, 5, 3), (68, 4, 6, 0),
    (68, 4, 3, 3), (68, 3, 4, 1), (68, 2, 6, 3), (68, 3, 4, 3), (68, 5, 0, 0), (68, 4, 5, 1), (68, 2, 4, 2), (68, 4, 3, 2),
    (68, 3, 6, 2), (68, 4, 4, 3), (68, 4, 6, 1), (69, 3, 5, 2), (69, 3, 5, 3), (69, 4, 5, 2), (69, 3, 6, 3), (69, 4, 6, 3),
    (69, 5, 2, 0), (69, 5, 1, 0), (69, 4, 6, 2), (69, 3, 4, 2), (69, 4, 4, 2), (69, 5, 3, 0), (69, 4, 4, 1), (69, 4, 5, 3),
    (71, 5, 6, 0), (71, 5, 4, 0), (71, 5, 5, 0),
)

PRE, S0, S1, S2, S3, S4 = range(6)
STAGES = ("fetch", "stage0", "stage1", "stage2", "stage3", "stage4")


def column_sum(ref, at, value):
    ref[at] = ref[at] + jnp.sum(value, 0, keepdims=True)


def backward_kernel(length, plan, n_up_parts, *refs):
    (w_first, w_second, w_out, w_low, w_high, w_down), refs = refs[:6], refs[6:]
    x, c, n1, merged, logsum, attended, middle, n2, act, slope, g_down, small, refs = refs[:12] + (refs[12:],)
    output, input_grad, f_qkv, f_out, f_up, f_down, f_vec, g_qkv, g_out, g_up, mid_grad, ag, back, refs = refs[:13] + (
        refs[13:],
    )
    landing, refs = refs[:7], refs[7:]
    sets, refs = refs[: 7 * 7], refs[7 * 7 :]
    tmps, refs = refs[:7], refs[7:]
    vec_bufs, refs = refs[:7], refs[7:]
    (g_vec, narrow, wide, left, right, acc, out_acc, branch, dk_acc, dv_acc, sems, vec_sems, csem) = refs
    tokens, width = x.shape
    hidden = act.shape[1]
    tile = 512
    pairs = width // 128
    p = Place()
    greet_column(p)
    sets = [sets[7 * i : 7 * i + 7] for i in range(7)]
    half = hidden // n_up_parts
    entries = [
        (g_down, f_down),
        (g_up.at[0], f_up.at[:, :, :, pl.ds(0, half)]),
        (g_up.at[1], f_up.at[:, :, :, pl.ds(half, half)]),
        (g_out, f_out),
        (g_qkv.at[0], f_qkv.at[:, :, :, pl.ds(0, width)]),
        (g_qkv.at[1], f_qkv.at[:, :, :, pl.ds(width, width)]),
        (g_qkv.at[2], f_qkv.at[:, :, :, pl.ds(2 * width, width)]),
    ]
    rs = [Scatter(p, g, f, landing[k], sets[k], tmps[k], sems.at[k]) for k, (g, f) in enumerate(entries)]

    vectors = VectorScatter(p, g_vec, f_vec, vec_bufs, vec_sems)

    def turn(slot, first, count):
        table = {}
        for at, stage, k, i in plan:
            if first <= at < first + count:
                table.setdefault(at, []).append(lambda stage=stage, k=k, i=i: getattr(rs[k], STAGES[stage])(i))
        hook(slot, table)

    loads = [
        pltpu.make_async_copy(c, left, csem.at[0]),
        pltpu.make_async_copy(n2, right, csem.at[1]),
    ]
    for load in loads:
        load.start()
    rs[0].start()
    narrow[...] = jnp.zeros_like(narrow)
    wide[...] = jnp.zeros_like(wide)
    g_vec[...] = jnp.zeros_like(g_vec)
    acc[...] = jnp.zeros_like(acc)
    out_acc[...] = jnp.zeros_like(out_acc)
    for load in loads:
        load.wait()

    n_up = hidden // tile

    def ffn_body(wd, s, wu_low, wu_high, g):
        j = pl.program_id(0)

        @pl.when(j == n_up // 2 + 1)
        def _():
            rs[1].start()

        turn(3 * j, 0, 3 * n_up)
        grad = (dot(left[...], rows_of(wd), NT) * s[...].astype(F32)).astype(BF16)
        at = pl.ds(pl.multiple_of(j * tile, tile), tile)
        wide[:, at] = jnp.sum(grad.astype(F32), 0, keepdims=True)
        turn(3 * j + 1, 0, 3 * n_up)
        g[0] = dot(right[...], grad, TN).astype(BF16).reshape(g.shape[1:])
        turn(3 * j + 2, 0, 3 * n_up)

        @pl.when(j < n_up // 2)
        def _():
            acc[...] += dot(grad, rows_of(wu_low), NT)

        @pl.when(j >= n_up // 2)
        def _():
            acc[...] += dot(grad, rows_of(wu_high), NT)

    per = n_up // n_up_parts
    q_down = w_down.shape[2]
    blocks = tile // (2 * q_down)
    shape = g_up.shape[1:7]
    n, two, q, _ = w_low.shape
    pltpu.emit_pipeline(
        ffn_body,
        grid=(n_up,),
        in_specs=[
            pl.BlockSpec((blocks, 2, q_down, width), lambda j: (j, 0, 0, 0)),
            pl.BlockSpec((tokens, tile), lambda j: (0, j)),
            pl.BlockSpec((n, two, q, tile), lambda j: (0, 0, 0, jnp.minimum(j, n_up // 2 - 1))),
            pl.BlockSpec((n, two, q, tile), lambda j: (0, 0, 0, jnp.maximum(j - n_up // 2, 0))),
        ],
        out_specs=[pl.BlockSpec((1,) + shape + (tile,), lambda j: (j // per, 0, 0, 0, 0, 0, 0, j % per))],
    )(w_down, slope, w_low, w_high, g_up)
    rs[2].start()
    load = pltpu.make_async_copy(n1, right, csem.at[1])
    load.start()
    base = 3 * n_up

    step = 128
    n_rows = tokens // step
    thin = hidden // (2 * n_rows)
    first_two = base

    def norm_two_body(m, a, w, o):
        i = pl.program_id(0)
        turn(first_two + i, first_two, n_rows)
        out_acc[...] += dot(a[...], rows_of(w))
        rows = pl.ds(pl.multiple_of(i * step, step), step)
        upstream = left[rows, :].astype(F32)
        part, gain, shift = norm_back(m[...], small[6:7], acc[rows, :])
        total = upstream + part
        o[...] = total
        low = total.astype(BF16)
        branch[rows, :] = low
        narrow[2:3] += jnp.sum(low.astype(F32), 0, keepdims=True)
        narrow[3:4] += jnp.sum(upstream, 0, keepdims=True)
        narrow[6:7] += gain[None]
        narrow[7:8] += shift[None]

    row_spec = pl.BlockSpec((step, width), lambda i: (i, 0))
    pltpu.emit_pipeline(
        norm_two_body,
        grid=(n_rows,),
        in_specs=[
            row_spec,
            pl.BlockSpec((tokens, thin), lambda i: (0, i)),
            pl.BlockSpec((thin // (2 * q_down), 2, q_down, width), lambda i: (i, 0, 0, 0)),
        ],
        out_specs=[row_spec],
    )(middle, act, w_down, mid_grad)
    base += n_rows

    n_out = width // 256
    first_out = base

    def out_body(a, w, g, o):
        i = pl.program_id(0)
        turn(first_out + i, first_out, n_out)
        g[...] = dot(a[...], branch[...], TN).astype(BF16).reshape(g.shape)
        rows = pl.ds(pl.multiple_of(i * 256, 256), 256)
        o[...] = dot(branch[rows, :], rows_of(w), NT).astype(BF16)

    q = g_out.shape[5]
    levels = 256 // (16 * q)
    assert levels == 1
    pltpu.emit_pipeline(
        out_body,
        grid=(n_out,),
        in_specs=[pl.BlockSpec((tokens, 256), lambda i: (0, i)), whole_spec(w_out)],
        out_specs=[
            pl.BlockSpec((1, 2, 2, 2, 2, q, width), lambda i: (i, 0, 0, 0, 0, 0, 0)),
            pl.BlockSpec((256, width), lambda i: (i, 0)),
        ],
    )(attended, w_out, g_out, ag)
    rs[3].start()
    base += n_out

    first_attend = base
    n_attend = (tokens // length) * pairs

    def attend_body(q, k, v, g, l, d):
        s, h = pl.program_id(0), pl.program_id(1)
        turn(first_attend + s * pairs + h, first_attend, n_attend)
        bwd_body(q, k, v, g, l.at[0, 0], d.at[0], d.at[1], d.at[2], dk_acc, dv_acc, 256)
        at = pl.ds(pl.multiple_of(h * 128, 128), 128)
        narrow[0:1, at] += jnp.sum(d[0].astype(F32), 0, keepdims=True)
        narrow[1:2, at] += jnp.sum(d[2].astype(F32), 0, keepdims=True)

    def head_spec(off):
        return pl.BlockSpec((length, 128), lambda s, h: (s, off + h))

    pltpu.emit_pipeline(
        attend_body,
        grid=(tokens // length, pairs),
        in_specs=[head_spec(0), head_spec(pairs), head_spec(2 * pairs), head_spec(0)]
        + [pl.BlockSpec((1, 1, 2, length), lambda s, h: (s, h, 0, 0))],
        out_specs=[pl.BlockSpec((3, length, 128), lambda s, h: (0, s, h))],
    )(merged, merged, merged, ag, logsum, back)
    base += n_attend
    load.wait()

    first_qkv = base
    n_qkv = 3 * width // tile
    per_part = width // tile

    def grad_body(d, g):
        j = pl.program_id(0)
        for k in (1, 2):

            @pl.when(j == k * per_part + 1)
            def _(k=k):
                rs[3 + k].start()

        turn(first_qkv + j, first_qkv, n_qkv)
        g[0] = dot(right[...], d[0], TN).astype(BF16).reshape(g.shape[1:])

    shape = g_qkv.shape[1:7]
    back_spec = pl.BlockSpec((1, tokens, tile), lambda j: (j // per_part, 0, j % per_part))
    pltpu.emit_pipeline(
        grad_body,
        grid=(n_qkv,),
        in_specs=[back_spec],
        out_specs=[
            pl.BlockSpec((1,) + shape + (tile,), lambda j: (j // per_part, 0, 0, 0, 0, 0, 0, j % per_part))
        ],
    )(back, g_qkv)
    rs[6].start()
    base += n_qkv
    first_in = base
    acc[...] = jnp.zeros_like(acc)

    def in_body(d, w_one, w_two):
        j = pl.program_id(0)
        turn(first_in + j, first_in, n_qkv)

        @pl.when(j < 3)
        def _():
            acc[...] += dot(d[0], rows_of(w_one), NT)

        @pl.when(j >= 3)
        def _():
            acc[...] += dot(d[0], rows_of(w_two), NT)

    n, two, q, _ = w_first.shape
    pltpu.emit_pipeline(
        in_body,
        grid=(n_qkv,),
        in_specs=[
            pl.BlockSpec((1, tokens, tile), lambda j: (j % 3, 0, j // 3)),
            pl.BlockSpec((n, two, q, tile), lambda j: (0, 0, 0, jnp.minimum(j, 2))),
            pl.BlockSpec((n, two, q, tile), lambda j: (0, 0, 0, jnp.maximum(j - 3, 0))),
        ],
    )(back, w_first, w_second)
    base += n_qkv

    first_one = base
    step = 256
    n_rows = tokens // step

    def norm_one_body(v, m, o):
        i = pl.program_id(0)
        turn(first_one + i, first_one, n_rows)
        rows = pl.ds(pl.multiple_of(i * step, step), step)
        part, gain, shift = norm_back(v[...].astype(F32), small[4:5], acc[rows, :])
        o[...] = m[...] + part
        narrow[4:5] += gain[None]
        narrow[5:6] += shift[None]

    row_spec = pl.BlockSpec((step, width), lambda i: (i, 0))
    pltpu.emit_pipeline(norm_one_body, grid=(n_rows,), in_specs=[row_spec] * 2, out_specs=[row_spec])(
        x, mid_grad, input_grad
    )
    base += n_rows
    for k in range(16):
        at = (k // 4, (k // 2) % 2, k % 2)
        g_vec[at + (pl.ds(0, 8),)] = narrow[:, 128 * (k // 2) : 128 * (k // 2) + 128]
        for i in range(2):
            g_vec[at + (pl.ds(8 + i, 1),)] = wide[:, 256 * k + 128 * i : 256 * k + 128 * i + 128]

    load = pltpu.make_async_copy(middle, acc, csem.at[0])
    load.start()
    first_down = base
    n_down = n_up // 2
    vector_steps = {0: [vectors.start], 1: [vectors.cores], 3: [vectors.over_x]}

    def down_body(a, w):
        j = pl.program_id(0)
        hook(j, vector_steps)
        turn(first_down + j, first_down, n_down)
        out_acc[...] += dot(a[...], rows_of(w))

    pltpu.emit_pipeline(
        down_body,
        grid=(n_down,),
        in_specs=[
            pl.BlockSpec((tokens, tile), lambda j: (0, n_down + j)),
            pl.BlockSpec((blocks, 2, q_down, width), lambda j: (n_down + j, 0, 0, 0)),
        ],
    )(act, w_down)
    base += n_down
    load.wait()
    n_last, step = 4, tokens // 4
    stores = []
    for i in range(n_last):
        rows = pl.ds(i * step, step)
        branch[rows, :] = (acc[rows, :] + (out_acc[rows, :] + small[3:4])).astype(BF16)
        stores.append(pltpu.make_async_copy(branch.at[rows], output.at[rows], csem.at[i]))
        stores[-1].start()
    vectors.over_y()
    for at, stage, k, i in plan:
        if at >= base:
            getattr(rs[k], STAGES[stage])(i)
    vectors.over_z()
    for r in rs + [vectors]:
        r.finish()
    for store in stores:
        store.wait()


def backward_call(weights, x, c, kept, length):
    n1, merged, logsum, attended, middle, n2, act, slope, g_down, small = kept
    tokens, width = x.shape
    hidden = act.shape[1]
    q, q_down = width // 64, hidden // 64
    parts = 2
    low = lambda *shape: jax.ShapeDtypeStruct(shape, BF16)
    full = lambda *shape: jax.ShapeDtypeStruct(shape, F32)
    vmem, any_space = pl.BlockSpec(memory_space=pltpu.VMEM), pl.BlockSpec(memory_space=pl.ANY)
    kinds = [(q_down, width, BF16)] + [(q, hidden // parts, BF16)] * 2 + [(q, width, BF16)] * 4
    scratch = []
    for kind in kinds:
        scratch += Scatter.scratch(*kind)
    scratch += [pltpu.VMEM((2, 2, 2, 2) + kind[:2], kind[2]) for kind in kinds]
    scratch += VectorScatter.scratch()
    scratch += [
        pltpu.VMEM((4, 2, 2, 16, 128), F32),
        pltpu.VMEM((8, width), F32),
        pltpu.VMEM((1, hidden), F32),
        pltpu.VMEM((tokens, width), BF16),
        pltpu.VMEM((tokens, width), BF16),
        pltpu.VMEM((tokens, width), F32),
        pltpu.VMEM((tokens, width), F32),
        pltpu.VMEM((tokens, width), BF16),
        pltpu.VMEM((length, 128), F32),
        pltpu.VMEM((length, 128), F32),
        pltpu.SemaphoreType.DMA((7, RS_SEMS)),
        pltpu.SemaphoreType.DMA((12,)),
        pltpu.SemaphoreType.DMA((4,)),
    ]
    shards = [full(2, 2, q, 3 * width), full(2, 2, q, width), full(2, 2, q, hidden), full(2, 2, q_down, width)]
    outs = pl.pallas_call(
        lambda *refs: backward_kernel(length, PLAN, parts, *refs),
        in_specs=[any_space] * 17 + [vmem],
        out_specs=[any_space] * 2 + [vmem] * 5 + [any_space] * 13,
        out_shape=[low(tokens, width), full(tokens, width)]
        + shards
        + [full(16, 128)]
        + [
            low(3, 4, 2, 2, 2, 2, q, width),
            low(4, 2, 2, 2, 2, q, width),
            low(parts, 4, 2, 2, 2, 2, q, hidden // parts),
            full(tokens, width),
            low(tokens, width),
            low(3, tokens, width),
        ]
        + [jax.ShapeDtypeStruct((4, 2, 2, 2) + kind[:2], kind[2]) for kind in kinds],
        scratch_shapes=scratch,
        compiler_params=pltpu.CompilerParams(
            collective_id=1, has_side_effects=True, vmem_limit_bytes=66 * 10**6
        ),
        name="backward",
    )(*weights, x, c, n1, merged, logsum, attended, middle, n2, act, slope, g_down.reshape(4, 2, 2, 2, 2, q_down, width), small)
    grads = [o.reshape(-1, o.shape[-1]) for o in outs[2:6]]
    return outs[0], outs[1], grads, outs[6]


def forward_plain(x, weights, small, length):
    w_qkv, w_out, w_up, w_down = weights
    b_query, b_value, b_out, b_up, b_down, gain_one, shift_one, gain_two, shift_two = small
    xf = x.astype(F32)
    normed_one = layer_norm(xf, gain_one, shift_one).astype(BF16)
    qkv_bias = jnp.concatenate([b_query, jnp.zeros_like(b_query), b_value])
    merged = (dot(normed_one, w_qkv) + qkv_bias).astype(BF16)
    attended, logsum = attn_fwd(merged, length)
    middle = xf + (dot(attended, w_out) + b_out)
    normed_two = layer_norm(middle, gain_two, shift_two).astype(BF16)
    activated, slope = gelu_pair(dot(normed_two, w_up) + b_up)
    return normed_one, merged, logsum, attended, middle, normed_two, activated.astype(BF16), slope.astype(BF16)


def backward(x, c, weights, small, kept, length):
    w_qkv, w_out, w_up, w_down = weights
    b_down, gain_one, gain_two = small
    normed_one, merged, logsum, attended, middle, normed_two, activated, slope = kept
    width = x.shape[1]
    xf, cf = x.astype(F32), c.astype(F32)
    output = (middle + (dot(activated, w_down) + b_down)).astype(BF16)

    grad_down_bias = jnp.sum(cf, 0)
    hidden_grad = (dot(c, w_down, NT) * slope.astype(F32)).astype(BF16)
    grad_up_bias = jnp.sum(hidden_grad.astype(F32), 0)
    grad_up = dot(normed_two, hidden_grad, TN).astype(BF16)
    part, grad_gain_two, grad_shift_two = norm_back(middle, gain_two, dot(hidden_grad, w_up, NT))
    middle_grad = cf + part
    branch_grad = middle_grad.astype(BF16)
    grad_out_bias = jnp.sum(branch_grad.astype(F32), 0)
    grad_out = dot(attended, branch_grad, TN).astype(BF16)
    attended_grad = dot(branch_grad, w_out, NT).astype(BF16)
    back = attn_bwd(merged, attended_grad, logsum, length)
    grad_query_bias = jnp.sum(back[0].astype(F32), 0)
    grad_value_bias = jnp.sum(back[2].astype(F32), 0)
    grad_qkv = jnp.concatenate([dot(normed_one, back[j], TN).astype(BF16) for j in range(3)], 1)
    normed_one_grad = sum(dot(back[j], w_qkv[:, j * width : (j + 1) * width], NT) for j in range(3))
    part, grad_gain_one, grad_shift_one = norm_back(xf, gain_one, normed_one_grad)
    input_grad = middle_grad + part
    return (
        output,
        input_grad,
        (grad_qkv, grad_out, grad_up),
        (
            grad_query_bias,
            grad_value_bias,
            grad_out_bias,
            grad_up_bias,
            grad_down_bias,
            grad_gain_one,
            grad_shift_one,
            grad_gain_two,
            grad_shift_two,
        ),
    )


def pack_shards(vectors):
    wide = vectors[3]
    narrow = jnp.stack([v for k, v in enumerate(vectors) if k != 3])
    zeros = jnp.zeros_like(narrow)
    odd = lax.axis_index("fsdp") % 2 == 1
    lanes = jnp.concatenate([jnp.where(odd, zeros, narrow), jnp.where(odd, narrow, zeros)], 1)
    rows = jnp.concatenate([lanes, wide.reshape(2, 128)], 0)
    return jnp.pad(rows, ((0, 64 - rows.shape[0]), (0, 0)))


def unpack_shard(packed):
    odd = lax.axis_index("fsdp") % 2 == 1
    narrow = jnp.where(odd, packed[:8, 64:], packed[:8, :64])
    wide = packed[8:10].reshape(256)
    return tuple(narrow[j] for j in range(3)) + (wide,) + tuple(narrow[j] for j in range(3, 8))


def local_ring(block_input, *rest):
    shards, cotangent = rest[:13], rest[13]
    length, width = block_input.shape[1:]
    x, c = block_input.reshape(-1, width), cotangent.reshape(-1, width)
    weights, kept = forward_call(shards[:4] + (pack_shards(shards[4:]),), x, c, length)
    output, input_grad, grads, vec = backward_call(weights, x, c, kept, length)
    whole = (output.reshape(block_input.shape), input_grad.reshape(block_input.shape))
    return whole + tuple(grads) + unpack_shard(vec)


def local_any(block_input, *rest):
    shards, cotangent = rest[:13], rest[13]
    length, width = block_input.shape[1:]
    x, c = block_input.reshape(-1, width), cotangent.reshape(-1, width)
    gathered = [lax.all_gather(shard, "fsdp", axis=0, tiled=True) for shard in shards]
    weights, small = gathered[:4], tuple(v.astype(F32) for v in gathered[4:])
    kept = forward_plain(x, weights, small, length)
    output, input_grad, mats, vecs = backward(x, c, weights, (small[4], small[5], small[7]), kept, length)
    mats += (dot(kept[6], c, TN),)

    def reduce(grad):
        part = lax.psum_scatter(grad.astype(F32), "fsdp", scatter_dimension=0, tiled=True)
        return lax.psum(part, "seq")

    whole = (output.reshape(block_input.shape), input_grad.reshape(block_input.shape))
    return whole + tuple(reduce(grad) for grad in mats + vecs)


def solution(mesh):
    split = P(("fsdp", "seq"), None, None)
    matrix, vector = P("fsdp", None), P("fsdp")
    in_specs = (split,) + (matrix,) * 4 + (vector,) * 9 + (split,)
    out_specs = (split, split) + (matrix,) * 4 + (vector,) * 9
    local = local_ring if (mesh.shape["fsdp"], mesh.shape["seq"]) == (16, 2) else local_any
    return jax.shard_map(local, mesh=mesh, in_specs=in_specs, out_specs=out_specs, check_vma=False)
```

```python
import jax
import jax.numpy as jnp
from jax import lax
from jax.experimental import pallas as pl
from jax.experimental.pallas import tpu as pltpu
from jax.sharding import PartitionSpec as P

EPSILON = 1e-05
NEG_LARGE = -1e30
MESH = pl.DeviceIdType.MESH
NN = (((1,), (0,)), ((), ()))
NT = (((1,), (1,)), ((), ()))
TN = (((0,), (0,)), ((), ()))
BF16 = jnp.bfloat16
F32 = jnp.float32
VMEM_LIMIT = 60 * 2**20


def dot(left, right, dims=NN):
    return lax.dot_general(left, right, dims, preferred_element_type=F32)


class Place:
    def __init__(self):
        f = lax.axis_index("fsdp")
        self.c = lax.axis_index("seq")
        self.z, self.y, self.x = f // 4, (f // 2) % 2, f % 2

    def block(self, z, y, x):
        return z * 4 + y * 2 + x

    def dev(self, z, y, x):
        return (self.block(z, y, x), self.c)

    @property
    def xn(self):
        return self.dev(self.z, self.y, 1 - self.x)

    @property
    def yn(self):
        return self.dev(self.z, 1 - self.y, self.x)

    @property
    def up(self):
        return self.dev(self.z + 1, self.y, self.x)

    @property
    def down(self):
        return self.dev(self.z - 1, self.y, self.x)

    @property
    def partner(self):
        return (self.block(self.z, self.y, self.x), 1 - self.c)


def greet(p):
    barrier = pltpu.get_barrier_semaphore()

    def signal(device):
        pl.semaphore_signal(barrier, inc=1, device_id=device, device_id_type=MESH)

    for device in (p.xn, p.yn, p.partner):
        signal(device)

    @pl.when(p.z < 3)
    def _():
        signal(p.up)

    @pl.when(p.z > 0)
    def _():
        signal(p.down)

    inner = jnp.logical_and(p.z > 0, p.z < 3)

    @pl.when(inner)
    def _():
        pl.semaphore_wait(barrier, 5)

    @pl.when(jnp.logical_not(inner))
    def _():
        pl.semaphore_wait(barrier, 4)


def greet_column(p):
    barrier = pltpu.get_barrier_semaphore()
    column = [p.dev((p.z + k) % 4, p.y, p.x) for k in (1, 2, 3)]
    for device in [p.xn, p.yn, p.partner] + column:
        pl.semaphore_signal(barrier, inc=1, device_id=device, device_id_type=MESH)
    pl.semaphore_wait(barrier, 6)


def remote(src, dst, send, recv, device):
    return pltpu.make_async_remote_copy(
        src_ref=src, dst_ref=dst, send_sem=send, recv_sem=recv, device_id=device, device_id_type=MESH
    )


def wait_bytes(ref, sem):
    pltpu.make_async_copy(ref, ref, sem).wait()


AG_SEMS = 24


class Gather:
    def __init__(self, p, src, dst, sems):
        self.p, self.src, self.dst, self.sems = p, src, dst, sems
        self.rz = [None] * 4
        self.send, self.zsend, self.local, self.rp = (sems.at[20], sems.at[21], sems.at[22], sems.at[23])

    def half(self, z, y, x):
        return self.dst.at[2 * self.p.block(z, y, x) + self.p.c]

    def to(self, src, dst, recv, device, send=None):
        remote(src, dst, self.send if send is None else send, self.sems.at[recv], device).start()

    def spread(self, src, z):
        p = self.p
        mine = self.half(z, p.y, p.x)
        self.to(src, mine, 4 + z, p.xn)
        self.to(src, mine, 8 + z, p.yn)

    def along(self, src, z, up):
        p = self.p
        mine = self.half(z, p.y, p.x)

        @pl.when(p.z < 3 if up else p.z > 0)
        def _():
            self.to(src, mine, z, p.up if up else p.down, self.zsend)

    def start(self):
        p = self.p
        own = self.src.at[p.c]
        self.along(own, p.z, True)
        self.along(own, p.z, False)
        me = p.block(p.z, p.y, p.x)
        pltpu.make_async_copy(self.src, self.dst.at[pl.ds(2 * me, 2)], self.local).start()

    def at_distance(self, s, body):
        p = self.p
        if s == 0:
            body(p.z, None)
            return

        @pl.when(p.z - s >= 0)
        def _():
            body(p.z - s, True)

        @pl.when(p.z + s <= 3)
        def _():
            body(p.z + s, False)

    def z_step(self, s):
        p = self.p
        if s == 0:
            self.start()
            return

        def body(z, up):
            mine = self.half(z, p.y, p.x)
            wait_bytes(mine, self.sems.at[z])
            self.along(mine, z, up)
            self.to(mine, mine, 23, p.partner)

        self.at_distance(s, body)

    def spread_step(self, s):
        p = self.p

        def body(z, up):
            self.spread(self.src.at[p.c] if s == 0 else self.half(z, p.y, p.x), z)

        self.at_distance(s, body)

    def xy_step(self, s):
        p = self.p

        def body(z, up):
            a = self.half(z, p.y, 1 - p.x)
            wait_bytes(a, self.sems.at[4 + z])
            self.to(a.at[0], a.at[0], 12 + z, p.yn)
            self.to(a, a, 23, p.partner)
            b = self.half(z, 1 - p.y, p.x)
            wait_bytes(b, self.sems.at[8 + z])
            self.to(b.at[1], b.at[1], 16 + z, p.xn)
            self.to(b, b, 23, p.partner)

        self.at_distance(s, body)

    def diag_step(self, s):
        p = self.p

        def body(z, up):
            d = self.half(z, 1 - p.y, 1 - p.x)
            wait_bytes(d.at[0], self.sems.at[12 + z])
            wait_bytes(d.at[1], self.sems.at[16 + z])
            self.to(d, d, 23, p.partner)

        self.at_distance(s, body)

    def arrived(self):
        wait_bytes(self.dst.at[pl.ds(0, 15)], self.rp)
        wait_bytes(self.dst.at[pl.ds(0, 2)], self.local)

    def drain(self):
        p = self.p
        wait_bytes(self.dst.at[pl.ds(0, 27)], self.send)
        inner = jnp.logical_and(p.z > 0, p.z < 3)

        @pl.when(inner)
        def _():
            wait_bytes(self.dst.at[pl.ds(0, 5)], self.zsend)

        @pl.when(jnp.logical_not(inner))
        def _():
            wait_bytes(self.dst.at[pl.ds(0, 1)], self.zsend)


GATHER_STAGES = ("z_step", "spread_step", "xy_step", "diag_step")


def hook(index, table):
    keys = sorted(table)
    if len(keys) <= 1:
        for k in keys:

            @pl.when(index == k)
            def _(k=k):
                for step in table[k]:
                    step()

        return
    middle = keys[len(keys) // 2]

    @pl.when(index < middle)
    def _():
        hook(index, {k: table[k] for k in keys if k < middle})

    @pl.when(index >= middle)
    def _():
        hook(index, {k: table[k] for k in keys if k >= middle})


RS_SEMS = 44


class Scatter:
    def __init__(self, p, g, out, pr, bufs, tmp, sems):
        self.p, self.g, self.out, self.pr, self.tmp, self.sems = p, g, out, pr, tmp, sems
        self.o, self.x1, self.y1, self.x2, self.y2, self.u, self.d = bufs
        self.psend, self.zsend, self.fsend, self.frecv = (sems.at[36 + i] for i in range(4))

    @staticmethod
    def scratch(q, width, dtype):
        shapes = [(4, 2, 2, 2), (4, 2), (4, 2), (4,), (4,), (4, 2), (4, 2)]
        return [pltpu.VMEM(shape + (q, width), dtype) for shape in shapes]

    def level(self, i):
        z = self.p.z
        return jnp.where(z < 2, 3 - i, i)

    def sem(self, kind, i):
        return self.sems.at[4 * kind + i]

    def start(self):
        p = self.p
        for i in range(4):
            z = self.level(i)
            theirs = self.g.at[z, :, :, 1 - p.c]
            remote(theirs, self.pr.at[z], self.psend, self.sem(0, i), p.partner).start()
            pltpu.make_async_copy(self.g.at[z, :, :, p.c], self.o.at[z], self.sem(1, i)).start()

    def fetch(self, i):
        z = self.level(i)
        wait_bytes(self.pr.at[z], self.sem(0, i))
        pltpu.make_async_copy(self.pr.at[z], self.tmp.at[i % 2], self.sems.at[40 + i]).start()

    def stage0(self, i):
        p = self.p
        z = self.level(i)
        wait_bytes(self.o.at[z], self.sem(1, i))
        if self.tmp is None:
            theirs = self.pr.at[z]
            wait_bytes(theirs, self.sem(0, i))
        else:
            theirs = self.tmp.at[i % 2]
            wait_bytes(theirs, self.sems.at[40 + i])

        self.o[z] = self.o[z] + theirs[...]
        remote(self.o.at[z, :, 1 - p.x, 0], self.x1.at[z], self.sems.at[32], self.sem(2, i), p.xn).start()
        remote(self.o.at[z, 1 - p.y, :, 1], self.y1.at[z], self.sems.at[33], self.sem(3, i), p.yn).start()

    def stage1(self, i):
        p = self.p
        z = self.level(i)
        wait_bytes(self.x1.at[z], self.sem(2, i))
        for y in range(2):
            self.o[z, y, p.x, 0] = self.o[z, y, p.x, 0] + self.x1[z, y]
        remote(self.o.at[z, 1 - p.y, p.x, 0], self.y2.at[z], self.sems.at[35], self.sem(4, i), p.yn).start()
        wait_bytes(self.y1.at[z], self.sem(3, i))
        for x in range(2):
            self.o[z, p.y, x, 1] = self.o[z, p.y, x, 1] + self.y1[z, x]
        remote(self.o.at[z, p.y, 1 - p.x, 1], self.x2.at[z], self.sems.at[34], self.sem(5, i), p.xn).start()

    def along(self, z, up):
        p = self.p
        buf, kind = (self.u, 6) if up else (self.d, 7)
        remote(
            self.o.at[z, p.y, p.x], buf.at[z], self.zsend, self.sems.at[4 * kind + z], p.up if up else p.down
        ).start()

    def chain(self, z, up):
        p = self.p
        buf, kind = (self.u, 6) if up else (self.d, 7)
        wait_bytes(buf.at[z], self.sems.at[4 * kind + z])
        self.o[z, p.y, p.x] = self.o[z, p.y, p.x] + buf[z]
        self.along(z, up)

    def stage2(self, i):
        p = self.p
        z = self.level(i)
        wait_bytes(self.y2.at[z], self.sem(4, i))
        wait_bytes(self.x2.at[z], self.sem(5, i))
        self.o[z, p.y, p.x, 0] = self.o[z, p.y, p.x, 0] + self.y2[z]
        self.o[z, p.y, p.x, 1] = self.o[z, p.y, p.x, 1] + self.x2[z]

        @pl.when(jnp.logical_and(p.z == 0, z > 0))
        def _():
            self.along(z, True)

        @pl.when(jnp.logical_and(p.z == 3, z < 3))
        def _():
            self.along(z, False)

    def stage3(self, i):
        p = self.p
        z = self.level(i)
        inner = jnp.logical_and(p.z > 0, p.z < 3)

        @pl.when(jnp.logical_and(inner, z > p.z))
        def _():
            self.chain(z, True)

        @pl.when(jnp.logical_and(inner, z < p.z))
        def _():
            self.chain(z, False)

    def stage4(self, i=0):
        p = self.p
        z = p.z
        self.out[p.c] = self.o[z, p.y, p.x].astype(F32)

        @pl.when(z > 0)
        def _():
            wait_bytes(self.u.at[z], self.sems.at[24 + z])
            self.out[p.c] = self.out[p.c] + self.u[z].astype(F32)

        @pl.when(z < 3)
        def _():
            wait_bytes(self.d.at[z], self.sems.at[28 + z])
            self.out[p.c] = self.out[p.c] + self.d[z].astype(F32)

        remote(self.out.at[p.c], self.out.at[p.c], self.fsend, self.frecv, p.partner).start()

    def finish(self):
        p = self.p
        wait_bytes(self.out.at[1 - p.c], self.frecv)
        wait_bytes(self.out.at[p.c], self.fsend)
        wait_bytes(self.o, self.psend)
        for k, ref in enumerate((self.x1, self.y1, self.x2, self.y2)):
            wait_bytes(ref, self.sems.at[32 + k])
        wait_bytes(self.u.at[pl.ds(0, 3)], self.zsend)


class VectorScatter:
    def __init__(self, p, g, out, bufs, sems):
        self.p, self.g, self.out, self.sems = p, g, out, sems
        self.pv, self.xv, self.yv, self.zv, self.t1, self.t2, self.t3 = bufs

    @staticmethod
    def scratch():
        shapes = [(4, 2, 2), (4, 2), (4,), (4,), (4, 2, 2), (4, 2), (4,)]
        return [pltpu.VMEM(shape + (16, 128), F32) for shape in shapes]

    def start(self):
        remote(self.g, self.pv, self.sems.at[0], self.sems.at[1], self.p.partner).start()

    def cores(self):
        p = self.p
        wait_bytes(self.pv, self.sems.at[1])
        self.t1[...] = self.g[...] + self.pv[...]
        remote(self.t1.at[:, :, 1 - p.x], self.xv, self.sems.at[2], self.sems.at[3], p.xn).start()

    def over_x(self):
        p = self.p
        wait_bytes(self.xv, self.sems.at[3])
        self.t2[...] = self.t1[:, :, p.x] + self.xv[...]
        remote(self.t2.at[:, 1 - p.y], self.yv, self.sems.at[4], self.sems.at[5], p.yn).start()

    def over_y(self):
        p = self.p
        wait_bytes(self.yv, self.sems.at[5])
        self.t3[...] = self.t2[:, p.y] + self.yv[...]
        for k in (1, 2, 3):
            z = (p.z + k) % 4
            there = p.dev(z, p.y, p.x)
            remote(self.t3.at[z], self.zv.at[p.z], self.sems.at[6], self.sems.at[8 + p.z], there).start()

    def over_z(self):
        p = self.p
        total = self.t3[p.z]
        for k in (1, 2, 3):
            z = (p.z + k) % 4
            wait_bytes(self.zv.at[z], self.sems.at[8 + z])
            total = total + self.zv[z]
        narrow = lax.broadcasted_iota(jnp.int32, total.shape, 0) < 8
        moved = jnp.logical_and(narrow, p.x == 1)
        self.out[...] = jnp.where(moved, pltpu.roll(total, 64, 1), total)

    def finish(self):
        wait_bytes(self.g, self.sems.at[0])
        wait_bytes(self.xv, self.sems.at[2])
        wait_bytes(self.yv, self.sems.at[4])
        wait_bytes(self.zv.at[pl.ds(0, 3)], self.sems.at[6])


def lane_masks(rows, width, dtype=BF16):
    lanes = lax.broadcasted_iota(jnp.int32,(rows,width),1)
    return lanes < width//2
def pick(h, low, v):
    z=jnp.zeros_like(v)
    return jnp.where(low, v, z) if h==0 else jnp.where(low, z, v)
def fwd_body(q_ref,k_ref,v_ref,o_ref,l_ref, B):
    S=q_ref.shape[0]
    low=lane_masks(S,128)
    q=q_ref[...]*BF16(0.125); k=k_ref[...]; v=v_ref[...]
    qs=[pick(h,low,q) for h in (0,1)]; vs=[pick(h,low,v) for h in (0,1)]
    for b in range(S//B):
        end=(b+1)*B
        acc=None
        for h in (0,1):
            st=dot(k[:end],qs[h][b*B:end],NT)
            key=lax.broadcasted_iota(jnp.int32,(B,B),0); qry=lax.broadcasted_iota(jnp.int32,(B,B),1)
            diag=jnp.where(key<=qry, st[b*B:end], NEG_LARGE)
            st=jnp.concatenate([st[:b*B],diag],0) if b else diag
            m=jnp.max(st,0,keepdims=True)
            p=jnp.exp(st-m)
            l=jnp.sum(p,0,keepdims=True)
            l_ref[h:h+1,b*B:end]=m+jnp.log(l)
            pt=(p*(1.0/l)).astype(BF16)
            o=dot(pt,vs[h][:end],TN)
            acc=o if acc is None else acc+o
        o_ref[b*B:end,:]=acc.astype(BF16)
def bwd_body(q_ref, k_ref, v_ref, g_ref, l_ref, dq_ref, dk_ref, dv_ref, dk_acc, dv_acc, B):
    S = q_ref.shape[0]
    low = lane_masks(S, 128)
    q = q_ref[...] * BF16(0.125)
    k, v, g = k_ref[...], v_ref[...], g_ref[...]
    qs, gs, ks = ([pick(h, low, t) for h in (0, 1)] for t in (q, g, k))
    key = lax.broadcasted_iota(jnp.int32, (B, B), 0)
    query = lax.broadcasted_iota(jnp.int32, (B, B), 1)
    blocks = list(reversed(range(S // B)))
    scores, grads = {}, {}
    for b in blocks:
        end = (b + 1) * B
        for h in (0, 1):
            scores[b, h] = dot(k[:end], qs[h][b * B : end], NT)
            grads[b, h] = dot(v[:end], gs[h][b * B : end], NT)
    for b in blocks:
        end = (b + 1) * B
        dq = dk = dv = None
        for h in (0, 1):
            qb, gb = qs[h][b * B : end], gs[h][b * B : end]
            p = jnp.exp(scores[b, h] - l_ref[h : h + 1, b * B : end])
            diag = jnp.where(key <= query, p[b * B : end], 0.0)
            p = jnp.concatenate([p[: b * B], diag], 0) if b else diag
            inner = jnp.sum(p * grads[b, h], 0, keepdims=True)
            ds = (p * (grads[b, h] - inner)).astype(BF16)
            parts = dot(ds, ks[h][:end], TN), dot(ds, qb, NN), dot(p.astype(BF16), gb, NN)
            dq, dk, dv = parts if h == 0 else (dq + parts[0], dk + parts[1], dv + parts[2])
        dq_ref[b * B : end, :] = (dq * 0.125).astype(BF16)
        if b == S // B - 1:
            dk_acc[...] = dk
            dv_acc[...] = dv
        else:
            dk_acc[:end, :] += dk
            dv_acc[:end, :] += dv
    dk_ref[...] = dk_acc[...].astype(BF16)
    dv_ref[...] = dv_acc[...].astype(BF16)


def attn_fwd(merged, S, B=256):
    T=merged.shape[0]; D=merged.shape[1]//3; n=D//128
    def body(q,k,v,o,l): fwd_body(q,k,v,o,l.at[0,0],B)
    sp=lambda off: pl.BlockSpec((S,128),lambda s,h: (s,off+h))
    return pl.pallas_call(body,grid=(T//S,n),in_specs=[sp(0),sp(n),sp(2*n)],
        out_specs=[pl.BlockSpec((S,128),lambda s,h:(s,h)),pl.BlockSpec((1,1,2,S),lambda s,h:(s,h,0,0))],
        out_shape=[jax.ShapeDtypeStruct((T,D),BF16),jax.ShapeDtypeStruct((T//S,n,2,S),F32)],
        name="attn_fwd",compiler_params=pltpu.CompilerParams(vmem_limit_bytes=40*2**20))(merged,merged,merged)
def attn_bwd(merged, g, lse, S, B=256):
    T=merged.shape[0]; D=merged.shape[1]//3; n=D//128
    def body(q,k,v,gr,l,d,dka,dva): bwd_body(q,k,v,gr,l.at[0,0],d.at[0],d.at[1],d.at[2],dka,dva,B)
    sp=lambda off: pl.BlockSpec((S,128),lambda s,h: (s,off+h))
    return pl.pallas_call(body,grid=(T//S,n),in_specs=[sp(0),sp(n),sp(2*n),sp(0),pl.BlockSpec((1,1,2,S),lambda s,h:(s,h,0,0))],
        out_specs=pl.BlockSpec((3,S,128),lambda s,h:(0,s,h)),
        out_shape=jax.ShapeDtypeStruct((3,T,D),BF16),
        scratch_shapes=[pltpu.VMEM((S,128),F32)]*2,
        name="attn_bwd",compiler_params=pltpu.CompilerParams(vmem_limit_bytes=40*2**20))(merged,merged,merged,g,lse)


def layer_norm(values, gain, shift):
    center = values - jnp.mean(values, -1, keepdims=True)
    spread = jnp.mean(center * center, -1, keepdims=True)
    return center * lax.rsqrt(spread + EPSILON) * gain + shift


def norm_back(values, gain, grad):
    center = values - jnp.mean(values, -1, keepdims=True)
    inverse = lax.rsqrt(jnp.mean(center * center, -1, keepdims=True) + EPSILON)
    unit = center * inverse
    scaled = grad * gain
    first = jnp.mean(scaled, -1, keepdims=True)
    second = jnp.mean(scaled * unit, -1, keepdims=True)
    return (inverse * (scaled - first - unit * second), jnp.sum(grad * unit, 0), jnp.sum(grad, 0))


def gelu_pair(u):
    a = 0.7978845608028654
    square = u * u
    half = 0.5 + 0.5 * jnp.tanh(u * (a + (a * 0.044715) * square))
    value = u * half
    slope = half + value * (1.0 - half) * (2.0 * a + (6.0 * a * 0.044715) * square)
    return value, slope


def whole_spec(ref, tile=None, first=0):
    n, two, q, width = ref.shape
    if tile is None:
        return pl.BlockSpec((n, two, q, width), lambda j: (0, 0, 0, 0))
    return pl.BlockSpec((n, two, q, tile), lambda j: (0, 0, 0, first + j))


def rows_of(block):
    value = block[...]
    return value.reshape(-1, value.shape[-1])


GATHER_PLAN = (
    (0, 0, 1, 0), (0, 1, 1, 0), (0, 0, 0, 0), (0, 0, 2, 0), (0, 1, 0, 0), (0, 1, 2, 0), (0, 0, 0, 1), (0, 2, 1, 0),
    (0, 0, 1, 1), (0, 2, 0, 0), (0, 1, 0, 1), (0, 1, 1, 1), (0, 0, 2, 1), (0, 2, 2, 0), (0, 0, 0, 2), (0, 1, 0, 2),
    (0, 0, 1, 2), (0, 1, 1, 2), (0, 2, 0, 1), (0, 0, 3, 0), (0, 3, 0, 0), (0, 0, 0, 3), (0, 0, 2, 2), (0, 2, 0, 2),
    (0, 1, 2, 2), (0, 0, 1, 3), (0, 1, 0, 3), (0, 3, 1, 0), (0, 2, 1, 2), (0, 1, 1, 3), (0, 0, 5, 0), (0, 3, 0, 1),
    (0, 3, 0, 2), (0, 0, 3, 1), (0, 2, 0, 3), (0, 0, 2, 3), (0, 1, 2, 3), (0, 3, 0, 3), (0, 2, 1, 1), (0, 2, 1, 3),
    (0, 1, 3, 0), (0, 1, 2, 1), (0, 0, 4, 0), (0, 1, 3, 1), (0, 0, 6, 0), (1, 3, 1, 1), (1, 3, 1, 3), (1, 1, 5, 0),
    (1, 3, 1, 2), (1, 2, 2, 3), (1, 0, 3, 2), (1, 2, 2, 2), (1, 2, 3, 0), (2, 0, 4, 1), (2, 1, 3, 2), (3, 2, 2, 1),
    (5, 1, 4, 0), (6, 2, 3, 1), (6, 0, 5, 1), (6, 0, 4, 2), (7, 3, 2, 2), (7, 1, 4, 1), (9, 2, 5, 0), (9, 3, 2, 3),
    (10, 1, 4, 2), (10, 3, 2, 0), (10, 0, 5, 2), (10, 3, 2, 1), (10, 3, 3, 0), (11, 0, 6, 1), (11, 2, 3, 2), (11, 0, 3, 3),
    (12, 1, 3, 3), (12, 0, 4, 3), (12, 1, 4, 3), (12, 1, 5, 2), (14, 0, 5, 3), (16, 0, 6, 2), (16, 2, 4, 0), (17, 2, 4, 3),
    (17, 2, 3, 3), (18, 1, 5, 1), (19, 2, 4, 2), (20, 2, 4, 1), (20, 3, 3, 2), (21, 3, 3, 3), (21, 3, 3, 1), (22, 1, 5, 3),
    (22, 2, 5, 2), (22, 0, 6, 3), (24, 3, 4, 0), (25, 2, 5, 1), (25, 3, 4, 3), (25, 1, 6, 1), (25, 2, 5, 3), (26, 3, 4, 2),
    (26, 1, 6, 3), (26, 3, 4, 1), (26, 1, 6, 0), (27, 3, 5, 2), (29, 3, 5, 3), (29, 3, 5, 1), (29, 1, 6, 2), (30, 3, 5, 0),
    (34, 2, 6, 0), (36, 2, 6, 1), (36, 2, 6, 2), (36, 2, 6, 3), (38, 3, 6, 0), (41, 3, 6, 1), (42, 3, 6, 2), (42, 3, 6, 3),
)


def forward_kernel(length, plan, *refs):
    (s_qkv, s_out, s_up, s_down, s_vec), refs = refs[:5], refs[5:]
    x, c = refs[:2]
    (w_qkv, w_out, w_up, w_down, w_vec), refs = refs[2:7], refs[7:]
    n1, merged, logsum, attended, middle, n2, act, slope, grad_down, small, refs = refs[:10] + (refs[10:],)
    b_up, qkv_bias, vec, x_ref, c_ref, n1_ref, n2_ref, first_half, second_half, sems, local = refs
    tokens, width = x_ref.shape
    p = Place()
    for part, half in enumerate((first_half, second_half)):
        for k in range(3):
            columns = pl.ds(k * width + part * width // 2, width // 2)
            half[:, :, :, pl.ds(k * width // 2, width // 2)] = s_qkv[:, :, :, columns]
    greet(p)
    n_half = s_up.shape[3] // 2
    lows, highs = (s_up.at[:, :, :, pl.ds(k * n_half, n_half)] for k in (0, 1))
    columns = 3 * width // 2
    pieces = [
        (s_vec, w_vec),
        (first_half, w_qkv.at[:, :, :, pl.ds(0, columns)]),
        (second_half, w_qkv.at[:, :, :, pl.ds(columns, columns)]),
        (s_out, w_out),
        (lows, w_up.at[:, :, :, pl.ds(0, n_half)]),
        (highs, w_up.at[:, :, :, pl.ds(n_half, n_half)]),
        (s_down, w_down),
    ]
    gathers = [Gather(p, source, whole, sems.at[i]) for i, (source, whole) in enumerate(pieces)]
    g_vec, g_first, g_second, g_out, g_low, g_high, g_down = gathers

    def steps(at):
        return [
            lambda stage=stage, w=w, s=s: getattr(gathers[w], GATHER_STAGES[stage])(s)
            for when, stage, w, s in plan
            if when == at
        ]

    def run(at):
        for step in steps(at):
            step()

    def turn(index, first, count, skip=0):
        hook(index, {k: steps(first + k) for k in range(skip, count) if steps(first + k)})

    loads = [pltpu.make_async_copy(x, x_ref, local.at[0]), pltpu.make_async_copy(c, c_ref, local.at[1])]
    for load in loads:
        load.start()
    run(0)
    g_vec.arrived()
    load = pltpu.make_async_copy(w_vec, vec, local.at[2])
    load.start()
    load.wait()
    for load in loads:
        load.wait()
    for k in range(8):
        small[:, pl.ds(128 * k, 128)] = (vec[4 * k, 0, :8] + vec[4 * k + 2, 0, :8]).astype(F32)
    for k in range(16):
        for i in range(2):
            b_up[:, pl.ds(256 * k + 128 * i, 128)] = vec[2 * k, 0, 8 + i : 9 + i].astype(F32)
    qkv_bias[:, :width] = small[0:1]
    qkv_bias[:, width : 2 * width] = jnp.zeros_like(small[0:1])
    qkv_bias[:, 2 * width :] = small[1:2]

    def norm_rows(i, carry):
        rows = pl.ds(i * 128, 128)
        n1_ref[rows, :] = layer_norm(x_ref[rows, :].astype(F32), small[4:5], small[5:6]).astype(BF16)
        return carry

    lax.fori_loop(0, tokens // 128, norm_rows, 0)
    store_n1 = pltpu.make_async_copy(n1_ref, n1, local.at[0])
    store_n1.start()
    base = 1
    tile = 512

    halves = width // tile
    pairs = width // 128 // halves
    n_attend = (tokens // length) * pairs

    def head_spec(off):
        return pl.BlockSpec((length, 128), lambda s, h: (s, off + h))

    for part, g in enumerate((g_first, g_second)):
        run(base)
        g.arrived()

        def qkv_body(w_ref, o_ref, first=base, part=part):
            j = pl.program_id(0)
            turn(j, first, 3, 1)
            at = pl.ds(pl.multiple_of((j * halves + part) * tile, tile), tile)
            o_ref[...] = (dot(n1_ref[...], rows_of(w_ref)) + qkv_bias[:, at]).astype(BF16)

        pltpu.emit_pipeline(
            qkv_body,
            grid=(3,),
            in_specs=[whole_spec(w_qkv, tile, 3 * part)],
            out_specs=[pl.BlockSpec((tokens, tile), lambda j, part=part: (0, j * halves + part))],
        )(w_qkv, merged)
        base += 3

        def attend_body(q, k, v, o, l, first=base):
            s, h = pl.program_id(0), pl.program_id(1)
            turn(s * pairs + h, first, n_attend)
            fwd_body(q, k, v, o, l.at[0, 0], 256)

        off = part * pairs
        third = width // 128
        pltpu.emit_pipeline(
            attend_body,
            grid=(tokens // length, pairs),
            in_specs=[head_spec(off), head_spec(third + off), head_spec(2 * third + off)],
            out_specs=[
                head_spec(off),
                pl.BlockSpec((1, 1, 2, length), lambda s, h, off=off: (s, off + h, 0, 0)),
            ],
        )(merged, merged, merged, attended, logsum)
        base += n_attend

    run(base)
    g_out.arrived()
    n_out, first_out = tokens // 256, base

    def out_body(a_ref, w_ref, m_ref):
        i = pl.program_id(0)
        turn(i, first_out, n_out, 1)
        rows = pl.ds(pl.multiple_of(i * 256, 256), 256)
        value = x_ref[rows, :].astype(F32) + (dot(a_ref[...], rows_of(w_ref)) + small[2:3])
        m_ref[...] = value
        n2_ref[rows, :] = layer_norm(value, small[6:7], small[7:8]).astype(BF16)

    pltpu.emit_pipeline(
        out_body,
        grid=(tokens // 256,),
        in_specs=[pl.BlockSpec((256, width), lambda i: (i, 0)), whole_spec(w_out)],
        out_specs=[pl.BlockSpec((256, width), lambda i: (i, 0))],
    )(attended, w_out, middle)

    store_n2 = pltpu.make_async_copy(n2_ref, n2, local.at[1])
    store_n2.start()
    base += n_out
    n_up = act.shape[1] // tile
    n_part = n_up // 2
    for part, g in enumerate((g_low, g_high)):
        run(base)
        g.arrived()

        def up_body(w_ref, a_ref, s_ref, first=base, part=part):
            j = pl.program_id(0)
            turn(j, first, n_part, 1)
            bias = b_up[:, pl.ds(pl.multiple_of((part * n_part + j) * tile, tile), tile)]
            value, grad = gelu_pair(dot(n2_ref[...], rows_of(w_ref)) + bias)
            a_ref[...] = value.astype(BF16)
            s_ref[...] = grad.astype(BF16)

        column_spec = pl.BlockSpec((tokens, tile), lambda j, part=part: (0, part * n_part + j))
        pltpu.emit_pipeline(
            up_body,
            grid=(n_part,),
            in_specs=[whole_spec(w_up, tile, part * n_part)],
            out_specs=[column_spec, column_spec],
        )(w_up, act, slope)
        base += n_part

    first_grad = base

    def grad_body(a_ref, o_ref):
        turn(pl.program_id(0), first_grad, n_up)
        o_ref[...] = dot(a_ref[...], c_ref[...], TN).astype(BF16)

    pltpu.emit_pipeline(
        grad_body,
        grid=(n_up,),
        in_specs=[pl.BlockSpec((tokens, tile), lambda j: (0, j))],
        out_specs=[pl.BlockSpec((tile, width), lambda j: (j, 0))],
    )(act, grad_down)
    run(base + n_up)
    g_down.arrived()
    for g in gathers:
        g.drain()
    store_n1.wait()
    store_n2.wait()


def forward_call(shards, x, c, length):
    tokens, width = x.shape
    hidden = 16 * shards[3].shape[0]
    views = [s.reshape(2, 2, s.shape[0] // 4, s.shape[1]) for s in shards]
    q = views[0].shape[2]
    whole = [jax.ShapeDtypeStruct((32,) + v.shape[1:], BF16) for v in views]
    vmem, any_space = pl.BlockSpec(memory_space=pltpu.VMEM), pl.BlockSpec(memory_space=pl.ANY)
    low = lambda *shape: jax.ShapeDtypeStruct(shape, BF16)
    outs = pl.pallas_call(
        lambda *refs: forward_kernel(length, GATHER_PLAN, *refs),
        in_specs=[vmem] * 5 + [any_space] * 2,
        out_specs=[any_space] * 14 + [vmem],
        out_shape=whole
        + [
            low(tokens, width),
            low(tokens, 3 * width),
            jax.ShapeDtypeStruct((tokens // length, width // 128, 2, length), F32),
            low(tokens, width),
            jax.ShapeDtypeStruct((tokens, width), F32),
            low(tokens, width),
            low(tokens, hidden),
            low(tokens, hidden),
            low(hidden, width),
            jax.ShapeDtypeStruct((8, width), F32),
        ],
        scratch_shapes=[
            pltpu.VMEM((1, hidden), F32),
            pltpu.VMEM((1, 3 * width), F32),
            pltpu.VMEM(whole[4].shape, BF16),
            pltpu.VMEM((tokens, width), BF16),
            pltpu.VMEM((tokens, width), BF16),
            pltpu.VMEM((tokens, width), BF16),
            pltpu.VMEM((tokens, width), BF16),
            pltpu.VMEM((2, 2, q, 3 * width // 2), BF16),
            pltpu.VMEM((2, 2, q, 3 * width // 2), BF16),
            pltpu.SemaphoreType.DMA((7, AG_SEMS)),
            pltpu.SemaphoreType.DMA((3,)),
        ],
        compiler_params=pltpu.CompilerParams(collective_id=0, has_side_effects=True, vmem_limit_bytes=VMEM_LIMIT),
        name="forward",
    )(*views, x, c)
    return outs[:4], outs[5:]


PLAN = (
    (4, 0, 0, 0), (7, 1, 0, 0), (7, 0, 0, 1), (9, 0, 0, 2), (11, 1, 0, 1), (11, 0, 0, 3), (13, 1, 0, 2), (18, 2, 0, 0),
    (18, 1, 0, 3), (20, 0, 1, 1), (21, 2, 0, 2), (22, 2, 0, 1), (25, 3, 0, 0), (27, 1, 1, 1), (28, 0, 2, 0), (28, 0, 1, 0),
    (30, 0, 2, 1), (30, 1, 2, 0), (32, 1, 1, 0), (32, 1, 2, 1), (34, 0, 1, 2), (35, 1, 1, 2), (35, 2, 2, 0), (35, 3, 0, 1),
    (35, 2, 1, 1), (37, 0, 2, 3), (39, 1, 2, 3), (39, 0, 2, 2), (39, 0, 1, 3), (40, 4, 0, 0), (40, 1, 1, 3), (40, 1, 2, 2),
    (40, 3, 1, 1), (40, 2, 2, 1), (40, 1, 3, 1), (41, 1, 3, 0), (46, 2, 1, 0), (47, 3, 0, 2), (48, 2, 1, 2), (48, 2, 0, 3),
    (48, 2, 2, 3), (49, 1, 3, 3), (50, 2, 3, 0), (50, 3, 1, 0), (51, 1, 3, 2), (53, 2, 1, 3), (54, 2, 3, 1), (54, 4, 1, 0),
    (55, 2, 3, 3), (55, 2, 3, 2), (55, 2, 2, 2), (57, 1, 4, 0), (57, 3, 0, 3), (57, 1, 4, 1), (57, 4, 0, 1), (57, 3, 2, 0),
    (58, 1, 4, 2), (58, 4, 1, 1), (58, 3, 3, 3), (58, 3, 2, 1), (58, 3, 3, 1), (59, 1, 5, 1), (59, 3, 3, 0), (59, 3, 2, 2),
    (59, 1, 5, 0), (59, 1, 4, 3), (61, 2, 4, 0), (61, 3, 1, 3), (61, 1, 6, 0), (62, 3, 1, 2), (62, 4, 1, 3), (62, 2, 5, 0),
    (62, 4, 0, 3), (62, 1, 6, 1), (62, 3, 2, 3), (62, 1, 5, 3), (62, 4, 2, 1), (62, 4, 2, 0), (62, 4, 3, 1), (62, 2, 5, 1),
    (64, 2, 6, 0), (64, 2, 4, 1), (64, 3, 5, 0), (64, 3, 4, 0), (65, 1, 5, 2), (66, 2, 6, 1), (66, 2, 4, 3), (66, 4, 2, 3),
    (66, 4, 3, 0), (66, 1, 6, 2), (66, 2, 4, 2), (66, 3, 5, 1), (66, 3, 3, 2), (66, 1, 6, 3), (66, 2, 5, 3), (66, 4, 5, 0),
    (67, 2, 5, 2), (67, 3, 6, 0), (67, 4, 4, 0), (67, 3, 4, 1), (68, 4, 3, 3), (68, 2, 6, 2), (68, 3, 6, 1), (69, 4, 6, 0),
    (69, 3, 4, 2), (69, 3, 4, 3), (69, 2, 6, 3), (69, 5, 2, 0), (69, 4, 4, 3), (69, 5, 0, 0), (69, 4, 4, 1), (69, 5, 1, 0),
    (69, 4, 5, 1), (69, 3, 5, 2), (69, 3, 5, 3), (69, 4, 5, 3), (70, 4, 6, 1), (70, 3, 6, 2), (70, 5, 3, 0), (70, 3, 6, 3),
    (70, 4, 6, 3), (71, 5, 4, 0), (72, 5, 5, 0), (72, 5, 6, 0),
)

PRE, S0, S1, S2, S3, S4 = range(6)
STAGES = ("fetch", "stage0", "stage1", "stage2", "stage3", "stage4")


def column_sum(ref, at, value):
    ref[at] = ref[at] + jnp.sum(value, 0, keepdims=True)


def backward_kernel(length, plan, n_up_parts, *refs):
    (w_qkv, w_out, w_up, w_down), refs = refs[:4], refs[4:]
    x, c, n1, merged, logsum, attended, middle, n2, act, slope, g_down, small, refs = refs[:12] + (refs[12:],)
    output, input_grad, f_qkv, f_out, f_up, f_down, f_vec, g_qkv, g_out, g_up, mid_grad, ag, back, refs = refs[:13] + (
        refs[13:],
    )
    landing, refs = refs[:3], refs[3:]
    sets, refs = refs[: 7 * 7], refs[7 * 7 :]
    tmps, refs = refs[:3] + (None,) * 4, refs[3:]
    landing, refs = landing + refs[:4], refs[4:]
    vec_bufs, refs = refs[:7], refs[7:]
    (g_vec, narrow, wide, left, right, acc, out_acc, branch, dk_acc, dv_acc, sems, vec_sems, csem) = refs
    tokens, width = x.shape
    hidden = act.shape[1]
    tile = 512
    pairs = width // 128
    p = Place()
    greet_column(p)
    sets = [sets[7 * i : 7 * i + 7] for i in range(7)]
    half = hidden // n_up_parts
    entries = [
        (g_down, f_down),
        (g_up.at[0], f_up.at[:, :, :, pl.ds(0, half)]),
        (g_up.at[1], f_up.at[:, :, :, pl.ds(half, half)]),
        (g_out, f_out),
        (g_qkv.at[0], f_qkv.at[:, :, :, pl.ds(0, width)]),
        (g_qkv.at[1], f_qkv.at[:, :, :, pl.ds(width, width)]),
        (g_qkv.at[2], f_qkv.at[:, :, :, pl.ds(2 * width, width)]),
    ]
    rs = [Scatter(p, g, f, landing[k], sets[k], tmps[k], sems.at[k]) for k, (g, f) in enumerate(entries)]

    vectors = VectorScatter(p, g_vec, f_vec, vec_bufs, vec_sems)

    def turn(slot, first, count, step=1):
        table = {}
        for at, stage, k, i in plan:
            if at in range(first, first + count, step):
                table.setdefault(at, []).append(lambda stage=stage, k=k, i=i: getattr(rs[k], STAGES[stage])(i))
        hook(slot, table)

    loads = [
        pltpu.make_async_copy(c, left, csem.at[0]),
        pltpu.make_async_copy(n2, right, csem.at[1]),
    ]
    for load in loads:
        load.start()
    rs[0].start()
    narrow[...] = jnp.zeros_like(narrow)
    wide[...] = jnp.zeros_like(wide)
    g_vec[...] = jnp.zeros_like(g_vec)
    acc[...] = jnp.zeros_like(acc)
    out_acc[...] = jnp.zeros_like(out_acc)

    n_up = hidden // tile

    def ffn_body(wd, s, wu, g):
        j = pl.program_id(0)

        @pl.when(j == 0)
        def _():
            for load in loads:
                load.wait()

        @pl.when(j == n_up // 2 + 1)
        def _():
            rs[1].start()

        turn(3 * j, 0, 3 * n_up - 0, 3)
        grad = (dot(left[...], rows_of(wd), NT) * s[...].astype(F32)).astype(BF16)
        at = pl.ds(pl.multiple_of(j * tile, tile), tile)
        wide[:, at] = jnp.sum(grad.astype(F32), 0, keepdims=True)
        turn(3 * j + 1, 1, 3 * n_up - 1, 3)
        g[0] = dot(right[...], grad, TN).astype(BF16).reshape(g.shape[1:])
        turn(3 * j + 2, 2, 3 * n_up - 2, 3)
        acc[...] += dot(grad, rows_of(wu), NT)

    per = n_up // n_up_parts
    q_down = w_down.shape[2]
    blocks = tile // (2 * q_down)
    shape = g_up.shape[1:7]
    pltpu.emit_pipeline(
        ffn_body,
        grid=(n_up,),
        in_specs=[
            pl.BlockSpec((blocks, 2, q_down, width), lambda j: (j, 0, 0, 0)),
            pl.BlockSpec((tokens, tile), lambda j: (0, j)),
            whole_spec(w_up, tile),
        ],
        out_specs=[pl.BlockSpec((1,) + shape + (tile,), lambda j: (j // per, 0, 0, 0, 0, 0, 0, j % per))],
    )(w_down, slope, w_up, g_up)
    rs[2].start()
    load = pltpu.make_async_copy(n1, right, csem.at[1])
    load.start()
    base = 3 * n_up

    step = 128
    n_rows = tokens // step
    thin = hidden // (2 * n_rows)
    first_two = base

    def norm_two_body(m, a, w, o):
        i = pl.program_id(0)
        turn(first_two + i, first_two, n_rows)
        out_acc[...] += dot(a[...], rows_of(w))
        rows = pl.ds(pl.multiple_of(i * step, step), step)
        upstream = left[rows, :].astype(F32)
        part, gain, shift = norm_back(m[...], small[6:7], acc[rows, :])
        total = upstream + part
        o[...] = total
        low = total.astype(BF16)
        branch[rows, :] = low
        narrow[2:3] += jnp.sum(low.astype(F32), 0, keepdims=True)
        narrow[3:4] += jnp.sum(upstream, 0, keepdims=True)
        narrow[6:7] += gain[None]
        narrow[7:8] += shift[None]

    row_spec = pl.BlockSpec((step, width), lambda i: (i, 0))
    pltpu.emit_pipeline(
        norm_two_body,
        grid=(n_rows,),
        in_specs=[
            row_spec,
            pl.BlockSpec((tokens, thin), lambda i: (0, i)),
            pl.BlockSpec((thin // (2 * q_down), 2, q_down, width), lambda i: (i, 0, 0, 0)),
        ],
        out_specs=[row_spec],
    )(middle, act, w_down, mid_grad)
    base += n_rows

    n_out = width // 256
    first_out = base

    def out_body(a, w, g, o):
        i = pl.program_id(0)
        turn(first_out + i, first_out, n_out)
        g[...] = dot(a[...], branch[...], TN).astype(BF16).reshape(g.shape)
        rows = pl.ds(pl.multiple_of(i * 256, 256), 256)
        o[...] = dot(branch[rows, :], rows_of(w), NT).astype(BF16)

    q = g_out.shape[5]
    levels = 256 // (16 * q)
    assert levels == 1
    pltpu.emit_pipeline(
        out_body,
        grid=(n_out,),
        in_specs=[pl.BlockSpec((tokens, 256), lambda i: (0, i)), whole_spec(w_out)],
        out_specs=[
            pl.BlockSpec((1, 2, 2, 2, 2, q, width), lambda i: (i, 0, 0, 0, 0, 0, 0)),
            pl.BlockSpec((256, width), lambda i: (i, 0)),
        ],
    )(attended, w_out, g_out, ag)
    rs[3].start()
    base += n_out

    first_attend = base
    n_attend = (tokens // length) * pairs

    def attend_body(q, k, v, g, l, d):
        s, h = pl.program_id(0), pl.program_id(1)
        turn(first_attend + s * pairs + h, first_attend, n_attend)
        bwd_body(q, k, v, g, l.at[0, 0], d.at[0], d.at[1], d.at[2], dk_acc, dv_acc, 256)
        at = pl.ds(pl.multiple_of(h * 128, 128), 128)
        narrow[0:1, at] += jnp.sum(d[0].astype(F32), 0, keepdims=True)
        narrow[1:2, at] += jnp.sum(d[2].astype(F32), 0, keepdims=True)

    def head_spec(off):
        return pl.BlockSpec((length, 128), lambda s, h: (s, off + h))

    pltpu.emit_pipeline(
        attend_body,
        grid=(tokens // length, pairs),
        in_specs=[head_spec(0), head_spec(pairs), head_spec(2 * pairs), head_spec(0)]
        + [pl.BlockSpec((1, 1, 2, length), lambda s, h: (s, h, 0, 0))],
        out_specs=[pl.BlockSpec((3, length, 128), lambda s, h: (0, s, h))],
    )(merged, merged, merged, ag, logsum, back)
    base += n_attend
    load.wait()

    first_qkv = base
    n_qkv = 3 * width // tile
    per_part = width // tile

    def grad_body(d, g):
        j = pl.program_id(0)
        for k in (1, 2):

            @pl.when(j == k * per_part + 1)
            def _(k=k):
                rs[3 + k].start()

        turn(first_qkv + j, first_qkv, n_qkv)
        g[0] = dot(right[...], d[0], TN).astype(BF16).reshape(g.shape[1:])

    shape = g_qkv.shape[1:7]
    back_spec = pl.BlockSpec((1, tokens, tile), lambda j: (j // per_part, 0, j % per_part))
    pltpu.emit_pipeline(
        grad_body,
        grid=(n_qkv,),
        in_specs=[back_spec],
        out_specs=[
            pl.BlockSpec((1,) + shape + (tile,), lambda j: (j // per_part, 0, 0, 0, 0, 0, 0, j % per_part))
        ],
    )(back, g_qkv)
    rs[6].start()
    base += n_qkv
    first_in = base
    acc[...] = jnp.zeros_like(acc)

    def in_body(d, w):
        turn(first_in + pl.program_id(0), first_in, n_qkv)
        acc[...] += dot(d[0], rows_of(w), NT)

    pltpu.emit_pipeline(
        in_body,
        grid=(n_qkv,),
        in_specs=[pl.BlockSpec((1, tokens, tile), lambda j: (j % 3, 0, j // 3)), whole_spec(w_qkv, tile)],
    )(back, w_qkv)
    base += n_qkv

    first_one = base
    step = 256
    n_rows = tokens // step

    def norm_one_body(v, m, o):
        i = pl.program_id(0)
        turn(first_one + i, first_one, n_rows)
        rows = pl.ds(pl.multiple_of(i * step, step), step)
        part, gain, shift = norm_back(v[...].astype(F32), small[4:5], acc[rows, :])
        o[...] = m[...] + part
        narrow[4:5] += gain[None]
        narrow[5:6] += shift[None]

    row_spec = pl.BlockSpec((step, width), lambda i: (i, 0))
    pltpu.emit_pipeline(norm_one_body, grid=(n_rows,), in_specs=[row_spec] * 2, out_specs=[row_spec])(
        x, mid_grad, input_grad
    )
    base += n_rows
    for k in range(16):
        at = (k // 4, (k // 2) % 2, k % 2)
        g_vec[at + (pl.ds(0, 8),)] = narrow[:, 128 * (k // 2) : 128 * (k // 2) + 128]
        for i in range(2):
            g_vec[at + (pl.ds(8 + i, 1),)] = wide[:, 256 * k + 128 * i : 256 * k + 128 * i + 128]

    load = pltpu.make_async_copy(middle, acc, csem.at[0])
    load.start()
    first_down = base
    n_down = n_up // 2
    vector_steps = {0: [vectors.start], 1: [vectors.cores], 3: [vectors.over_x]}

    def down_body(a, w):
        j = pl.program_id(0)
        hook(j, vector_steps)
        turn(first_down + j, first_down, n_down)
        out_acc[...] += dot(a[...], rows_of(w))

    pltpu.emit_pipeline(
        down_body,
        grid=(n_down,),
        in_specs=[
            pl.BlockSpec((tokens, tile), lambda j: (0, n_down + j)),
            pl.BlockSpec((blocks, 2, q_down, width), lambda j: (n_down + j, 0, 0, 0)),
        ],
    )(act, w_down)
    base += n_down
    load.wait()
    n_last, step = 4, tokens // 4
    stores = []
    for i in range(n_last):
        rows = pl.ds(i * step, step)
        branch[rows, :] = (acc[rows, :] + (out_acc[rows, :] + small[3:4])).astype(BF16)
        stores.append(pltpu.make_async_copy(branch.at[rows], output.at[rows], csem.at[i]))
        stores[-1].start()
    vectors.over_y()
    for at, stage, k, i in plan:
        if at >= base:
            getattr(rs[k], STAGES[stage])(i)
    vectors.over_z()
    for r in rs + [vectors]:
        r.finish()
    for store in stores:
        store.wait()


def backward_call(weights, x, c, kept, length):
    n1, merged, logsum, attended, middle, n2, act, slope, g_down, small = kept
    tokens, width = x.shape
    hidden = act.shape[1]
    q, q_down = width // 64, hidden // 64
    parts = 2
    low = lambda *shape: jax.ShapeDtypeStruct(shape, BF16)
    full = lambda *shape: jax.ShapeDtypeStruct(shape, F32)
    vmem, any_space = pl.BlockSpec(memory_space=pltpu.VMEM), pl.BlockSpec(memory_space=pl.ANY)
    kinds = [(q_down, width, BF16)] + [(q, hidden // parts, BF16)] * 2 + [(q, width, BF16)] * 4
    scratch = []
    for kind in kinds:
        scratch += Scatter.scratch(*kind)
    scratch += [pltpu.VMEM((2, 2, 2, 2) + kind[:2], kind[2]) for kind in kinds[:3]]
    scratch += [pltpu.VMEM((4, 2, 2, 2) + kind[:2], kind[2]) for kind in kinds[3:]]
    scratch += VectorScatter.scratch()
    scratch += [
        pltpu.VMEM((4, 2, 2, 16, 128), F32),
        pltpu.VMEM((8, width), F32),
        pltpu.VMEM((1, hidden), F32),
        pltpu.VMEM((tokens, width), BF16),
        pltpu.VMEM((tokens, width), BF16),
        pltpu.VMEM((tokens, width), F32),
        pltpu.VMEM((tokens, width), F32),
        pltpu.VMEM((tokens, width), BF16),
        pltpu.VMEM((length, 128), F32),
        pltpu.VMEM((length, 128), F32),
        pltpu.SemaphoreType.DMA((7, RS_SEMS)),
        pltpu.SemaphoreType.DMA((12,)),
        pltpu.SemaphoreType.DMA((4,)),
    ]
    shards = [full(2, 2, q, 3 * width), full(2, 2, q, width), full(2, 2, q, hidden), full(2, 2, q_down, width)]
    outs = pl.pallas_call(
        lambda *refs: backward_kernel(length, PLAN, parts, *refs),
        in_specs=[any_space] * 15 + [vmem],
        out_specs=[any_space] * 2 + [vmem] * 5 + [any_space] * 9,
        out_shape=[low(tokens, width), full(tokens, width)]
        + shards
        + [full(16, 128)]
        + [
            low(3, 4, 2, 2, 2, 2, q, width),
            low(4, 2, 2, 2, 2, q, width),
            low(parts, 4, 2, 2, 2, 2, q, hidden // parts),
            full(tokens, width),
            low(tokens, width),
            low(3, tokens, width),
        ]
        + [jax.ShapeDtypeStruct((4, 2, 2, 2) + kind[:2], kind[2]) for kind in kinds[:3]],
        scratch_shapes=scratch,
        compiler_params=pltpu.CompilerParams(
            collective_id=1, has_side_effects=True, vmem_limit_bytes=66 * 10**6
        ),
        name="backward",
    )(*weights, x, c, n1, merged, logsum, attended, middle, n2, act, slope, g_down.reshape(4, 2, 2, 2, 2, q_down, width), small)
    grads = [o.reshape(-1, o.shape[-1]) for o in outs[2:6]]
    return outs[0], outs[1], grads, outs[6]


def forward_plain(x, weights, small, length):
    w_qkv, w_out, w_up, w_down = weights
    b_query, b_value, b_out, b_up, b_down, gain_one, shift_one, gain_two, shift_two = small
    xf = x.astype(F32)
    normed_one = layer_norm(xf, gain_one, shift_one).astype(BF16)
    qkv_bias = jnp.concatenate([b_query, jnp.zeros_like(b_query), b_value])
    merged = (dot(normed_one, w_qkv) + qkv_bias).astype(BF16)
    attended, logsum = attn_fwd(merged, length)
    middle = xf + (dot(attended, w_out) + b_out)
    normed_two = layer_norm(middle, gain_two, shift_two).astype(BF16)
    activated, slope = gelu_pair(dot(normed_two, w_up) + b_up)
    return normed_one, merged, logsum, attended, middle, normed_two, activated.astype(BF16), slope.astype(BF16)


def backward(x, c, weights, small, kept, length):
    w_qkv, w_out, w_up, w_down = weights
    b_down, gain_one, gain_two = small
    normed_one, merged, logsum, attended, middle, normed_two, activated, slope = kept
    width = x.shape[1]
    xf, cf = x.astype(F32), c.astype(F32)
    output = (middle + (dot(activated, w_down) + b_down)).astype(BF16)

    grad_down_bias = jnp.sum(cf, 0)
    hidden_grad = (dot(c, w_down, NT) * slope.astype(F32)).astype(BF16)
    grad_up_bias = jnp.sum(hidden_grad.astype(F32), 0)
    grad_up = dot(normed_two, hidden_grad, TN).astype(BF16)
    part, grad_gain_two, grad_shift_two = norm_back(middle, gain_two, dot(hidden_grad, w_up, NT))
    middle_grad = cf + part
    branch_grad = middle_grad.astype(BF16)
    grad_out_bias = jnp.sum(branch_grad.astype(F32), 0)
    grad_out = dot(attended, branch_grad, TN).astype(BF16)
    attended_grad = dot(branch_grad, w_out, NT).astype(BF16)
    back = attn_bwd(merged, attended_grad, logsum, length)
    grad_query_bias = jnp.sum(back[0].astype(F32), 0)
    grad_value_bias = jnp.sum(back[2].astype(F32), 0)
    grad_qkv = jnp.concatenate([dot(normed_one, back[j], TN).astype(BF16) for j in range(3)], 1)
    normed_one_grad = sum(dot(back[j], w_qkv[:, j * width : (j + 1) * width], NT) for j in range(3))
    part, grad_gain_one, grad_shift_one = norm_back(xf, gain_one, normed_one_grad)
    input_grad = middle_grad + part
    return (
        output,
        input_grad,
        (grad_qkv, grad_out, grad_up),
        (
            grad_query_bias,
            grad_value_bias,
            grad_out_bias,
            grad_up_bias,
            grad_down_bias,
            grad_gain_one,
            grad_shift_one,
            grad_gain_two,
            grad_shift_two,
        ),
    )


def pack_shards(vectors):
    wide = vectors[3]
    narrow = jnp.stack([v for k, v in enumerate(vectors) if k != 3])
    zeros = jnp.zeros_like(narrow)
    odd = lax.axis_index("fsdp") % 2 == 1
    lanes = jnp.concatenate([jnp.where(odd, zeros, narrow), jnp.where(odd, narrow, zeros)], 1)
    rows = jnp.concatenate([lanes, wide.reshape(2, 128)], 0)
    return jnp.pad(rows, ((0, 64 - rows.shape[0]), (0, 0)))


def unpack_shard(packed):
    narrow = packed[:8, :64]
    wide = packed[8:10].reshape(256)
    return tuple(narrow[j] for j in range(3)) + (wide,) + tuple(narrow[j] for j in range(3, 8))


def local_ring(block_input, *rest):
    shards, cotangent = rest[:13], rest[13]
    length, width = block_input.shape[1:]
    x, c = block_input.reshape(-1, width), cotangent.reshape(-1, width)
    weights, kept = forward_call(shards[:4] + (pack_shards(shards[4:]),), x, c, length)
    output, input_grad, grads, vec = backward_call(weights, x, c, kept, length)
    whole = (output.reshape(block_input.shape), input_grad.reshape(block_input.shape))
    return whole + tuple(grads) + unpack_shard(vec)


def local_any(block_input, *rest):
    shards, cotangent = rest[:13], rest[13]
    length, width = block_input.shape[1:]
    x, c = block_input.reshape(-1, width), cotangent.reshape(-1, width)
    gathered = [lax.all_gather(shard, "fsdp", axis=0, tiled=True) for shard in shards]
    weights, small = gathered[:4], tuple(v.astype(F32) for v in gathered[4:])
    kept = forward_plain(x, weights, small, length)
    output, input_grad, mats, vecs = backward(x, c, weights, (small[4], small[5], small[7]), kept, length)
    mats += (dot(kept[6], c, TN),)

    def reduce(grad):
        part = lax.psum_scatter(grad.astype(F32), "fsdp", scatter_dimension=0, tiled=True)
        return lax.psum(part, "seq")

    whole = (output.reshape(block_input.shape), input_grad.reshape(block_input.shape))
    return whole + tuple(reduce(grad) for grad in mats + vecs)


def solution(mesh):
    split = P(("fsdp", "seq"), None, None)
    matrix, vector = P("fsdp", None), P("fsdp")
    in_specs = (split,) + (matrix,) * 4 + (vector,) * 9 + (split,)
    out_specs = (split, split) + (matrix,) * 4 + (vector,) * 9
    local = local_ring if (mesh.shape["fsdp"], mesh.shape["seq"]) == (16, 2) else local_any
    return jax.shard_map(local, mesh=mesh, in_specs=in_specs, out_specs=out_specs, check_vma=False)
```
